8 devices in a mesh: frag: 1 (over z), dev: 8 (over y, x, core).
Axes of the slice: x: 2, y: 2, z: 1, core: 2. Of those that a mesh axis runs over, the one named last changes fastest.
Arguments:
- ao_ints: bfloat16 [120, 120, 120, 120], P(('frag', 'dev'))
- c_occ: bfloat16 [120, 8], P('frag')
- c_vir: bfloat16 [120, 108], P('frag')
Outputs:
- output 1: float32 [108, 108, 64], P('frag', None, 'dev')
- output 2: float32 [8, 108, 864], P('frag', None, 'dev')
All inputs are finite; a program needn't handle non-finite values.
Results may differ from the reference program's by a relative error of at most 0.001.
Values are sent between devices in bfloat16 or wider.
A program may use at most 1 GiB of HBM per device.

```python
import jax
import jax.numpy as jnp
from jax import lax

N_AO = 120
N_OCC = 8
N_VIR = 108


def setup_inputs(seed: int = 0, part: int = 0) -> dict:
    part_key = jax.random.fold_in(jax.random.key(seed), part)
    key_ints, key_occ, key_vir = jax.random.split(part_key, 3)
    row_keys = jax.random.split(key_ints, N_AO)

    def draw_row(row_key):
        return jax.random.normal(row_key, (N_AO, N_AO, N_AO), jnp.float32).astype(jnp.bfloat16)

    ao_ints = lax.map(draw_row, row_keys)
    coef_scale = N_AO ** -0.5
    c_occ = (jax.random.normal(key_occ, (N_AO, N_OCC), jnp.float32) * coef_scale).astype(jnp.bfloat16)
    c_vir = (jax.random.normal(key_vir, (N_AO, N_VIR), jnp.float32) * coef_scale).astype(jnp.bfloat16)
    return {'ao_ints': ao_ints, 'c_occ': c_occ, 'c_vir': c_vir}


def reference(ao_ints, c_occ, c_vir):
    occ32 = c_occ.astype(jnp.float32)
    vir32 = c_vir.astype(jnp.float32)

    def first_half(ao_row):
        quarter = jnp.einsum('qrs,rx->qsx', ao_row.astype(jnp.float32), occ32).astype(jnp.bfloat16)
        quarter32 = quarter.astype(jnp.float32)
        half_oo = jnp.einsum('qsx,sj->qxj', quarter32, occ32).astype(jnp.bfloat16)
        half_ov = jnp.einsum('qsx,sb->qxb', quarter32, vir32).astype(jnp.bfloat16)
        return half_oo, half_ov

    half_oo, half_ov = lax.map(first_half, ao_ints)
    half_oo = half_oo.reshape(N_AO, N_AO, N_OCC * N_OCC).astype(jnp.float32)
    half_ov = half_ov.reshape(N_AO, N_AO, N_OCC * N_VIR).astype(jnp.float32)
    mid_oo = jnp.einsum('pqm,qb->pbm', half_oo, vir32).astype(jnp.bfloat16).astype(jnp.float32)
    mid_ov = jnp.einsum('pqm,qa->pam', half_ov, vir32).astype(jnp.bfloat16).astype(jnp.float32)
    v_abij = jnp.einsum('pa,pbm->abm', vir32, mid_oo)
    v_iajb = jnp.einsum('pi,pam->iam', occ32, mid_ov)
    return v_abij, v_iajb
```

```python
import jax
import jax.numpy as jnp
from jax import lax
from jax.experimental import pallas as pl
from jax.experimental.pallas import tpu as pltpu
from jax.sharding import PartitionSpec as P

MESH = pl.DeviceIdType.MESH
BF = jnp.bfloat16
F32 = jnp.float32
ND = 8
NP = 15
NQ = 120
NO = 8
NV = 108
ROWS = NQ * NQ
NBUF = 4
SPLIT = 5
AB = 7


def mm(a, b):
    return jnp.dot(a, b, preferred_element_type=F32)


def mm_nt(a, b):
    return lax.dot_general(a, b, (((1,), (1,)), ((), ())), preferred_element_type=F32)


def iota(shape, dim):
    return lax.broadcasted_iota(jnp.int32, shape, dim)


def one_hot(mask):
    return jnp.where(mask, 1.0, 0.0).astype(BF)


def kernel(a_ref, co_ref, cv_ref, o1_ref, o2_ref,
           abuf, tbuf, sg, rg, s1, r1, k1, k4, v1k, e6, cot, cvt, cv,
           asem, sgsem, rgsem, s1sem, r1sem):
    me = lax.axis_index('dev')
    frag = lax.axis_index('frag')

    def a_copies(p):
        slot = lax.rem(p, NBUF)
        step = ROWS // SPLIT
        return [pltpu.make_async_copy(a_ref.at[p, pl.ds(k * step, step)],
                                      abuf.at[slot, pl.ds(k * step, step)],
                                      asem.at[slot]) for k in range(SPLIT)]

    def a_start(p):
        for c in a_copies(p):
            c.start()

    def a_wait(p):
        slot = lax.rem(p, NBUF)
        pltpu.make_async_copy(a_ref.at[p], abuf.at[slot], asem.at[slot]).wait()

    for p in range(NBUF - 1):
        a_start(p)

    barrier = pltpu.get_barrier_semaphore()
    for k in range(1, ND):
        pl.semaphore_signal(barrier, inc=1, device_id=(frag, lax.rem(me + k, ND)), device_id_type=MESH)

    cot[...] = jnp.zeros(cot.shape, BF)
    cvt[...] = jnp.zeros(cvt.shape, BF)
    cot[0:NO, 0:NQ] = co_ref[...]
    cvt[0:NV, 0:NQ] = cv_ref[...]
    cv[...] = mm_nt(one_hot(iota((128, 128), 0) == iota((128, 128), 1)), cvt[...]).astype(BF)
    xr = mm(one_hot((iota((64, 16), 0) >> 3) == iota((64, 16), 1)), cot[...]).astype(BF)
    diff = iota((128, 960), 1) - iota((128, 960), 0)
    hit = diff == 0
    for k in range(1, 8):
        hit = hit | (diff == 120 * k)
    off = iota((64, 960), 1) - 120 * (iota((64, 960), 0) & 7)
    k1[...] = jnp.where((off >= 0) & (off < 120), mm(xr, one_hot(hit)), 0.0).astype(BF)
    pi = mm(one_hot((iota((128, 16), 0) & 7) == iota((128, 16), 1)), cot[...]).astype(BF)
    for c in range(15):
        col = iota((128, 128), 1)
        w = mm(pi, one_hot(iota((128, 128), 0) == (col >> 4) + 8 * c))
        k4[:, c * 128:(c + 1) * 128] = jnp.where((iota((128, 128), 0) >> 3) == (col & 15), w, 0.0).astype(BF)
    e6[...] = one_hot((iota((128, 960), 1) >> 3) == iota((128, 960), 0))

    def v1_rows(t, carry):
        row = iota((96, 128), 0) + 96 * t
        z = mm(one_hot((row >> 3) == iota((96, 128), 1)), cvt[...]).astype(BF)
        w = mm(z, e6[...])
        keep = (iota((96, 960), 0) & 7) == (iota((96, 960), 1) & 7)
        v1k[pl.ds(pl.multiple_of(96 * t, 96), 96), :] = jnp.where(keep, w, 0.0).astype(BF)
        return carry

    lax.fori_loop(0, 9, v1_rows, 0)

    pl.semaphore_wait(barrier, ND - 1)

    def step1(p):
        slot = lax.rem(p, NBUF)
        tslot = lax.rem(p, 2)
        pad = jnp.zeros((960, 8), BF)
        for g in range(8):
            left = jnp.concatenate([abuf[slot, 1920 * g:1920 * g + 960, :], pad], axis=1)
            if g < 7:
                right = jnp.concatenate([abuf[slot, 1920 * g + 960:1920 * g + 1920, :], pad], axis=1)
                out = mm(k1[...], jnp.concatenate([left, right], axis=1))
                lo = out[:, :128].reshape(8, 8, 128)
                hi = out[:, 128:].reshape(8, 8, 128)
            else:
                lo = mm(k1[...], left).reshape(8, 8, 128)
                hi = jnp.zeros((8, 8, 128), F32)
            tbuf[tslot, :, 16 * g:16 * g + 16, :] = jnp.concatenate([lo, hi], axis=1).astype(BF)

    def step23(p):
        t = tbuf[lax.rem(p, 2)].reshape(1024, 128)
        h = mm(t, cv[...]).astype(BF).reshape(8, 128, 128)
        for x in range(0, 8, 2):
            g = mm(cvt[0:112, :], jnp.concatenate([h[x], h[x + 1]], axis=1)).astype(BF)
            sg[x, p] = g[:, :128]
            sg[x + 1, p] = g[:, 128:]
        hoo = mm_nt(cot[...], t)
        hoo = jnp.concatenate([hoo[0:8, 128 * x:128 * x + 128] for x in range(8)], axis=0).astype(BF)
        s1[:, p] = mm(hoo, cv[...]).astype(BF).reshape(8, 8, 128)

    def sends(p):
        out = []
        for k in range(1, ND):
            dst = lax.rem(me + k, ND)
            out.append(pltpu.make_async_remote_copy(
                src_ref=sg.at[dst, p], dst_ref=rg.at[me, p], send_sem=sgsem.at[k], recv_sem=rgsem.at[me],
                device_id=(frag, dst), device_id_type=MESH))
            out.append(pltpu.make_async_remote_copy(
                src_ref=s1.at[dst, p], dst_ref=r1.at[me, p], send_sem=s1sem.at[k], recv_sem=r1sem.at[me],
                device_id=(frag, dst), device_id_type=MESH))
        return out

    def send(p):
        for c in sends(p):
            c.start()
        rg[me, p] = sg[me, p]
        r1[me, p] = s1[me, p]

    a_wait(0)
    a_start(NBUF - 1)
    step1(0)

    def body(p, carry):
        @pl.when(p + NBUF - 1 < NP)
        def _():
            a_start(p + NBUF - 1)

        @pl.when(p >= 2)
        def _():
            send(p - 2)

        a_wait(p)
        step1(p)
        step23(p - 1)
        return carry

    lax.fori_loop(1, NP, body, 0)
    send(NP - 2)
    step23(NP - 1)
    send(NP - 1)

    for k in range(1, ND):
        src = lax.rem(me + k, ND)
        pltpu.make_async_copy(r1.at[src], r1.at[src], r1sem.at[src]).wait()
        pltpu.make_async_copy(rg.at[src], rg.at[src], rgsem.at[src]).wait()

    v = r1[...].reshape(960, 128)

    def v1_out(t, carry):
        w = mm(v1k[pl.ds(pl.multiple_of(96 * t, 96), 96), :], v)
        o1_ref[pl.ds(12 * t, 12)] = w.reshape(12, 8, 128)[:, :, :NV]
        return carry

    lax.fori_loop(0, 9, v1_out, 0)

    for ab in range(0, AB, 2):
        left = rg[:, :, 16 * ab:16 * ab + 16, :].reshape(1920, 128)
        if ab + 1 < AB:
            right = rg[:, :, 16 * ab + 16:16 * ab + 32, :].reshape(1920, 128)
            w = mm(k4[...], jnp.concatenate([left, right], axis=1)).reshape(16, 8, 256)
            o2_ref[16 * ab:16 * ab + 16] = w[:, :, :NV]
            o2_ref[16 * ab + 16:16 * ab + 32] = w[:, :, 128:128 + NV]
        else:
            w = mm(k4[...], left).reshape(16, 8, 128)
            o2_ref[16 * ab:NV] = w[:NV - 16 * ab, :, :NV]

    for k in range(1, ND):
        dst = lax.rem(me + k, ND)
        pltpu.make_async_copy(sg.at[dst], sg.at[dst], sgsem.at[k]).wait()
        pltpu.make_async_copy(s1.at[dst], s1.at[dst], s1sem.at[k]).wait()


def solution(mesh):
    def local_part(ao, co, cv):
        a = ao.reshape(NP, ROWS, NQ)
        vm = pl.BlockSpec(memory_space=pltpu.VMEM)
        o1, o2 = pl.pallas_call(
            kernel,
            out_shape=[jax.ShapeDtypeStruct((NV, NO, NV), F32), jax.ShapeDtypeStruct((NV, NO, NV), F32)],
            in_specs=[pl.BlockSpec(memory_space=pl.ANY), vm, vm],
            out_specs=[vm, vm],
            scratch_shapes=[
                pltpu.VMEM((NBUF, ROWS, NQ), BF),
                pltpu.VMEM((2, 8, 128, 128), BF),
                pltpu.VMEM((8, NP, 112, 128), BF),
                pltpu.VMEM((8, NP, 112, 128), BF),
                pltpu.VMEM((8, NP, 8, 128), BF),
                pltpu.VMEM((8, NP, 8, 128), BF),
                pltpu.VMEM((64, 960), BF),
                pltpu.VMEM((128, 1920), BF),
                pltpu.VMEM((864, 960), BF),
                pltpu.VMEM((128, 960), BF),
                pltpu.VMEM((16, 128), BF),
                pltpu.VMEM((128, 128), BF),
                pltpu.VMEM((128, 128), BF),
                pltpu.SemaphoreType.DMA((NBUF,)),
                pltpu.SemaphoreType.DMA((ND,)),
                pltpu.SemaphoreType.DMA((ND,)),
                pltpu.SemaphoreType.DMA((ND,)),
                pltpu.SemaphoreType.DMA((ND,)),
            ],
            compiler_params=pltpu.CompilerParams(collective_id=0, has_side_effects=True,
                                                 vmem_limit_bytes=60 * 1024 * 1024),
            name='mo_blocks',
        )(a, co.T, cv.T)
        return o1.transpose(0, 2, 1), o2.transpose(1, 0, 2)

    return jax.shard_map(local_part, mesh=mesh,
                         in_specs=(P(('frag', 'dev')), P('frag'), P('frag')),
                         out_specs=(P('frag', None, 'dev'), P('frag', None, 'dev')),
                         check_vma=False)
```

```python
import jax
import jax.numpy as jnp
from jax import lax
from jax.experimental import pallas as pl
from jax.experimental.pallas import tpu as pltpu
from jax.sharding import PartitionSpec as P

MESH = pl.DeviceIdType.MESH
BF = jnp.bfloat16
F32 = jnp.float32
ND = 8
NP = 15
NQ = 120
NO = 8
NV = 108
ROWS = NQ * NQ
NBUF = 4
SPLIT = 5
AB = 7
NE = 2
EX = 16 * NE
RSR = 8 * (NV - EX)
NCH = 2
CH = RSR // (2 * NCH)


def mm(a, b):
    return jnp.dot(a, b, preferred_element_type=F32)


def mm_nt(a, b):
    return lax.dot_general(a, b, (((1,), (1,)), ((), ())), preferred_element_type=F32)


def iota(shape, dim):
    return lax.broadcasted_iota(jnp.int32, shape, dim)


def one_hot(mask):
    return jnp.where(mask, 1.0, 0.0).astype(BF)


def kernel(a_ref, co_ref, cv_ref, o1_ref, o2_ref,
           abuf, tbuf, sg, rg, rs, s1, r1, sb, p1, z2, p2, k1, k4, k4c, v1k, e6, coin, cvin, cot, cvt, cv,
           asem, csem, sgsem, rgsem, s1sem, r1sem, ssem, rssem, p1s, p1r, p2s, p2r):
    me = lax.axis_index('dev')
    frag = lax.axis_index('frag')
    core = lax.rem(me, 2)
    mx = lax.rem(me // 2, 2)
    my = me // 4
    sib = me + 1 - 2 * core
    xn = me + 2 - 4 * mx
    yn = me + 4 - 8 * my
    dg = xn + 4 - 8 * my
    cols = [me, xn, yn, dg]

    def a_copies(p):
        slot = lax.rem(p, NBUF)
        step = ROWS // SPLIT
        return [pltpu.make_async_copy(a_ref.at[p, pl.ds(k * step, step)],
                                      abuf.at[slot, pl.ds(k * step, step)],
                                      asem.at[slot]) for k in range(SPLIT)]

    def a_start(p):
        for c in a_copies(p):
            c.start()

    def a_wait(p):
        slot = lax.rem(p, NBUF)
        pltpu.make_async_copy(a_ref.at[p], abuf.at[slot], asem.at[slot]).wait()

    cin = [pltpu.make_async_copy(co_ref, coin, csem.at[0]), pltpu.make_async_copy(cv_ref, cvin, csem.at[1])]
    for c in cin:
        c.start()
    for p in range(NBUF - 1):
        a_start(p)

    barrier = pltpu.get_barrier_semaphore()
    for k in range(1, ND):
        pl.semaphore_signal(barrier, inc=1, device_id=(frag, lax.rem(me + k, ND)), device_id_type=MESH)

    cot[...] = jnp.zeros(cot.shape, BF)
    cvt[...] = jnp.zeros(cvt.shape, BF)
    for c in cin:
        c.wait()
    cot[0:NO, 0:NQ] = coin[...]
    cvt[0:NV, 0:NQ] = cvin[...]
    cv[...] = mm_nt(one_hot(iota((128, 128), 0) == iota((128, 128), 1)), cvt[...]).astype(BF)
    xr = mm(one_hot((iota((64, 16), 0) >> 3) == iota((64, 16), 1)), cot[...]).astype(BF)
    diff = iota((128, 960), 1) - iota((128, 960), 0)
    hit = diff == 0
    for k in range(1, 8):
        hit = hit | (diff == 120 * k)
    off = iota((64, 960), 1) - 120 * (iota((64, 960), 0) & 7)
    k1[...] = jnp.where((off >= 0) & (off < 120), mm(xr, one_hot(hit)), 0.0).astype(BF)
    pi = mm(one_hot((iota((128, 16), 0) & 7) == iota((128, 16), 1)), cot[...]).astype(BF)
    for c in range(15):
        col = iota((128, 128), 1)
        w = mm(pi, one_hot(iota((128, 128), 0) == (col >> 4) + 8 * c))
        k4[:, c * 128:(c + 1) * 128] = jnp.where((iota((128, 128), 0) >> 3) == (col & 15), w, 0.0).astype(BF)
    for h, d in enumerate((me, sib)):
        col = iota((128, 240), 1)
        w = mm(pi, one_hot(iota((128, 240), 0) == (col >> 4) + NP * d))
        keep = (iota((128, 240), 0) >> 3) == (col & 15)
        k4c[h] = jnp.where(keep, w, 0.0).astype(BF)
    e6[...] = one_hot((iota((128, 960), 1) >> 3) == iota((128, 960), 0))

    def v1_rows(t):
        row = iota((96, 128), 0) + 96 * t
        z = mm(one_hot((row >> 3) == iota((96, 128), 1)), cvt[...]).astype(BF)
        w = mm(z, e6[...])
        keep = (iota((96, 960), 0) & 7) == (iota((96, 960), 1) & 7)
        v1k[pl.ds(pl.multiple_of(96 * t, 96), 96), :] = jnp.where(keep, w, 0.0).astype(BF)

    pl.semaphore_wait(barrier, ND - 1)

    def step1(p):
        slot = lax.rem(p, NBUF)
        tslot = lax.rem(p, 2)
        pad = jnp.zeros((960, 8), BF)
        for g in range(8):
            left = jnp.concatenate([abuf[slot, 1920 * g:1920 * g + 960, :], pad], axis=1)
            if g < 7:
                right = jnp.concatenate([abuf[slot, 1920 * g + 960:1920 * g + 1920, :], pad], axis=1)
                out = mm(k1[...], jnp.concatenate([left, right], axis=1))
                lo = out[:, :128].reshape(8, 8, 128)
                hi = out[:, 128:].reshape(8, 8, 128)
            else:
                lo = mm(k1[...], left).reshape(8, 8, 128)
                hi = jnp.zeros((8, 8, 128), F32)
            tbuf[tslot, :, 16 * g:16 * g + 16, :] = jnp.concatenate([lo, hi], axis=1).astype(BF)

    def step23(p):
        t = tbuf[lax.rem(p, 2)].reshape(1024, 128)
        h = mm(t, cv[...]).astype(BF).reshape(8, 128, 128)
        for x in range(0, 8, 2):
            g = mm(cvt[0:112, :], jnp.concatenate([h[x], h[x + 1]], axis=1)).astype(BF)
            sg[x, p] = g[:, :128]
            sg[x + 1, p] = g[:, 128:]
        hoo = mm_nt(cot[...], t)
        hoo = jnp.concatenate([hoo[0:8, 128 * x:128 * x + 128] for x in range(8)], axis=0).astype(BF)
        s1[:, p] = mm(hoo, cv[...]).astype(BF).reshape(8, 8, 128)

    def sends(p):
        out = []
        for k in range(1, ND):
            dst = lax.rem(me + k, ND)
            out.append(pltpu.make_async_remote_copy(
                src_ref=sg.at[dst, p, 0:EX], dst_ref=rg.at[me, p], send_sem=sgsem.at[k], recv_sem=rgsem.at[me],
                device_id=(frag, dst), device_id_type=MESH))
            out.append(pltpu.make_async_remote_copy(
                src_ref=s1.at[dst, p], dst_ref=r1.at[me, p], send_sem=s1sem.at[k], recv_sem=r1sem.at[me],
                device_id=(frag, dst), device_id_type=MESH))
        for k in range(4):
            out.append(pltpu.make_async_remote_copy(
                src_ref=sg.at[cols[k] + 1 - 2 * core, p, EX:112], dst_ref=rs.at[k, p],
                send_sem=ssem, recv_sem=rssem, device_id=(frag, sib), device_id_type=MESH))
        return out

    def send(p):
        for c in sends(p):
            c.start()
        rg[me, p] = sg[me, p, 0:EX]
        r1[me, p] = s1[me, p]

    a_wait(0)
    a_start(NBUF - 1)
    step1(0)

    def body(p, carry):
        @pl.when(p + NBUF - 1 < NP)
        def _():
            a_start(p + NBUF - 1)

        @pl.when(p >= 2)
        def _():
            send(p - 2)

        a_wait(p)
        step1(p)
        step23(p - 1)

        @pl.when(p < 10)
        def _():
            v1_rows(p - 1)

        return carry

    lax.fori_loop(1, NP, body, 0)
    send(NP - 2)
    step23(NP - 1)
    send(NP - 1)

    def rcopy(src, dst, ss, rr, dev):
        return pltpu.make_async_remote_copy(src_ref=src, dst_ref=dst, send_sem=ss, recv_sem=rr,
                                            device_id=(frag, dev), device_id_type=MESH)

    def bwait(view, sem):
        pltpu.make_async_copy(view, view, sem).wait()

    bwait(rs, rssem)
    for u, v in ((1, 3), (2, 0)):
        for b in range(AB - NE):
            side = []
            for c in (u, v):
                own = sg[cols[c], :, EX + 16 * b:EX + 16 * b + 16, :].reshape(240, 128)
                oth = rs[c, :, 16 * b:16 * b + 16, :].reshape(240, 128)
                side.append((own, oth))
            w = (mm(k4c[0], jnp.concatenate([side[0][0], side[1][0]], axis=1))
                 + mm(k4c[1], jnp.concatenate([side[0][1], side[1][1]], axis=1)))
            n = min(128, RSR - 128 * b)
            sb[u, 128 * b:128 * b + n, :] = w[:n, :128]
            sb[v, 128 * b:128 * b + n, :] = w[:n, 128:]

    def rows(half, c):
        return pl.ds((half * NCH + c) * CH, CH)

    first = ((1, xn, yn, 2), (2, yn, xn, 1))
    for c in range(NCH):
        for half, (col, peer, _, _) in enumerate(first):
            for m, cc in enumerate((col, 3)):
                rcopy(sb.at[cc, rows(half, c)], p1.at[m, rows(half, c)],
                      p1s.at[half, c], p1r.at[half, c], peer).start()

    for k in range(1, ND):
        src = lax.rem(me + k, ND)
        bwait(r1.at[src], r1sem.at[src])
        bwait(rg.at[src], rgsem.at[src])

    v = r1[...].reshape(960, 128)

    def v1_out(t, carry):
        w = mm(v1k[pl.ds(pl.multiple_of(96 * t, 96), 96), :], v)
        o1_ref[pl.ds(12 * t, 12)] = w.reshape(12, 8, 128)[:, :, :NV]
        return carry

    lax.fori_loop(0, 9, v1_out, 0)

    for ab in range(0, NE, 2):
        left = rg[:, :, 16 * ab:16 * ab + 16, :].reshape(1920, 128)
        right = rg[:, :, 16 * ab + 16:16 * ab + 32, :].reshape(1920, 128)
        w = mm(k4[...], jnp.concatenate([left, right], axis=1)).reshape(16, 8, 256)
        o2_ref[16 * ab:16 * ab + 16] = w[:, :, :NV]
        o2_ref[16 * ab + 16:16 * ab + 32] = w[:, :, 128:128 + NV]

    for c in range(NCH):
        for half, (_, _, peer, col) in enumerate(first):
            bwait(p1.at[:, rows(half, c)], p1r.at[half, c])
            z2[rows(half, c), :] = sb[col, rows(half, c), :] + p1[1, rows(half, c), :]
        for half, (_, _, peer, col) in enumerate(first):
            rcopy(z2.at[rows(half, c)], p2.at[rows(half, c)], p2s.at[half, c], p2r.at[half, c], peer).start()
    for c in range(NCH):
        for half in range(2):
            bwait(p2.at[rows(half, c)], p2r.at[half, c])
            w = sb[0, rows(half, c), :] + p1[0, rows(half, c), :] + p2[rows(half, c), :]
            a0 = EX + (half * NCH + c) * CH // 8
            o2_ref[a0:a0 + CH // 8] = w.reshape(CH // 8, 8, 128)[:, :, :NV]

    for k in range(1, ND):
        dst = lax.rem(me + k, ND)
        bwait(rg.at[dst], sgsem.at[k])
        bwait(s1.at[dst], s1sem.at[k])
    bwait(rs, ssem)
    for c in range(NCH):
        for half in range(2):
            bwait(p1.at[:, rows(half, c)], p1s.at[half, c])
            bwait(p2.at[rows(half, c)], p2s.at[half, c])


def solution(mesh):
    def local_part(ao, co, cv):
        a = ao.reshape(NP, ROWS, NQ)
        vm = pl.BlockSpec(memory_space=pltpu.VMEM)
        o1, o2 = pl.pallas_call(
            kernel,
            out_shape=[jax.ShapeDtypeStruct((NV, NO, NV), F32), jax.ShapeDtypeStruct((NV, NO, NV), F32)],
            in_specs=[pl.BlockSpec(memory_space=pltpu.HBM)] * 3,
            out_specs=[vm, vm],
            scratch_shapes=[
                pltpu.VMEM((NBUF, ROWS, NQ), BF),
                pltpu.VMEM((2, 8, 128, 128), BF),
                pltpu.VMEM((8, NP, 112, 128), BF),
                pltpu.VMEM((8, NP, EX, 128), BF),
                pltpu.VMEM((4, NP, 112 - EX, 128), BF),
                pltpu.VMEM((8, NP, 8, 128), BF),
                pltpu.VMEM((8, NP, 8, 128), BF),
                pltpu.VMEM((4, RSR, 128), F32),
                pltpu.VMEM((2, RSR, 128), F32),
                pltpu.VMEM((RSR, 128), F32),
                pltpu.VMEM((RSR, 128), F32),
                pltpu.VMEM((64, 960), BF),
                pltpu.VMEM((128, 1920), BF),
                pltpu.VMEM((2, 128, 240), BF),
                pltpu.VMEM((864, 960), BF),
                pltpu.VMEM((128, 960), BF),
                pltpu.VMEM((NO, NQ), BF),
                pltpu.VMEM((NV, NQ), BF),
                pltpu.VMEM((16, 128), BF),
                pltpu.VMEM((128, 128), BF),
                pltpu.VMEM((128, 128), BF),
                pltpu.SemaphoreType.DMA((NBUF,)),
                pltpu.SemaphoreType.DMA((2,)),
                pltpu.SemaphoreType.DMA((ND,)),
                pltpu.SemaphoreType.DMA((ND,)),
                pltpu.SemaphoreType.DMA((ND,)),
                pltpu.SemaphoreType.DMA((ND,)),
                pltpu.SemaphoreType.DMA,
                pltpu.SemaphoreType.DMA,
                pltpu.SemaphoreType.DMA((2, NCH)),
                pltpu.SemaphoreType.DMA((2, NCH)),
                pltpu.SemaphoreType.DMA((2, NCH)),
                pltpu.SemaphoreType.DMA((2, NCH)),
            ],
            compiler_params=pltpu.CompilerParams(collective_id=0, has_side_effects=True,
                                                 vmem_limit_bytes=34 * 1024 * 1024),
            name='mo_blocks',
        )(a, co.T, cv.T)
        return o1.transpose(0, 2, 1), o2.transpose(1, 0, 2)

    return jax.shard_map(local_part, mesh=mesh,
                         in_specs=(P(('frag', 'dev')), P('frag'), P('frag')),
                         out_specs=(P('frag', None, 'dev'), P('frag', None, 'dev')),
                         check_vma=False)
```

```python
import jax
import jax.numpy as jnp
from jax import lax
from jax.experimental import pallas as pl
from jax.experimental.pallas import tpu as pltpu
from jax.sharding import PartitionSpec as P

MESH = pl.DeviceIdType.MESH
BF = jnp.bfloat16
F32 = jnp.float32
ND = 8
NP = 15
NQ = 120
NO = 8
NV = 108
ROWS = NQ * NQ
NBUF = 4
SPLIT = 5
AB = 7
NE = 2
EX = 16 * NE
GO = EX
SENT = EX + 8
RS0 = EX + 16
XR = 128
RSR = 8 * (NV - EX)
NCH = 2
CH = RSR // (2 * NCH)


def mm(a, b):
    return jnp.dot(a, b, preferred_element_type=F32)


def mm_nt(a, b):
    return lax.dot_general(a, b, (((1,), (1,)), ((), ())), preferred_element_type=F32)


def iota(shape, dim):
    return lax.broadcasted_iota(jnp.int32, shape, dim)


def one_hot(mask):
    return jnp.where(mask, 1.0, 0.0).astype(BF)


def kernel(a_ref, co_ref, cv_ref, o1_ref, o2_ref,
           abuf, tbuf, sg, rg, rs, sb, p1, z2, p2, k1, k4, k4c, v1k, e6, coin, cvin, cot, cvt, cv,
           asem, csem, sgsem, rgsem, ssem, rssem, p1s, p1r, p2s, p2r):
    me = lax.axis_index('dev')
    frag = lax.axis_index('frag')
    core = lax.rem(me, 2)
    mx = lax.rem(me // 2, 2)
    my = me // 4
    sib = me + 1 - 2 * core
    xn = me + 2 - 4 * mx
    yn = me + 4 - 8 * my
    dg = xn + 4 - 8 * my
    cols = [me, xn, yn, dg]

    def a_copies(p):
        slot = lax.rem(p, NBUF)
        step = ROWS // SPLIT
        return [pltpu.make_async_copy(a_ref.at[p, pl.ds(k * step, step)],
                                      abuf.at[slot, pl.ds(k * step, step)],
                                      asem.at[slot]) for k in range(SPLIT)]

    def a_start(p):
        for c in a_copies(p):
            c.start()

    def a_wait(p):
        slot = lax.rem(p, NBUF)
        pltpu.make_async_copy(a_ref.at[p], abuf.at[slot], asem.at[slot]).wait()

    cin = [pltpu.make_async_copy(co_ref, coin, csem.at[0]), pltpu.make_async_copy(cv_ref, cvin, csem.at[1])]
    for c in cin:
        c.start()
    for p in range(NBUF - 1):
        a_start(p)

    barrier = pltpu.get_barrier_semaphore()
    for k in range(1, ND):
        pl.semaphore_signal(barrier, inc=1, device_id=(frag, lax.rem(me + k, ND)), device_id_type=MESH)

    cot[...] = jnp.zeros(cot.shape, BF)
    cvt[...] = jnp.zeros(cvt.shape, BF)
    for c in cin:
        c.wait()
    cot[0:NO, 0:NQ] = coin[...]
    cvt[0:NV, 0:NQ] = cvin[...]
    cv[...] = mm_nt(one_hot(iota((128, 128), 0) == iota((128, 128), 1)), cvt[...]).astype(BF)
    xr = mm(one_hot((iota((64, 16), 0) >> 3) == iota((64, 16), 1)), cot[...]).astype(BF)
    diff = iota((128, 960), 1) - iota((128, 960), 0)
    hit = diff == 0
    for k in range(1, 8):
        hit = hit | (diff == 120 * k)
    off = iota((64, 960), 1) - 120 * (iota((64, 960), 0) & 7)
    k1[...] = jnp.where((off >= 0) & (off < 120), mm(xr, one_hot(hit)), 0.0).astype(BF)
    pi = mm(one_hot((iota((128, 16), 0) & 7) == iota((128, 16), 1)), cot[...]).astype(BF)
    for h, d in enumerate((me, sib)):
        col = iota((128, 240), 1)
        w = mm(pi, one_hot(iota((128, 240), 0) == (col >> 4) + NP * d))
        keep = (iota((128, 240), 0) >> 3) == (col & 15)
        k4c[h] = jnp.where(keep, w, 0.0).astype(BF)
    pl.semaphore_wait(barrier, ND - 1)

    def step1(p):
        slot = lax.rem(p, NBUF)
        tslot = lax.rem(p, 2)
        pad = jnp.zeros((960, 8), BF)
        for g in range(8):
            left = jnp.concatenate([abuf[slot, 1920 * g:1920 * g + 960, :], pad], axis=1)
            if g < 7:
                right = jnp.concatenate([abuf[slot, 1920 * g + 960:1920 * g + 1920, :], pad], axis=1)
                out = mm(k1[...], jnp.concatenate([left, right], axis=1))
                lo = out[:, :128].reshape(8, 8, 128)
                hi = out[:, 128:].reshape(8, 8, 128)
            else:
                lo = mm(k1[...], left).reshape(8, 8, 128)
                hi = jnp.zeros((8, 8, 128), F32)
            tbuf[tslot, :, 16 * g:16 * g + 16, :] = jnp.concatenate([lo, hi], axis=1).astype(BF)

    def step23(p):
        t = tbuf[lax.rem(p, 2)].reshape(1024, 128)
        h = mm(t, cv[...]).astype(BF).reshape(8, 128, 128)
        hoo = mm_nt(cot[...], t)
        for x in range(0, 8, 2):
            g = mm(cvt[0:112, :], jnp.concatenate([h[x], h[x + 1]], axis=1)).astype(BF)
            for y in range(2):
                sg[x // 2, y, p, 0:EX] = g[0:EX, 128 * y:128 * y + 128]
                sg[x // 2, y, p, RS0:RS0 + 112 - EX] = g[EX:, 128 * y:128 * y + 128]
        hoo = jnp.concatenate([hoo[0:8, 128 * x:128 * x + 128] for x in range(8)], axis=0).astype(BF)
        goo = mm(hoo, cv[...]).astype(BF).reshape(4, 2, 8, 128)
        for y in range(2):
            sg[:, y, p, GO:GO + 8] = goo[:, y]

    def sends(p):
        out = [pltpu.make_async_remote_copy(
            src_ref=sg.at[:, 1 - core, p, RS0:RS0 + 112 - EX], dst_ref=rs.at[:, p],
            send_sem=ssem, recv_sem=rssem, device_id=(frag, sib), device_id_type=MESH)]
        for k in range(1, ND):
            dst = lax.rem(me + k, ND)
            out.append(pltpu.make_async_remote_copy(
                src_ref=sg.at[dst // 2, lax.rem(dst, 2), p, 0:SENT], dst_ref=rg.at[me, p, 0:SENT],
                send_sem=sgsem.at[k], recv_sem=rgsem.at[me], device_id=(frag, dst), device_id_type=MESH))
        return out

    def send(p):
        for c in sends(p):
            c.start()
        rg[me, p, 0:EX] = sg[me // 2, core, p, 0:EX]
        rg[me, p, GO:GO + 8] = sg[me // 2, core, p, GO:GO + 8]

    a_wait(0)
    a_start(NBUF - 1)
    step1(0)

    def body(p, carry):
        @pl.when(p + NBUF - 1 < NP)
        def _():
            a_start(p + NBUF - 1)

        @pl.when(p >= 2)
        def _():
            send(p - 2)

        a_wait(p)
        step23(p - 1)
        step1(p)
        return carry

    lax.fori_loop(1, NP, body, 0)
    send(NP - 2)
    step23(NP - 1)
    send(NP - 1)

    def rcopy(src, dst, ss, rr, dev):
        return pltpu.make_async_remote_copy(src_ref=src, dst_ref=dst, send_sem=ss, recv_sem=rr,
                                            device_id=(frag, dev), device_id_type=MESH)

    def bwait(view, sem):
        pltpu.make_async_copy(view, view, sem).wait()

    bwait(rs, rssem)
    for u, v in ((1, 3), (2, 0)):
        for b in range(AB - NE):
            side = []
            for c in (u, v):
                own = sg[cols[c] // 2, core, :, RS0 + 16 * b:RS0 + 16 * b + 16, :].reshape(240, 128)
                oth = rs[cols[c] // 2, :, 16 * b:16 * b + 16, :].reshape(240, 128)
                side.append((own, oth))
            w = (mm(k4c[0], jnp.concatenate([side[0][0], side[1][0]], axis=1))
                 + mm(k4c[1], jnp.concatenate([side[0][1], side[1][1]], axis=1)))
            n = min(128, RSR - 128 * b)
            sb[u, 128 * b:128 * b + n, :] = w[:n, :128]
            sb[v, 128 * b:128 * b + n, :] = w[:n, 128:]

    def rows(half, c):
        return pl.ds((half * NCH + c) * CH, CH)

    first = ((1, xn, yn, 2), (2, yn, xn, 1))
    for c in range(NCH):
        for half, (col, peer, _, _) in enumerate(first):
            for m, cc in enumerate((col, 3)):
                rcopy(sb.at[cc, rows(half, c)], p1.at[m, rows(half, c)],
                      p1s.at[half, c], p1r.at[half, c], peer).start()

    for c in range(15):
        col = iota((128, 128), 1)
        w = mm(pi, one_hot(iota((128, 128), 0) == (col >> 4) + 8 * c))
        k4[:, c * 128:(c + 1) * 128] = jnp.where((iota((128, 128), 0) >> 3) == (col & 15), w, 0.0).astype(BF)
    e6[...] = one_hot((iota((128, 960), 1) >> 3) == iota((128, 960), 0))

    def v1_rows(t):
        row = iota((96, 128), 0) + 96 * t
        z = mm(one_hot((row >> 3) == iota((96, 128), 1)), cvt[...]).astype(BF)
        w = mm(z, e6[...])
        keep = (iota((96, 960), 0) & 7) == (iota((96, 960), 1) & 7)
        v1k[pl.ds(pl.multiple_of(96 * t, 96), 96), :] = jnp.where(keep, w, 0.0).astype(BF)

    def v1_build(t, carry):
        v1_rows(t)
        return carry

    lax.fori_loop(0, 9, v1_build, 0)
    for k in range(1, ND):
        src = lax.rem(me + k, ND)
        bwait(rg.at[src, :, 0:SENT], rgsem.at[src])

    v = rg[:, :, GO:GO + 8, :].reshape(960, 128)

    def v1_out(t, carry):
        w = mm(v1k[pl.ds(pl.multiple_of(96 * t, 96), 96), :], v)
        o1_ref[pl.ds(12 * t, 12)] = w.reshape(12, 8, 128)[:, :, :NV]
        return carry

    lax.fori_loop(0, 9, v1_out, 0)

    for ab in range(0, NE, 2):
        left = rg[:, :, 16 * ab:16 * ab + 16, :].reshape(1920, 128)
        right = rg[:, :, 16 * ab + 16:16 * ab + 32, :].reshape(1920, 128)
        w = mm(k4[...], jnp.concatenate([left, right], axis=1)).reshape(16, 8, 256)
        o2_ref[16 * ab:16 * ab + 16] = w[:, :, :NV]
        o2_ref[16 * ab + 16:16 * ab + 32] = w[:, :, 128:128 + NV]

    for c in range(NCH):
        for half, (_, _, peer, col) in enumerate(first):
            bwait(p1.at[:, rows(half, c)], p1r.at[half, c])
            z2[rows(half, c), :] = sb[col, rows(half, c), :] + p1[1, rows(half, c), :]
        for half, (_, _, peer, col) in enumerate(first):
            rcopy(z2.at[rows(half, c)], p2.at[rows(half, c)], p2s.at[half, c], p2r.at[half, c], peer).start()
    for c in range(NCH):
        for half in range(2):
            bwait(p2.at[rows(half, c)], p2r.at[half, c])
            w = sb[0, rows(half, c), :] + p1[0, rows(half, c), :] + p2[rows(half, c), :]
            a0 = EX + (half * NCH + c) * CH // 8
            o2_ref[a0:a0 + CH // 8] = w.reshape(CH // 8, 8, 128)[:, :, :NV]

    for k in range(1, ND):
        dst = lax.rem(me + k, ND)
        bwait(rg.at[dst, :, 0:SENT], sgsem.at[k])
    bwait(rs, ssem)
    for c in range(NCH):
        for half in range(2):
            bwait(p1.at[:, rows(half, c)], p1s.at[half, c])
            bwait(p2.at[rows(half, c)], p2s.at[half, c])


def write_out(x1_ref, x2_ref, y1_ref, y2_ref, sem):
    copies = [pltpu.make_async_copy(x1_ref, y1_ref, sem.at[0]), pltpu.make_async_copy(x2_ref, y2_ref, sem.at[1])]
    for c in copies:
        c.start()
    for c in copies:
        c.wait()


def solution(mesh):
    def local_part(ao, co, cv):
        a = ao.reshape(NP, ROWS, NQ)
        co, cv = (pltpu.with_memory_space_constraint(t.T, pltpu.HBM) for t in (co, cv))
        vm = pl.BlockSpec(memory_space=pltpu.VMEM)
        o1, o2 = pl.pallas_call(
            kernel,
            out_shape=[jax.ShapeDtypeStruct((NV, NO, NV), F32), jax.ShapeDtypeStruct((NV, NO, NV), F32)],
            in_specs=[pl.BlockSpec(memory_space=pltpu.HBM)] * 3,
            out_specs=[vm, vm],
            scratch_shapes=[
                pltpu.VMEM((NBUF, ROWS, NQ), BF),
                pltpu.VMEM((2, 8, 128, 128), BF),
                pltpu.VMEM((4, 2, NP, XR, 128), BF),
                pltpu.VMEM((8, NP, EX + 16, 128), BF),
                pltpu.VMEM((4, NP, 112 - EX, 128), BF),
                pltpu.VMEM((4, RSR, 128), F32),
                pltpu.VMEM((2, RSR, 128), F32),
                pltpu.VMEM((RSR, 128), F32),
                pltpu.VMEM((RSR, 128), F32),
                pltpu.VMEM((64, 960), BF),
                pltpu.VMEM((128, 1920), BF),
                pltpu.VMEM((2, 128, 240), BF),
                pltpu.VMEM((864, 960), BF),
                pltpu.VMEM((128, 960), BF),
                pltpu.VMEM((NO, NQ), BF),
                pltpu.VMEM((NV, NQ), BF),
                pltpu.VMEM((16, 128), BF),
                pltpu.VMEM((128, 128), BF),
                pltpu.VMEM((128, 128), BF),
                pltpu.SemaphoreType.DMA((NBUF,)),
                pltpu.SemaphoreType.DMA((2,)),
                pltpu.SemaphoreType.DMA((ND,)),
                pltpu.SemaphoreType.DMA((ND,)),
                pltpu.SemaphoreType.DMA,
                pltpu.SemaphoreType.DMA,
                pltpu.SemaphoreType.DMA((2, NCH)),
                pltpu.SemaphoreType.DMA((2, NCH)),
                pltpu.SemaphoreType.DMA((2, NCH)),
                pltpu.SemaphoreType.DMA((2, NCH)),
            ],
            compiler_params=pltpu.CompilerParams(collective_id=0, has_side_effects=True,
                                                 vmem_limit_bytes=34 * 1024 * 1024),
            name='mo_blocks',
        )(a, co, cv)
        o1, o2 = pl.pallas_call(
            write_out,
            out_shape=[jax.ShapeDtypeStruct((NV, NO, NV), F32), jax.ShapeDtypeStruct((NV, NO, NV), F32)],
            in_specs=[vm, vm],
            out_specs=[pl.BlockSpec(memory_space=pltpu.HBM)] * 2,
            scratch_shapes=[pltpu.SemaphoreType.DMA((2,))],
            compiler_params=pltpu.CompilerParams(vmem_limit_bytes=2 * 1024 * 1024),
            name='write_out',
        )(o1, o2)
        return o1.transpose(0, 2, 1), o2.transpose(1, 0, 2)

    return jax.shard_map(local_part, mesh=mesh,
                         in_specs=(P(('frag', 'dev')), P('frag'), P('frag')),
                         out_specs=(P('frag', None, 'dev'), P('frag', None, 'dev')),
                         check_vma=False)
```

```python
import jax
import jax.numpy as jnp
from jax import lax
from jax.experimental import pallas as pl
from jax.experimental.pallas import tpu as pltpu
from jax.sharding import PartitionSpec as P

MESH = pl.DeviceIdType.MESH
BF = jnp.bfloat16
F32 = jnp.float32
ND = 8
NP = 15
NQ = 120
NO = 8
NV = 108
ROWS = NQ * NQ
NBUF = 4
SPLIT = 5
AB = 7
NE = 1
EX = 16 * NE
GO = EX
SENT = EX + 8
RS0 = EX + 16
XR = 128
RSR = 8 * (NV - EX)
NCH = 2
HALF = RSR // 16 * 8
CUTS = [[0, HALF // 16 * 8, HALF], [HALF, HALF + (RSR - HALF) // 16 * 8, RSR]]


def mm(a, b):
    return jnp.dot(a, b, preferred_element_type=F32)


def mm_nt(a, b):
    return lax.dot_general(a, b, (((1,), (1,)), ((), ())), preferred_element_type=F32)


def iota(shape, dim):
    return lax.broadcasted_iota(jnp.int32, shape, dim)


def one_hot(mask):
    return jnp.where(mask, 1.0, 0.0).astype(BF)


def kernel(a_ref, co_ref, cv_ref, o1_ref, o2_ref,
           abuf, tbuf, sg, rg, rs, sb, p1, z2, p2, k1, k4, k4c, v1k, e6, coin, cvin, cot, cvt, cv,
           asem, csem, sgsem, rgsem, ssem, rssem, p1s, p1r, p2s, p2r):
    me = lax.axis_index('dev')
    frag = lax.axis_index('frag')
    core = lax.rem(me, 2)
    mx = lax.rem(me // 2, 2)
    my = me // 4
    sib = me + 1 - 2 * core
    xn = me + 2 - 4 * mx
    yn = me + 4 - 8 * my
    dg = xn + 4 - 8 * my
    cols = [me, xn, yn, dg]

    def a_copies(p):
        slot = lax.rem(p, NBUF)
        step = ROWS // SPLIT
        return [pltpu.make_async_copy(a_ref.at[p, pl.ds(k * step, step)],
                                      abuf.at[slot, pl.ds(k * step, step)],
                                      asem.at[slot]) for k in range(SPLIT)]

    def a_start(p):
        for c in a_copies(p):
            c.start()

    def a_wait(p):
        slot = lax.rem(p, NBUF)
        pltpu.make_async_copy(a_ref.at[p], abuf.at[slot], asem.at[slot]).wait()

    cin = [pltpu.make_async_copy(co_ref, coin, csem.at[0]), pltpu.make_async_copy(cv_ref, cvin, csem.at[1])]
    for c in cin:
        c.start()
    for p in range(NBUF - 1):
        a_start(p)

    barrier = pltpu.get_barrier_semaphore()
    for k in range(1, ND):
        pl.semaphore_signal(barrier, inc=1, device_id=(frag, lax.rem(me + k, ND)), device_id_type=MESH)

    cot[...] = jnp.zeros(cot.shape, BF)
    cvt[...] = jnp.zeros(cvt.shape, BF)
    for c in cin:
        c.wait()
    cot[0:NO, 0:NQ] = coin[...]
    cvt[0:NV, 0:NQ] = cvin[...]
    cv[...] = mm_nt(one_hot(iota((128, 128), 0) == iota((128, 128), 1)), cvt[...]).astype(BF)
    xr = mm(one_hot((iota((64, 16), 0) >> 3) == iota((64, 16), 1)), cot[...]).astype(BF)
    diff = iota((128, 960), 1) - iota((128, 960), 0)
    hit = diff == 0
    for k in range(1, 8):
        hit = hit | (diff == 120 * k)
    off = iota((64, 960), 1) - 120 * (iota((64, 960), 0) & 7)
    k1[...] = jnp.where((off >= 0) & (off < 120), mm(xr, one_hot(hit)), 0.0).astype(BF)
    pi = mm(one_hot((iota((128, 16), 0) & 7) == iota((128, 16), 1)), cot[...]).astype(BF)
    for h, d in enumerate((me, sib)):
        col = iota((128, 240), 1)
        w = mm(pi, one_hot(iota((128, 240), 0) == (col >> 4) + NP * d))
        keep = (iota((128, 240), 0) >> 3) == (col & 15)
        k4c[h] = jnp.where(keep, w, 0.0).astype(BF)
    pl.semaphore_wait(barrier, ND - 1)

    def step1(p):
        slot = lax.rem(p, NBUF)
        tslot = lax.rem(p, 2)
        pad = jnp.zeros((960, 8), BF)
        for g in range(8):
            left = jnp.concatenate([abuf[slot, 1920 * g:1920 * g + 960, :], pad], axis=1)
            if g < 7:
                right = jnp.concatenate([abuf[slot, 1920 * g + 960:1920 * g + 1920, :], pad], axis=1)
                out = mm(k1[...], jnp.concatenate([left, right], axis=1))
                lo = out[:, :128].reshape(8, 8, 128)
                hi = out[:, 128:].reshape(8, 8, 128)
            else:
                lo = mm(k1[...], left).reshape(8, 8, 128)
                hi = jnp.zeros((8, 8, 128), F32)
            tbuf[tslot, :, 16 * g:16 * g + 16, :] = jnp.concatenate([lo, hi], axis=1).astype(BF)

    def step23(p):
        t = tbuf[lax.rem(p, 2)].reshape(1024, 128)
        h = mm(t, cv[...]).astype(BF).reshape(8, 128, 128)
        hoo = mm_nt(cot[...], t)
        for x in range(0, 8, 2):
            g = mm(cvt[0:112, :], jnp.concatenate([h[x], h[x + 1]], axis=1)).astype(BF)
            for y in range(2):
                sg[x // 2, y, p, 0:EX] = g[0:EX, 128 * y:128 * y + 128]
                sg[x // 2, y, p, RS0:RS0 + 112 - EX] = g[EX:, 128 * y:128 * y + 128]
        hoo = jnp.concatenate([hoo[0:8, 128 * x:128 * x + 128] for x in range(8)], axis=0).astype(BF)
        goo = mm(hoo, cv[...]).astype(BF).reshape(4, 2, 8, 128)
        for y in range(2):
            sg[:, y, p, GO:GO + 8] = goo[:, y]

    def sends(p):
        out = [pltpu.make_async_remote_copy(
            src_ref=sg.at[:, 1 - core, p, RS0:RS0 + 112 - EX], dst_ref=rs.at[:, p],
            send_sem=ssem, recv_sem=rssem, device_id=(frag, sib), device_id_type=MESH)]
        for k in range(1, ND):
            dst = lax.rem(me + k, ND)
            out.append(pltpu.make_async_remote_copy(
                src_ref=sg.at[dst // 2, lax.rem(dst, 2), p, 0:SENT], dst_ref=rg.at[me, p, 0:SENT],
                send_sem=sgsem.at[k], recv_sem=rgsem.at[me], device_id=(frag, dst), device_id_type=MESH))
        return out

    def send(p):
        for c in sends(p):
            c.start()
        rg[me, p, 0:EX] = sg[me // 2, core, p, 0:EX]
        rg[me, p, GO:GO + 8] = sg[me // 2, core, p, GO:GO + 8]

    a_wait(0)
    a_start(NBUF - 1)
    step1(0)

    def body(p, carry):
        @pl.when(p + NBUF - 1 < NP)
        def _():
            a_start(p + NBUF - 1)

        @pl.when(p >= 2)
        def _():
            send(p - 2)

        a_wait(p)
        step23(p - 1)
        step1(p)
        return carry

    lax.fori_loop(1, NP, body, 0)
    send(NP - 2)
    step23(NP - 1)
    send(NP - 1)

    def rcopy(src, dst, ss, rr, dev):
        return pltpu.make_async_remote_copy(src_ref=src, dst_ref=dst, send_sem=ss, recv_sem=rr,
                                            device_id=(frag, dev), device_id_type=MESH)

    def bwait(view, sem):
        pltpu.make_async_copy(view, view, sem).wait()

    bwait(rs, rssem)
    for u, v in ((1, 3), (2, 0)):
        for b in range(AB - NE):
            side = []
            for c in (u, v):
                own = sg[cols[c] // 2, core, :, RS0 + 16 * b:RS0 + 16 * b + 16, :].reshape(240, 128)
                oth = rs[cols[c] // 2, :, 16 * b:16 * b + 16, :].reshape(240, 128)
                side.append((own, oth))
            w = (mm(k4c[0], jnp.concatenate([side[0][0], side[1][0]], axis=1))
                 + mm(k4c[1], jnp.concatenate([side[0][1], side[1][1]], axis=1)))
            n = min(128, RSR - 128 * b)
            sb[u, 128 * b:128 * b + n, :] = w[:n, :128]
            sb[v, 128 * b:128 * b + n, :] = w[:n, 128:]

    def rows(half, c):
        return slice(CUTS[half][c], CUTS[half][c + 1])

    first = ((1, xn, yn, 2), (2, yn, xn, 1))
    for c in range(NCH):
        for half, (col, peer, _, _) in enumerate(first):
            for m, cc in enumerate((col, 3)):
                rcopy(sb.at[cc, rows(half, c)], p1.at[m, rows(half, c)],
                      p1s.at[half, c], p1r.at[half, c], peer).start()

    for c in range(15):
        col = iota((128, 128), 1)
        w = mm(pi, one_hot(iota((128, 128), 0) == (col >> 4) + 8 * c))
        k4[:, c * 128:(c + 1) * 128] = jnp.where((iota((128, 128), 0) >> 3) == (col & 15), w, 0.0).astype(BF)
    e6[...] = one_hot((iota((128, 960), 1) >> 3) == iota((128, 960), 0))

    def v1_rows(t):
        row = iota((96, 128), 0) + 96 * t
        z = mm(one_hot((row >> 3) == iota((96, 128), 1)), cvt[...]).astype(BF)
        w = mm(z, e6[...])
        keep = (iota((96, 960), 0) & 7) == (iota((96, 960), 1) & 7)
        v1k[pl.ds(pl.multiple_of(96 * t, 96), 96), :] = jnp.where(keep, w, 0.0).astype(BF)

    def v1_build(t, carry):
        v1_rows(t)
        return carry

    lax.fori_loop(0, 9, v1_build, 0)
    for k in range(1, ND):
        src = lax.rem(me + k, ND)
        bwait(rg.at[src, :, 0:SENT], rgsem.at[src])

    v = rg[:, :, GO:GO + 8, :].reshape(960, 128)

    def v1_out(t, carry):
        w = mm(v1k[pl.ds(pl.multiple_of(96 * t, 96), 96), :], v)
        o1_ref[pl.ds(12 * t, 12)] = w.reshape(12, 8, 128)[:, :, :NV]
        return carry

    lax.fori_loop(0, 9, v1_out, 0)

    for ab in range(0, NE, 2):
        n = min(2, NE - ab)
        w = mm(k4[...], jnp.concatenate([rg[:, :, 16 * (ab + u):16 * (ab + u) + 16, :].reshape(1920, 128)
                                         for u in range(n)], axis=1)).reshape(16, 8, 128 * n)
        for u in range(n):
            o2_ref[16 * (ab + u):16 * (ab + u) + 16] = w[:, :, 128 * u:128 * u + NV]

    for c in range(NCH):
        for half, (_, _, peer, col) in enumerate(first):
            bwait(p1.at[:, rows(half, c)], p1r.at[half, c])
            z2[rows(half, c), :] = sb[col, rows(half, c), :] + p1[1, rows(half, c), :]
        for half, (_, _, peer, col) in enumerate(first):
            rcopy(z2.at[rows(half, c)], p2.at[rows(half, c)], p2s.at[half, c], p2r.at[half, c], peer).start()
    for c in range(NCH):
        for half in range(2):
            bwait(p2.at[rows(half, c)], p2r.at[half, c])
            w = sb[0, rows(half, c), :] + p1[0, rows(half, c), :] + p2[rows(half, c), :]
            a0, a1 = EX + CUTS[half][c] // 8, EX + CUTS[half][c + 1] // 8
            o2_ref[a0:a1] = w.reshape(a1 - a0, 8, 128)[:, :, :NV]

    for k in range(1, ND):
        dst = lax.rem(me + k, ND)
        bwait(rg.at[dst, :, 0:SENT], sgsem.at[k])
    bwait(rs, ssem)
    for c in range(NCH):
        for half in range(2):
            bwait(p1.at[:, rows(half, c)], p1s.at[half, c])
            bwait(p2.at[rows(half, c)], p2s.at[half, c])


def write_out(x1_ref, x2_ref, y1_ref, y2_ref, sem):
    copies = [pltpu.make_async_copy(x1_ref, y1_ref, sem.at[0]), pltpu.make_async_copy(x2_ref, y2_ref, sem.at[1])]
    for c in copies:
        c.start()
    for c in copies:
        c.wait()


def solution(mesh):
    def local_part(ao, co, cv):
        a = ao.reshape(NP, ROWS, NQ)
        co, cv = (pltpu.with_memory_space_constraint(t.T, pltpu.HBM) for t in (co, cv))
        vm = pl.BlockSpec(memory_space=pltpu.VMEM)
        o1, o2 = pl.pallas_call(
            kernel,
            out_shape=[jax.ShapeDtypeStruct((NV, NO, NV), F32), jax.ShapeDtypeStruct((NV, NO, NV), F32)],
            in_specs=[pl.BlockSpec(memory_space=pltpu.HBM)] * 3,
            out_specs=[vm, vm],
            scratch_shapes=[
                pltpu.VMEM((NBUF, ROWS, NQ), BF),
                pltpu.VMEM((2, 8, 128, 128), BF),
                pltpu.VMEM((4, 2, NP, XR, 128), BF),
                pltpu.VMEM((8, NP, EX + 16, 128), BF),
                pltpu.VMEM((4, NP, 112 - EX, 128), BF),
                pltpu.VMEM((4, RSR, 128), F32),
                pltpu.VMEM((2, RSR, 128), F32),
                pltpu.VMEM((RSR, 128), F32),
                pltpu.VMEM((RSR, 128), F32),
                pltpu.VMEM((64, 960), BF),
                pltpu.VMEM((128, 1920), BF),
                pltpu.VMEM((2, 128, 240), BF),
                pltpu.VMEM((864, 960), BF),
                pltpu.VMEM((128, 960), BF),
                pltpu.VMEM((NO, NQ), BF),
                pltpu.VMEM((NV, NQ), BF),
                pltpu.VMEM((16, 128), BF),
                pltpu.VMEM((128, 128), BF),
                pltpu.VMEM((128, 128), BF),
                pltpu.SemaphoreType.DMA((NBUF,)),
                pltpu.SemaphoreType.DMA((2,)),
                pltpu.SemaphoreType.DMA((ND,)),
                pltpu.SemaphoreType.DMA((ND,)),
                pltpu.SemaphoreType.DMA,
                pltpu.SemaphoreType.DMA,
                pltpu.SemaphoreType.DMA((2, NCH)),
                pltpu.SemaphoreType.DMA((2, NCH)),
                pltpu.SemaphoreType.DMA((2, NCH)),
                pltpu.SemaphoreType.DMA((2, NCH)),
            ],
            compiler_params=pltpu.CompilerParams(collective_id=0, has_side_effects=True,
                                                 vmem_limit_bytes=34 * 1024 * 1024),
            name='mo_blocks',
        )(a, co, cv)
        o1, o2 = pl.pallas_call(
            write_out,
            out_shape=[jax.ShapeDtypeStruct((NV, NO, NV), F32), jax.ShapeDtypeStruct((NV, NO, NV), F32)],
            in_specs=[vm, vm],
            out_specs=[pl.BlockSpec(memory_space=pltpu.HBM)] * 2,
            scratch_shapes=[pltpu.SemaphoreType.DMA((2,))],
            compiler_params=pltpu.CompilerParams(vmem_limit_bytes=2 * 1024 * 1024),
            name='write_out',
        )(o1, o2)
        return o1.transpose(0, 2, 1), o2.transpose(1, 0, 2)

    return jax.shard_map(local_part, mesh=mesh,
                         in_specs=(P(('frag', 'dev')), P('frag'), P('frag')),
                         out_specs=(P('frag', None, 'dev'), P('frag', None, 'dev')),
                         check_vma=False)
```

```python
import jax
import jax.numpy as jnp
from jax import lax
from jax.experimental import pallas as pl
from jax.experimental.pallas import tpu as pltpu
from jax.sharding import PartitionSpec as P

MESH = pl.DeviceIdType.MESH
BF = jnp.bfloat16
F32 = jnp.float32
ND = 8
NP = 15
NQ = 120
NO = 8
NV = 108
ROWS = NQ * NQ
NBUF = 4
SPLIT = 5
AB = 7
NE = 3
EX = 16 * NE
GO = EX
SENT = EX + 8
RS0 = EX + 16
XR = 128
RSR = 8 * (NV - EX)
NCH = 2
HALF = RSR // 16 * 8
CUTS = [[0, HALF // 16 * 8, HALF], [HALF, HALF + (RSR - HALF) // 16 * 8, RSR]]


def mm(a, b):
    return jnp.dot(a, b, preferred_element_type=F32)


def mm_nt(a, b):
    return lax.dot_general(a, b, (((1,), (1,)), ((), ())), preferred_element_type=F32)


def iota(shape, dim):
    return lax.broadcasted_iota(jnp.int32, shape, dim)


def one_hot(mask):
    return jnp.where(mask, 1.0, 0.0).astype(BF)


def kernel(a_ref, co_ref, cv_ref, o1_ref, o2_ref,
           abuf, tbuf, sg, rg, rs, sb, p1, z2, p2, k1, k4, k4c, v1k, e6, coin, cvin, cot, cvt, cv,
           asem, csem, sgsem, rgsem, ssem, rssem, p1s, p1r, p2s, p2r):
    me = lax.axis_index('dev')
    frag = lax.axis_index('frag')
    core = lax.rem(me, 2)
    mx = lax.rem(me // 2, 2)
    my = me // 4
    sib = me + 1 - 2 * core
    xn = me + 2 - 4 * mx
    yn = me + 4 - 8 * my
    dg = xn + 4 - 8 * my
    cols = [me, xn, yn, dg]

    def a_copies(p):
        slot = lax.rem(p, NBUF)
        step = ROWS // SPLIT
        return [pltpu.make_async_copy(a_ref.at[p, pl.ds(k * step, step)],
                                      abuf.at[slot, pl.ds(k * step, step)],
                                      asem.at[slot]) for k in range(SPLIT)]

    def a_start(p):
        for c in a_copies(p):
            c.start()

    def a_wait(p):
        slot = lax.rem(p, NBUF)
        pltpu.make_async_copy(a_ref.at[p], abuf.at[slot], asem.at[slot]).wait()

    cin = [pltpu.make_async_copy(co_ref, coin, csem.at[0]), pltpu.make_async_copy(cv_ref, cvin, csem.at[1])]
    for c in cin:
        c.start()
    for p in range(NBUF - 1):
        a_start(p)

    barrier = pltpu.get_barrier_semaphore()
    for k in range(1, ND):
        pl.semaphore_signal(barrier, inc=1, device_id=(frag, lax.rem(me + k, ND)), device_id_type=MESH)

    cot[...] = jnp.zeros(cot.shape, BF)
    cvt[...] = jnp.zeros(cvt.shape, BF)
    for c in cin:
        c.wait()
    cot[0:NO, 0:NQ] = coin[...]
    cvt[0:NV, 0:NQ] = cvin[...]
    cv[...] = mm_nt(one_hot(iota((128, 128), 0) == iota((128, 128), 1)), cvt[...]).astype(BF)
    xr = mm(one_hot((iota((64, 16), 0) >> 3) == iota((64, 16), 1)), cot[...]).astype(BF)
    diff = iota((128, 960), 1) - iota((128, 960), 0)
    hit = diff == 0
    for k in range(1, 8):
        hit = hit | (diff == 120 * k)
    off = iota((64, 960), 1) - 120 * (iota((64, 960), 0) & 7)
    k1[...] = jnp.where((off >= 0) & (off < 120), mm(xr, one_hot(hit)), 0.0).astype(BF)
    pi = mm(one_hot((iota((128, 16), 0) & 7) == iota((128, 16), 1)), cot[...]).astype(BF)
    for h, d in enumerate((me, sib)):
        col = iota((128, 240), 1)
        w = mm(pi, one_hot(iota((128, 240), 0) == (col >> 4) + NP * d))
        keep = (iota((128, 240), 0) >> 3) == (col & 15)
        k4c[h] = jnp.where(keep, w, 0.0).astype(BF)
    pl.semaphore_wait(barrier, ND - 1)

    def step1(p):
        slot = lax.rem(p, NBUF)
        tslot = lax.rem(p, 2)
        pad = jnp.zeros((960, 8), BF)
        for g in range(8):
            left = jnp.concatenate([abuf[slot, 1920 * g:1920 * g + 960, :], pad], axis=1)
            if g < 7:
                right = jnp.concatenate([abuf[slot, 1920 * g + 960:1920 * g + 1920, :], pad], axis=1)
                out = mm(k1[...], jnp.concatenate([left, right], axis=1))
                lo = out[:, :128].reshape(8, 8, 128)
                hi = out[:, 128:].reshape(8, 8, 128)
            else:
                lo = mm(k1[...], left).reshape(8, 8, 128)
                hi = jnp.zeros((8, 8, 128), F32)
            tbuf[tslot, :, 16 * g:16 * g + 16, :] = jnp.concatenate([lo, hi], axis=1).astype(BF)

    def step23(p):
        t = tbuf[lax.rem(p, 2)].reshape(1024, 128)
        h = mm(t, cv[...]).astype(BF).reshape(8, 128, 128)
        hoo = mm_nt(cot[...], t)
        for x in range(0, 8, 2):
            g = mm(cvt[0:112, :], jnp.concatenate([h[x], h[x + 1]], axis=1)).astype(BF)
            for y in range(2):
                sg[x // 2, y, p, 0:EX] = g[0:EX, 128 * y:128 * y + 128]
                sg[x // 2, y, p, RS0:RS0 + 112 - EX] = g[EX:, 128 * y:128 * y + 128]
        hoo = jnp.concatenate([hoo[0:8, 128 * x:128 * x + 128] for x in range(8)], axis=0).astype(BF)
        goo = mm(hoo, cv[...]).astype(BF).reshape(4, 2, 8, 128)
        for y in range(2):
            sg[:, y, p, GO:GO + 8] = goo[:, y]

    def sends(p):
        out = [pltpu.make_async_remote_copy(
            src_ref=sg.at[:, 1 - core, p, RS0:RS0 + 112 - EX], dst_ref=rs.at[:, p],
            send_sem=ssem, recv_sem=rssem, device_id=(frag, sib), device_id_type=MESH)]
        for k in range(1, ND):
            dst = lax.rem(me + k, ND)
            out.append(pltpu.make_async_remote_copy(
                src_ref=sg.at[dst // 2, lax.rem(dst, 2), p, 0:SENT], dst_ref=rg.at[me, p, 0:SENT],
                send_sem=sgsem.at[k], recv_sem=rgsem.at[me], device_id=(frag, dst), device_id_type=MESH))
        return out

    def send(p):
        for c in sends(p):
            c.start()
        rg[me, p, 0:EX] = sg[me // 2, core, p, 0:EX]
        rg[me, p, GO:GO + 8] = sg[me // 2, core, p, GO:GO + 8]

    a_wait(0)
    a_start(NBUF - 1)
    step1(0)

    def body(p, carry):
        @pl.when(p + NBUF - 1 < NP)
        def _():
            a_start(p + NBUF - 1)

        @pl.when(p >= 2)
        def _():
            send(p - 2)

        a_wait(p)
        step23(p - 1)
        step1(p)
        return carry

    lax.fori_loop(1, NP, body, 0)
    send(NP - 2)
    step23(NP - 1)
    send(NP - 1)

    def rcopy(src, dst, ss, rr, dev):
        return pltpu.make_async_remote_copy(src_ref=src, dst_ref=dst, send_sem=ss, recv_sem=rr,
                                            device_id=(frag, dev), device_id_type=MESH)

    def bwait(view, sem):
        pltpu.make_async_copy(view, view, sem).wait()

    bwait(rs, rssem)
    for u, v in ((1, 3), (2, 0)):
        for b in range(AB - NE):
            side = []
            for c in (u, v):
                own = sg[cols[c] // 2, core, :, RS0 + 16 * b:RS0 + 16 * b + 16, :].reshape(240, 128)
                oth = rs[cols[c] // 2, :, 16 * b:16 * b + 16, :].reshape(240, 128)
                side.append((own, oth))
            w = (mm(k4c[0], jnp.concatenate([side[0][0], side[1][0]], axis=1))
                 + mm(k4c[1], jnp.concatenate([side[0][1], side[1][1]], axis=1)))
            n = min(128, RSR - 128 * b)
            sb[u, 128 * b:128 * b + n, :] = w[:n, :128]
            sb[v, 128 * b:128 * b + n, :] = w[:n, 128:]

    def rows(half, c):
        return slice(CUTS[half][c], CUTS[half][c + 1])

    first = ((1, xn, yn, 2), (2, yn, xn, 1))
    for c in range(NCH):
        for half, (col, peer, _, _) in enumerate(first):
            for m, cc in enumerate((col, 3)):
                rcopy(sb.at[cc, rows(half, c)], p1.at[m, rows(half, c)],
                      p1s.at[half, c], p1r.at[half, c], peer).start()

    for c in range(15):
        col = iota((128, 128), 1)
        w = mm(pi, one_hot(iota((128, 128), 0) == (col >> 4) + 8 * c))
        k4[:, c * 128:(c + 1) * 128] = jnp.where((iota((128, 128), 0) >> 3) == (col & 15), w, 0.0).astype(BF)
    e6[...] = one_hot((iota((128, 960), 1) >> 3) == iota((128, 960), 0))

    def v1_rows(t):
        row = iota((96, 128), 0) + 96 * t
        z = mm(one_hot((row >> 3) == iota((96, 128), 1)), cvt[...]).astype(BF)
        w = mm(z, e6[...])
        keep = (iota((96, 960), 0) & 7) == (iota((96, 960), 1) & 7)
        v1k[pl.ds(pl.multiple_of(96 * t, 96), 96), :] = jnp.where(keep, w, 0.0).astype(BF)

    def v1_build(t, carry):
        v1_rows(t)
        return carry

    lax.fori_loop(0, 9, v1_build, 0)
    for k in range(1, ND):
        src = lax.rem(me + k, ND)
        bwait(rg.at[src, :, 0:SENT], rgsem.at[src])

    v = rg[:, :, GO:GO + 8, :].reshape(960, 128)

    def v1_out(t, carry):
        w = mm(v1k[pl.ds(pl.multiple_of(96 * t, 96), 96), :], v)
        o1_ref[pl.ds(12 * t, 12)] = w.reshape(12, 8, 128)[:, :, :NV]
        return carry

    lax.fori_loop(0, 9, v1_out, 0)

    for ab in range(0, NE, 2):
        n = min(2, NE - ab)
        w = mm(k4[...], jnp.concatenate([rg[:, :, 16 * (ab + u):16 * (ab + u) + 16, :].reshape(1920, 128)
                                         for u in range(n)], axis=1)).reshape(16, 8, 128 * n)
        for u in range(n):
            o2_ref[16 * (ab + u):16 * (ab + u) + 16] = w[:, :, 128 * u:128 * u + NV]

    for c in range(NCH):
        for half, (_, _, peer, col) in enumerate(first):
            bwait(p1.at[:, rows(half, c)], p1r.at[half, c])
            z2[rows(half, c), :] = sb[col, rows(half, c), :] + p1[1, rows(half, c), :]
        for half, (_, _, peer, col) in enumerate(first):
            rcopy(z2.at[rows(half, c)], p2.at[rows(half, c)], p2s.at[half, c], p2r.at[half, c], peer).start()
    for c in range(NCH):
        for half in range(2):
            bwait(p2.at[rows(half, c)], p2r.at[half, c])
            w = sb[0, rows(half, c), :] + p1[0, rows(half, c), :] + p2[rows(half, c), :]
            a0, a1 = EX + CUTS[half][c] // 8, EX + CUTS[half][c + 1] // 8
            o2_ref[a0:a1] = w.reshape(a1 - a0, 8, 128)[:, :, :NV]

    for k in range(1, ND):
        dst = lax.rem(me + k, ND)
        bwait(rg.at[dst, :, 0:SENT], sgsem.at[k])
    bwait(rs, ssem)
    for c in range(NCH):
        for half in range(2):
            bwait(p1.at[:, rows(half, c)], p1s.at[half, c])
            bwait(p2.at[rows(half, c)], p2s.at[half, c])


def write_out(x1_ref, x2_ref, y1_ref, y2_ref, sem):
    copies = [pltpu.make_async_copy(x1_ref, y1_ref, sem.at[0]), pltpu.make_async_copy(x2_ref, y2_ref, sem.at[1])]
    for c in copies:
        c.start()
    for c in copies:
        c.wait()


def solution(mesh):
    def local_part(ao, co, cv):
        a = ao.reshape(NP, ROWS, NQ)
        co, cv = (pltpu.with_memory_space_constraint(t.T, pltpu.HBM) for t in (co, cv))
        vm = pl.BlockSpec(memory_space=pltpu.VMEM)
        o1, o2 = pl.pallas_call(
            kernel,
            out_shape=[jax.ShapeDtypeStruct((NV, NO, NV), F32), jax.ShapeDtypeStruct((NV, NO, NV), F32)],
            in_specs=[pl.BlockSpec(memory_space=pltpu.HBM)] * 3,
            out_specs=[vm, vm],
            scratch_shapes=[
                pltpu.VMEM((NBUF, ROWS, NQ), BF),
                pltpu.VMEM((2, 8, 128, 128), BF),
                pltpu.VMEM((4, 2, NP, XR, 128), BF),
                pltpu.VMEM((8, NP, EX + 16, 128), BF),
                pltpu.VMEM((4, NP, 112 - EX, 128), BF),
                pltpu.VMEM((4, RSR, 128), F32),
                pltpu.VMEM((2, RSR, 128), F32),
                pltpu.VMEM((RSR, 128), F32),
                pltpu.VMEM((RSR, 128), F32),
                pltpu.VMEM((64, 960), BF),
                pltpu.VMEM((128, 1920), BF),
                pltpu.VMEM((2, 128, 240), BF),
                pltpu.VMEM((864, 960), BF),
                pltpu.VMEM((128, 960), BF),
                pltpu.VMEM((NO, NQ), BF),
                pltpu.VMEM((NV, NQ), BF),
                pltpu.VMEM((16, 128), BF),
                pltpu.VMEM((128, 128), BF),
                pltpu.VMEM((128, 128), BF),
                pltpu.SemaphoreType.DMA((NBUF,)),
                pltpu.SemaphoreType.DMA((2,)),
                pltpu.SemaphoreType.DMA((ND,)),
                pltpu.SemaphoreType.DMA((ND,)),
                pltpu.SemaphoreType.DMA,
                pltpu.SemaphoreType.DMA,
                pltpu.SemaphoreType.DMA((2, NCH)),
                pltpu.SemaphoreType.DMA((2, NCH)),
                pltpu.SemaphoreType.DMA((2, NCH)),
                pltpu.SemaphoreType.DMA((2, NCH)),
            ],
            compiler_params=pltpu.CompilerParams(collective_id=0, has_side_effects=True,
                                                 vmem_limit_bytes=34 * 1024 * 1024),
            name='mo_blocks',
        )(a, co, cv)
        o1, o2 = pl.pallas_call(
            write_out,
            out_shape=[jax.ShapeDtypeStruct((NV, NO, NV), F32), jax.ShapeDtypeStruct((NV, NO, NV), F32)],
            in_specs=[vm, vm],
            out_specs=[pl.BlockSpec(memory_space=pltpu.HBM)] * 2,
            scratch_shapes=[pltpu.SemaphoreType.DMA((2,))],
            compiler_params=pltpu.CompilerParams(vmem_limit_bytes=2 * 1024 * 1024),
            name='write_out',
        )(o1, o2)
        return o1.transpose(0, 2, 1), o2.transpose(1, 0, 2)

    return jax.shard_map(local_part, mesh=mesh,
                         in_specs=(P(('frag', 'dev')), P('frag'), P('frag')),
                         out_specs=(P('frag', None, 'dev'), P('frag', None, 'dev')),
                         check_vma=False)
```

```python
import jax
import jax.numpy as jnp
from jax import lax
from jax.experimental import pallas as pl
from jax.experimental.pallas import tpu as pltpu
from jax.sharding import PartitionSpec as P

MESH = pl.DeviceIdType.MESH
BF = jnp.bfloat16
F32 = jnp.float32
ND = 8
NP = 15
NQ = 120
NO = 8
NV = 108
ROWS = NQ * NQ
NBUF = 4
SPLIT = 5
VB = 6
GR = 16 * VB
GC = 20
NE = 2
EX = 16 * NE
GO = EX
SENT = EX + 8
RS0 = EX + 16
RS1 = RS0 + GR - EX
RSR = 8 * (GR - EX)
NCH = 2
HALF = RSR // 16 * 8
CUTS = [[0, HALF // 16 * 8, HALF], [HALF, HALF + (RSR - HALF) // 16 * 8, RSR]]


def mm(a, b):
    return jnp.dot(a, b, preferred_element_type=F32)


def mm_nt(a, b):
    return lax.dot_general(a, b, (((1,), (1,)), ((), ())), preferred_element_type=F32)


def iota(shape, dim):
    return lax.broadcasted_iota(jnp.int32, shape, dim)


def one_hot(mask):
    return jnp.where(mask, 1.0, 0.0).astype(BF)


def kernel(a_ref, co_ref, cv_ref, o1_ref, o2_ref,
           abuf, tbuf, sg, rg, rs, sb, p1, z2, p2, k1, k4, k4c, v1k, e6, coin, cvin, cot, cvt, cv,
           asem, csem, sgsem, rgsem, ssem, rssem, p1s, p1r, p2s, p2r):
    me = lax.axis_index('dev')
    frag = lax.axis_index('frag')
    core = lax.rem(me, 2)
    mx = lax.rem(me // 2, 2)
    my = me // 4
    sib = me + 1 - 2 * core
    xn = me + 2 - 4 * mx
    yn = me + 4 - 8 * my
    dg = xn + 4 - 8 * my
    cols = [me, xn, yn, dg]

    def a_copies(p):
        slot = lax.rem(p, NBUF)
        step = ROWS // SPLIT
        return [pltpu.make_async_copy(a_ref.at[p, pl.ds(k * step, step)],
                                      abuf.at[slot, pl.ds(k * step, step)],
                                      asem.at[slot]) for k in range(SPLIT)]

    def a_start(p):
        for c in a_copies(p):
            c.start()

    def a_wait(p):
        slot = lax.rem(p, NBUF)
        pltpu.make_async_copy(a_ref.at[p], abuf.at[slot], asem.at[slot]).wait()

    cin = [pltpu.make_async_copy(co_ref, coin, csem.at[0]), pltpu.make_async_copy(cv_ref, cvin, csem.at[1])]
    for c in cin:
        c.start()
    for p in range(NBUF - 1):
        a_start(p)

    barrier = pltpu.get_barrier_semaphore()
    for k in range(1, ND):
        pl.semaphore_signal(barrier, inc=1, device_id=(frag, lax.rem(me + k, ND)), device_id_type=MESH)

    cot[...] = jnp.zeros(cot.shape, BF)
    cvt[...] = jnp.zeros(cvt.shape, BF)
    for c in cin:
        c.wait()
    cot[0:NO, 0:NQ] = coin[...]
    cvt[0:NV, 0:NQ] = cvin[...]
    cv[...] = mm_nt(one_hot(iota((128, 128), 0) == iota((128, 128), 1)), cvt[...]).astype(BF)
    xr = mm(one_hot((iota((64, 16), 0) >> 3) == iota((64, 16), 1)), cot[...]).astype(BF)
    diff = iota((128, 960), 1) - iota((128, 960), 0)
    hit = diff == 0
    for k in range(1, 8):
        hit = hit | (diff == 120 * k)
    off = iota((64, 960), 1) - 120 * (iota((64, 960), 0) & 7)
    k1[...] = jnp.where((off >= 0) & (off < 120), mm(xr, one_hot(hit)), 0.0).astype(BF)
    pi = mm(one_hot((iota((128, 16), 0) & 7) == iota((128, 16), 1)), cot[...]).astype(BF)
    for h, d in enumerate((me, sib)):
        col = iota((128, 240), 1)
        w = mm(pi, one_hot(iota((128, 240), 0) == (col >> 4) + NP * d))
        keep = (iota((128, 240), 0) >> 3) == (col & 15)
        k4c[h] = jnp.where(keep, w, 0.0).astype(BF)
    pl.semaphore_wait(barrier, ND - 1)

    def step1(p):
        slot = lax.rem(p, NBUF)
        tslot = lax.rem(p, 2)
        pad = jnp.zeros((960, 8), BF)
        for g in range(8):
            left = jnp.concatenate([abuf[slot, 1920 * g:1920 * g + 960, :], pad], axis=1)
            if g < 7:
                right = jnp.concatenate([abuf[slot, 1920 * g + 960:1920 * g + 1920, :], pad], axis=1)
                out = mm(k1[...], jnp.concatenate([left, right], axis=1))
                lo = out[:, :128].reshape(8, 8, 128)
                hi = out[:, 128:].reshape(8, 8, 128)
            else:
                lo = mm(k1[...], left).reshape(8, 8, 128)
                hi = jnp.zeros((8, 8, 128), F32)
            tbuf[tslot, :, 16 * g:16 * g + 16, :] = jnp.concatenate([lo, hi], axis=1).astype(BF)

    def step23(p):
        t = tbuf[lax.rem(p, 2)].reshape(1024, 128)
        h = mm(t, cv[...]).astype(BF).reshape(8, 128, 128)
        hoo = mm_nt(cot[...], t)
        lane = iota((16, 128), 1)
        for x in range(0, 8, 2):
            g = mm(cvt[0:112, :], jnp.concatenate([h[x], h[x + 1]], axis=1))
            for y in range(2):
                last = g[GR:GR + 16, 128 * y:128 * y + 128]
                tiles = [jnp.where(lane < NV, g[16 * k:16 * k + 16, 128 * y:128 * y + 128],
                                   pltpu.roll(last, (NV - GC * k) % 128, 1)) for k in range(VB)]
                sg[x // 2, y, p, 0:EX] = jnp.concatenate(tiles[:NE], axis=0).astype(BF)
                sg[x // 2, y, p, RS0:RS1] = jnp.concatenate(tiles[NE:], axis=0).astype(BF)
        hoo = jnp.concatenate([hoo[0:8, 128 * x:128 * x + 128] for x in range(8)], axis=0).astype(BF)
        goo = mm(hoo, cv[...]).astype(BF).reshape(4, 2, 8, 128)
        for y in range(2):
            sg[:, y, p, GO:GO + 8] = goo[:, y]

    def sends(p):
        out = [pltpu.make_async_remote_copy(
            src_ref=sg.at[:, 1 - core, p, RS0:RS1], dst_ref=rs.at[:, p],
            send_sem=ssem, recv_sem=rssem, device_id=(frag, sib), device_id_type=MESH)]
        for k in range(1, ND):
            dst = lax.rem(me + k, ND)
            out.append(pltpu.make_async_remote_copy(
                src_ref=sg.at[dst // 2, lax.rem(dst, 2), p, 0:SENT], dst_ref=rg.at[me, p, 0:SENT],
                send_sem=sgsem.at[k], recv_sem=rgsem.at[me], device_id=(frag, dst), device_id_type=MESH))
        return out

    def send(p):
        for c in sends(p):
            c.start()
        rg[me, p, 0:EX] = sg[me // 2, core, p, 0:EX]
        rg[me, p, GO:GO + 8] = sg[me // 2, core, p, GO:GO + 8]

    a_wait(0)
    a_start(NBUF - 1)
    step1(0)

    def body(p, carry):
        @pl.when(p + NBUF - 1 < NP)
        def _():
            a_start(p + NBUF - 1)

        @pl.when(p >= 2)
        def _():
            send(p - 2)

        a_wait(p)
        step23(p - 1)
        step1(p)
        return carry

    lax.fori_loop(1, NP, body, 0)
    send(NP - 2)
    step23(NP - 1)
    send(NP - 1)

    def rcopy(src, dst, ss, rr, dev):
        return pltpu.make_async_remote_copy(src_ref=src, dst_ref=dst, send_sem=ss, recv_sem=rr,
                                            device_id=(frag, dev), device_id_type=MESH)

    def bwait(view, sem):
        pltpu.make_async_copy(view, view, sem).wait()

    bwait(rs, rssem)
    for u, v in ((1, 3), (2, 0)):
        for b in range(VB - NE):
            side = []
            for c in (u, v):
                own = sg[cols[c] // 2, core, :, RS0 + 16 * b:RS0 + 16 * b + 16, :].reshape(240, 128)
                oth = rs[cols[c] // 2, :, 16 * b:16 * b + 16, :].reshape(240, 128)
                side.append((own, oth))
            w = (mm(k4c[0], jnp.concatenate([side[0][0], side[1][0]], axis=1))
                 + mm(k4c[1], jnp.concatenate([side[0][1], side[1][1]], axis=1)))
            sb[u, 128 * b:128 * b + 128, :] = w[:, :128]
            sb[v, 128 * b:128 * b + 128, :] = w[:, 128:]

    def rows(half, c):
        return slice(CUTS[half][c], CUTS[half][c + 1])

    first = ((1, xn, yn, 2), (2, yn, xn, 1))
    for c in range(NCH):
        for half, (col, peer, _, _) in enumerate(first):
            for m, cc in enumerate((col, 3)):
                rcopy(sb.at[cc, rows(half, c)], p1.at[m, rows(half, c)],
                      p1s.at[half, c], p1r.at[half, c], peer).start()

    def put(w, a0):
        o2_ref[a0:a0 + w.shape[0]] = w[:, :, :NV]
        for k in range(VB):
            lo, hi = max(a0, 16 * k), min(a0 + w.shape[0], 16 * k + NV - GR)
            if lo < hi:
                n = min(GC, NV - GC * k)
                o2_ref[GR + lo - 16 * k:GR + hi - 16 * k, :, GC * k:GC * k + n] = w[lo - a0:hi - a0, :, NV:NV + n]

    for c in range(15):
        col = iota((128, 128), 1)
        w = mm(pi, one_hot(iota((128, 128), 0) == (col >> 4) + 8 * c))
        k4[:, c * 128:(c + 1) * 128] = jnp.where((iota((128, 128), 0) >> 3) == (col & 15), w, 0.0).astype(BF)
    e6[...] = one_hot((iota((128, 960), 1) >> 3) == iota((128, 960), 0))

    def v1_rows(t):
        row = iota((96, 128), 0) + 96 * t
        z = mm(one_hot((row >> 3) == iota((96, 128), 1)), cvt[...]).astype(BF)
        w = mm(z, e6[...])
        keep = (iota((96, 960), 0) & 7) == (iota((96, 960), 1) & 7)
        v1k[pl.ds(pl.multiple_of(96 * t, 96), 96), :] = jnp.where(keep, w, 0.0).astype(BF)

    def v1_build(t, carry):
        v1_rows(t)
        return carry

    lax.fori_loop(0, 9, v1_build, 0)
    for k in range(1, ND):
        src = lax.rem(me + k, ND)
        bwait(rg.at[src, :, 0:SENT], rgsem.at[src])

    v = rg[:, :, GO:GO + 8, :].reshape(960, 128)

    def v1_out(t, carry):
        w = mm(v1k[pl.ds(pl.multiple_of(96 * t, 96), 96), :], v)
        o1_ref[pl.ds(12 * t, 12)] = w.reshape(12, 8, 128)[:, :, :NV]
        return carry

    lax.fori_loop(0, 9, v1_out, 0)

    for ab in range(0, NE, 2):
        n = min(2, NE - ab)
        w = mm(k4[...], jnp.concatenate([rg[:, :, 16 * (ab + u):16 * (ab + u) + 16, :].reshape(1920, 128)
                                         for u in range(n)], axis=1)).reshape(16, 8, 128 * n)
        for u in range(n):
            put(w[:, :, 128 * u:128 * u + 128], 16 * (ab + u))

    for c in range(NCH):
        for half, (_, _, peer, col) in enumerate(first):
            bwait(p1.at[:, rows(half, c)], p1r.at[half, c])
            z2[rows(half, c), :] = sb[col, rows(half, c), :] + p1[1, rows(half, c), :]
        for half, (_, _, peer, col) in enumerate(first):
            rcopy(z2.at[rows(half, c)], p2.at[rows(half, c)], p2s.at[half, c], p2r.at[half, c], peer).start()
    for c in range(NCH):
        for half in range(2):
            bwait(p2.at[rows(half, c)], p2r.at[half, c])
            w = sb[0, rows(half, c), :] + p1[0, rows(half, c), :] + p2[rows(half, c), :]
            put(w.reshape(-1, 8, 128), EX + CUTS[half][c] // 8)

    for k in range(1, ND):
        dst = lax.rem(me + k, ND)
        bwait(rg.at[dst, :, 0:SENT], sgsem.at[k])
    bwait(rs, ssem)
    for c in range(NCH):
        for half in range(2):
            bwait(p1.at[:, rows(half, c)], p1s.at[half, c])
            bwait(p2.at[rows(half, c)], p2s.at[half, c])


def write_out(x1_ref, x2_ref, y1_ref, y2_ref, sem):
    copies = [pltpu.make_async_copy(x1_ref, y1_ref, sem.at[0]), pltpu.make_async_copy(x2_ref, y2_ref, sem.at[1])]
    for c in copies:
        c.start()
    for c in copies:
        c.wait()


def solution(mesh):
    def local_part(ao, co, cv):
        a = ao.reshape(NP, ROWS, NQ)
        co, cv = (pltpu.with_memory_space_constraint(t.T, pltpu.HBM) for t in (co, cv))
        vm = pl.BlockSpec(memory_space=pltpu.VMEM)
        o1, o2 = pl.pallas_call(
            kernel,
            out_shape=[jax.ShapeDtypeStruct((NV, NO, NV), F32), jax.ShapeDtypeStruct((NV, NO, NV), F32)],
            in_specs=[pl.BlockSpec(memory_space=pltpu.HBM)] * 3,
            out_specs=[vm, vm],
            scratch_shapes=[
                pltpu.VMEM((NBUF, ROWS, NQ), BF),
                pltpu.VMEM((2, 8, 128, 128), BF),
                pltpu.VMEM((4, 2, NP, RS1, 128), BF),
                pltpu.VMEM((8, NP, EX + 16, 128), BF),
                pltpu.VMEM((4, NP, GR - EX, 128), BF),
                pltpu.VMEM((4, RSR, 128), F32),
                pltpu.VMEM((2, RSR, 128), F32),
                pltpu.VMEM((RSR, 128), F32),
                pltpu.VMEM((RSR, 128), F32),
                pltpu.VMEM((64, 960), BF),
                pltpu.VMEM((128, 1920), BF),
                pltpu.VMEM((2, 128, 240), BF),
                pltpu.VMEM((864, 960), BF),
                pltpu.VMEM((128, 960), BF),
                pltpu.VMEM((NO, NQ), BF),
                pltpu.VMEM((NV, NQ), BF),
                pltpu.VMEM((16, 128), BF),
                pltpu.VMEM((128, 128), BF),
                pltpu.VMEM((128, 128), BF),
                pltpu.SemaphoreType.DMA((NBUF,)),
                pltpu.SemaphoreType.DMA((2,)),
                pltpu.SemaphoreType.DMA((ND,)),
                pltpu.SemaphoreType.DMA((ND,)),
                pltpu.SemaphoreType.DMA,
                pltpu.SemaphoreType.DMA,
                pltpu.SemaphoreType.DMA((2, NCH)),
                pltpu.SemaphoreType.DMA((2, NCH)),
                pltpu.SemaphoreType.DMA((2, NCH)),
                pltpu.SemaphoreType.DMA((2, NCH)),
            ],
            compiler_params=pltpu.CompilerParams(collective_id=0, has_side_effects=True,
                                                 vmem_limit_bytes=34 * 1024 * 1024),
            name='mo_blocks',
        )(a, co, cv)
        o1, o2 = pl.pallas_call(
            write_out,
            out_shape=[jax.ShapeDtypeStruct((NV, NO, NV), F32), jax.ShapeDtypeStruct((NV, NO, NV), F32)],
            in_specs=[vm, vm],
            out_specs=[pl.BlockSpec(memory_space=pltpu.HBM)] * 2,
            scratch_shapes=[pltpu.SemaphoreType.DMA((2,))],
            compiler_params=pltpu.CompilerParams(vmem_limit_bytes=2 * 1024 * 1024),
            name='write_out',
        )(o1, o2)
        return o1.transpose(0, 2, 1), o2.transpose(1, 0, 2)

    return jax.shard_map(local_part, mesh=mesh,
                         in_specs=(P(('frag', 'dev')), P('frag'), P('frag')),
                         out_specs=(P('frag', None, 'dev'), P('frag', None, 'dev')),
                         check_vma=False)
```

```python
import jax
import jax.numpy as jnp
from jax import lax
from jax.experimental import pallas as pl
from jax.experimental.pallas import tpu as pltpu
from jax.sharding import PartitionSpec as P

MESH = pl.DeviceIdType.MESH
BF = jnp.bfloat16
F32 = jnp.float32
ND = 8
NP = 15
NQ = 120
NO = 8
NV = 108
ROWS = NQ * NQ
NBUF = 4
SPLIT = 5
VB = 6
GR = 16 * VB
GC = 20
NE = 2
EX = 16 * NE
GO = EX
SENT = EX + 8
RS0 = EX + 16
RS1 = RS0 + GR - EX
RSR = 8 * (GR - EX)
NCH = 2
HB = (VB - NE) // 2
HALF = 128 * HB
CH = HALF // NCH


def mm(a, b):
    return jnp.dot(a, b, preferred_element_type=F32)


def mm_nt(a, b):
    return lax.dot_general(a, b, (((1,), (1,)), ((), ())), preferred_element_type=F32)


def iota(shape, dim):
    return lax.broadcasted_iota(jnp.int32, shape, dim)


def one_hot(mask):
    return jnp.where(mask, 1.0, 0.0).astype(BF)


def kernel(a_ref, co_ref, cv_ref, o1_ref, o2_ref,
           abuf, tbuf, sg, rg, rs, sb, p1, z2, p2, k1, k4, k4c, v1k, e6, coin, cvin, cot, cvt, cv,
           asem, csem, sgsem, rgsem, ssem, rssem, p1s, p1r, p2s, p2r):
    me = lax.axis_index('dev')
    frag = lax.axis_index('frag')
    core = lax.rem(me, 2)
    mx = lax.rem(me // 2, 2)
    my = me // 4
    sib = me + 1 - 2 * core
    xn = me + 2 - 4 * mx
    yn = me + 4 - 8 * my
    dg = xn + 4 - 8 * my
    cols = [me, xn, yn, dg]

    def a_copies(p):
        slot = lax.rem(p, NBUF)
        step = ROWS // SPLIT
        return [pltpu.make_async_copy(a_ref.at[p, pl.ds(k * step, step)],
                                      abuf.at[slot, pl.ds(k * step, step)],
                                      asem.at[slot]) for k in range(SPLIT)]

    def a_start(p):
        for c in a_copies(p):
            c.start()

    def a_wait(p):
        slot = lax.rem(p, NBUF)
        pltpu.make_async_copy(a_ref.at[p], abuf.at[slot], asem.at[slot]).wait()

    cin = [pltpu.make_async_copy(co_ref, coin, csem.at[0]), pltpu.make_async_copy(cv_ref, cvin, csem.at[1])]
    for c in cin:
        c.start()
    for p in range(NBUF - 1):
        a_start(p)

    barrier = pltpu.get_barrier_semaphore()
    for k in range(1, ND):
        pl.semaphore_signal(barrier, inc=1, device_id=(frag, lax.rem(me + k, ND)), device_id_type=MESH)

    cot[...] = jnp.zeros(cot.shape, BF)
    cvt[...] = jnp.zeros(cvt.shape, BF)
    for c in cin:
        c.wait()
    cot[0:NO, 0:NQ] = coin[...]
    cvt[0:NV, 0:NQ] = cvin[...]
    cv[...] = mm_nt(one_hot(iota((128, 128), 0) == iota((128, 128), 1)), cvt[...]).astype(BF)
    xr = mm(one_hot((iota((64, 16), 0) >> 3) == iota((64, 16), 1)), cot[...]).astype(BF)
    diff = iota((128, 960), 1) - iota((128, 960), 0)
    hit = diff == 0
    for k in range(1, 8):
        hit = hit | (diff == 120 * k)
    off = iota((64, 960), 1) - 120 * (iota((64, 960), 0) & 7)
    k1[...] = jnp.where((off >= 0) & (off < 120), mm(xr, one_hot(hit)), 0.0).astype(BF)
    pi = mm(one_hot((iota((128, 16), 0) & 7) == iota((128, 16), 1)), cot[...]).astype(BF)
    for h, d in enumerate((me, sib)):
        col = iota((128, 240), 1)
        w = mm(pi, one_hot(iota((128, 240), 0) == (col >> 4) + NP * d))
        keep = (iota((128, 240), 0) >> 3) == (col & 15)
        k4c[h] = jnp.where(keep, w, 0.0).astype(BF)
    pl.semaphore_wait(barrier, ND - 1)

    def step1(p):
        slot = lax.rem(p, NBUF)
        tslot = lax.rem(p, 2)
        pad = jnp.zeros((960, 8), BF)
        for g in range(8):
            left = jnp.concatenate([abuf[slot, 1920 * g:1920 * g + 960, :], pad], axis=1)
            if g < 7:
                right = jnp.concatenate([abuf[slot, 1920 * g + 960:1920 * g + 1920, :], pad], axis=1)
                out = mm(k1[...], jnp.concatenate([left, right], axis=1))
                lo = out[:, :128].reshape(8, 8, 128)
                hi = out[:, 128:].reshape(8, 8, 128)
            else:
                lo = mm(k1[...], left).reshape(8, 8, 128)
                hi = jnp.zeros((8, 8, 128), F32)
            tbuf[tslot, :, 16 * g:16 * g + 16, :] = jnp.concatenate([lo, hi], axis=1).astype(BF)

    def step23(p):
        t = tbuf[lax.rem(p, 2)].reshape(1024, 128)
        h = mm(t, cv[...]).astype(BF).reshape(8, 128, 128)
        hoo = mm_nt(cot[...], t)
        lane = iota((16, 128), 1)
        for x in range(0, 8, 2):
            g = mm(cvt[0:112, :], jnp.concatenate([h[x], h[x + 1]], axis=1))
            for y in range(2):
                last = g[GR:GR + 16, 128 * y:128 * y + 128]
                tiles = [jnp.where(lane < NV, g[16 * k:16 * k + 16, 128 * y:128 * y + 128],
                                   pltpu.roll(last, (NV - GC * k) % 128, 1)) for k in range(VB)]
                sg[x // 2, y, p, 0:EX] = jnp.concatenate(tiles[:NE], axis=0).astype(BF)
                sg[x // 2, y, p, RS0:RS1] = jnp.concatenate(tiles[NE:], axis=0).astype(BF)
        hoo = jnp.concatenate([hoo[0:8, 128 * x:128 * x + 128] for x in range(8)], axis=0).astype(BF)
        goo = mm(hoo, cv[...]).astype(BF).reshape(4, 2, 8, 128)
        for y in range(2):
            sg[:, y, p, GO:GO + 8] = goo[:, y]

    def sends(p):
        out = [pltpu.make_async_remote_copy(
            src_ref=sg.at[:, 1 - core, p, RS0:RS1], dst_ref=rs.at[:, p],
            send_sem=ssem, recv_sem=rssem, device_id=(frag, sib), device_id_type=MESH)]
        for k in range(1, ND):
            dst = lax.rem(me + k, ND)
            out.append(pltpu.make_async_remote_copy(
                src_ref=sg.at[dst // 2, lax.rem(dst, 2), p, 0:SENT], dst_ref=rg.at[me, p, 0:SENT],
                send_sem=sgsem.at[k], recv_sem=rgsem.at[me], device_id=(frag, dst), device_id_type=MESH))
        return out

    def send(p):
        for c in sends(p):
            c.start()
        rg[me, p, 0:EX] = sg[me // 2, core, p, 0:EX]
        rg[me, p, GO:GO + 8] = sg[me // 2, core, p, GO:GO + 8]

    a_wait(0)
    a_start(NBUF - 1)
    step1(0)

    def body(p, carry):
        @pl.when(p + NBUF - 1 < NP)
        def _():
            a_start(p + NBUF - 1)

        @pl.when(p >= 2)
        def _():
            send(p - 2)

        a_wait(p)
        step23(p - 1)
        step1(p)
        return carry

    lax.fori_loop(1, NP, body, 0)
    send(NP - 2)
    step23(NP - 1)
    send(NP - 1)

    def rcopy(src, dst, ss, rr, dev):
        return pltpu.make_async_remote_copy(src_ref=src, dst_ref=dst, send_sem=ss, recv_sem=rr,
                                            device_id=(frag, dev), device_id_type=MESH)

    def bwait(view, sem):
        pltpu.make_async_copy(view, view, sem).wait()

    units = [(3, 0), (3, 1), (1, 0), (2, 1), (2, 0), (1, 1), (0, 0), (0, 1)]

    def part(buf, at, kc):
        return mm(kc, jnp.concatenate([buf[at + (slice(None), slice(r, r + 16))].reshape(240, 128)
                                       for r in range(0, 16 * HB, 16)], axis=1))

    for c, half in units:
        r = RS0 + 16 * HB * half
        w = part(sg.at[:, :, :, r:r + 16 * HB], (cols[c] // 2, core), k4c[0])
        for b in range(HB):
            sb[c, HALF * half + 128 * b:HALF * half + 128 * b + 128, :] = w[:, 128 * b:128 * b + 128]

    def half_rows(half):
        return slice(HALF * half, HALF * half + HALF)

    def rows(half, c):
        return slice(HALF * half + CH * c, HALF * half + CH * c + CH)

    def first(n):
        c, half = units[n]
        m = 1 if c == 3 else 0
        return rcopy(sb.at[c, half_rows(half)], p1.at[m, half_rows(half)], p1s.at[half, m], p1r.at[half, m],
                     (xn, yn)[half])

    bwait(rs, rssem)
    for n, (c, half) in enumerate(units):
        r = 16 * HB * half
        w = part(rs.at[:, :, r:r + 16 * HB], (cols[c] // 2,), k4c[1])
        for b in range(HB):
            at = slice(HALF * half + 128 * b, HALF * half + 128 * b + 128)
            sb[c, at, :] = sb[c, at, :] + w[:, 128 * b:128 * b + 128]
        if 1 <= n <= 4:
            first(n - 1).start()

    def put(w, a0):
        o2_ref[a0:a0 + w.shape[0]] = w[:, :, :NV]
        for k in range(VB):
            lo, hi = max(a0, 16 * k), min(a0 + w.shape[0], 16 * k + NV - GR)
            if lo < hi:
                n = min(GC, NV - GC * k)
                o2_ref[GR + lo - 16 * k:GR + hi - 16 * k, :, GC * k:GC * k + n] = w[lo - a0:hi - a0, :, NV:NV + n]

    for c in range(15):
        col = iota((128, 128), 1)
        w = mm(pi, one_hot(iota((128, 128), 0) == (col >> 4) + 8 * c))
        k4[:, c * 128:(c + 1) * 128] = jnp.where((iota((128, 128), 0) >> 3) == (col & 15), w, 0.0).astype(BF)
    e6[...] = one_hot((iota((128, 960), 1) >> 3) == iota((128, 960), 0))

    def v1_rows(t):
        row = iota((96, 128), 0) + 96 * t
        z = mm(one_hot((row >> 3) == iota((96, 128), 1)), cvt[...]).astype(BF)
        w = mm(z, e6[...])
        keep = (iota((96, 960), 0) & 7) == (iota((96, 960), 1) & 7)
        v1k[pl.ds(pl.multiple_of(96 * t, 96), 96), :] = jnp.where(keep, w, 0.0).astype(BF)

    def v1_build(t, carry):
        v1_rows(t)
        return carry

    lax.fori_loop(0, 9, v1_build, 0)
    for k in range(1, ND):
        src = lax.rem(me + k, ND)
        bwait(rg.at[src, :, 0:SENT], rgsem.at[src])

    v = rg[:, :, GO:GO + 8, :].reshape(960, 128)

    def v1_out(t, carry):
        w = mm(v1k[pl.ds(pl.multiple_of(96 * t, 96), 96), :], v)
        o1_ref[pl.ds(12 * t, 12)] = w.reshape(12, 8, 128)[:, :, :NV]
        return carry

    lax.fori_loop(0, 9, v1_out, 0)

    for ab in range(0, NE, 2):
        n = min(2, NE - ab)
        w = mm(k4[...], jnp.concatenate([rg[:, :, 16 * (ab + u):16 * (ab + u) + 16, :].reshape(1920, 128)
                                         for u in range(n)], axis=1)).reshape(16, 8, 128 * n)
        for u in range(n):
            put(w[:, :, 128 * u:128 * u + 128], 16 * (ab + u))

    for half in range(2):
        bwait(p1.at[1, half_rows(half)], p1r.at[half, 1])
        z2[half_rows(half), :] = sb[2 - half, half_rows(half), :] + p1[1, half_rows(half), :]
    for c in range(NCH):
        for half in range(2):
            rcopy(z2.at[rows(half, c)], p2.at[rows(half, c)], p2s.at[half, c], p2r.at[half, c],
                  (yn, xn)[half]).start()
    for half in range(2):
        bwait(p1.at[0, half_rows(half)], p1r.at[half, 0])
        sb[0, half_rows(half), :] = sb[0, half_rows(half), :] + p1[0, half_rows(half), :]
    for c in range(NCH):
        for half in range(2):
            bwait(p2.at[rows(half, c)], p2r.at[half, c])
            w = sb[0, rows(half, c), :] + p2[rows(half, c), :]
            put(w.reshape(-1, 8, 128), EX + (HALF * half + CH * c) // 8)

    for k in range(1, ND):
        dst = lax.rem(me + k, ND)
        bwait(rg.at[dst, :, 0:SENT], sgsem.at[k])
    bwait(rs, ssem)
    for c in range(NCH):
        for half in range(2):
            bwait(p2.at[rows(half, c)], p2s.at[half, c])
    for m in range(2):
        for half in range(2):
            bwait(p1.at[m, half_rows(half)], p1s.at[half, m])


def write_out(x1_ref, x2_ref, y1_ref, y2_ref, sem):
    copies = [pltpu.make_async_copy(x1_ref, y1_ref, sem.at[0]), pltpu.make_async_copy(x2_ref, y2_ref, sem.at[1])]
    for c in copies:
        c.start()
    for c in copies:
        c.wait()


def solution(mesh):
    def local_part(ao, co, cv):
        a = ao.reshape(NP, ROWS, NQ)
        co, cv = (pltpu.with_memory_space_constraint(t.T, pltpu.HBM) for t in (co, cv))
        vm = pl.BlockSpec(memory_space=pltpu.VMEM)
        o1, o2 = pl.pallas_call(
            kernel,
            out_shape=[jax.ShapeDtypeStruct((NV, NO, NV), F32), jax.ShapeDtypeStruct((NV, NO, NV), F32)],
            in_specs=[pl.BlockSpec(memory_space=pltpu.HBM)] * 3,
            out_specs=[vm, vm],
            scratch_shapes=[
                pltpu.VMEM((NBUF, ROWS, NQ), BF),
                pltpu.VMEM((2, 8, 128, 128), BF),
                pltpu.VMEM((4, 2, NP, RS1, 128), BF),
                pltpu.VMEM((8, NP, EX + 16, 128), BF),
                pltpu.VMEM((4, NP, GR - EX, 128), BF),
                pltpu.VMEM((4, RSR, 128), F32),
                pltpu.VMEM((2, RSR, 128), F32),
                pltpu.VMEM((RSR, 128), F32),
                pltpu.VMEM((RSR, 128), F32),
                pltpu.VMEM((64, 960), BF),
                pltpu.VMEM((128, 1920), BF),
                pltpu.VMEM((2, 128, 240), BF),
                pltpu.VMEM((864, 960), BF),
                pltpu.VMEM((128, 960), BF),
                pltpu.VMEM((NO, NQ), BF),
                pltpu.VMEM((NV, NQ), BF),
                pltpu.VMEM((16, 128), BF),
                pltpu.VMEM((128, 128), BF),
                pltpu.VMEM((128, 128), BF),
                pltpu.SemaphoreType.DMA((NBUF,)),
                pltpu.SemaphoreType.DMA((2,)),
                pltpu.SemaphoreType.DMA((ND,)),
                pltpu.SemaphoreType.DMA((ND,)),
                pltpu.SemaphoreType.DMA,
                pltpu.SemaphoreType.DMA,
                pltpu.SemaphoreType.DMA((2, 2)),
                pltpu.SemaphoreType.DMA((2, 2)),
                pltpu.SemaphoreType.DMA((2, NCH)),
                pltpu.SemaphoreType.DMA((2, NCH)),
            ],
            compiler_params=pltpu.CompilerParams(collective_id=0, has_side_effects=True,
                                                 vmem_limit_bytes=34 * 1024 * 1024),
            name='mo_blocks',
        )(a, co, cv)
        o1, o2 = pl.pallas_call(
            write_out,
            out_shape=[jax.ShapeDtypeStruct((NV, NO, NV), F32), jax.ShapeDtypeStruct((NV, NO, NV), F32)],
            in_specs=[vm, vm],
            out_specs=[pl.BlockSpec(memory_space=pltpu.HBM)] * 2,
            scratch_shapes=[pltpu.SemaphoreType.DMA((2,))],
            compiler_params=pltpu.CompilerParams(vmem_limit_bytes=2 * 1024 * 1024),
            name='write_out',
        )(o1, o2)
        return o1.transpose(0, 2, 1), o2.transpose(1, 0, 2)

    return jax.shard_map(local_part, mesh=mesh,
                         in_specs=(P(('frag', 'dev')), P('frag'), P('frag')),
                         out_specs=(P('frag', None, 'dev'), P('frag', None, 'dev')),
                         check_vma=False)
```

```python
import jax
import jax.numpy as jnp
from jax import lax
from jax.experimental import pallas as pl
from jax.experimental.pallas import tpu as pltpu
from jax.sharding import PartitionSpec as P

MESH = pl.DeviceIdType.MESH
BF = jnp.bfloat16
F32 = jnp.float32
ND = 8
NP = 15
NQ = 120
NO = 8
NV = 108
ROWS = NQ * NQ
NBUF = 4
SPLIT = 5
VB = 6
GR = 16 * VB
GC = 20
EX = 40
VB = 6
GR = 16 * VB
GC = 20
GO = EX
SENT = EX + 8
RS0 = -(-SENT // 16) * 16
RSA = GR - EX
RSB = -(-RSA // 16)
RS1 = RS0 + 16 * RSB
RSR = 8 * RSA
NCH = 2
HB = RSB // 2
HALF = RSR // 2
CH = HALF // NCH


def mm(a, b):
    return jnp.dot(a, b, preferred_element_type=F32)


def mm_nt(a, b):
    return lax.dot_general(a, b, (((1,), (1,)), ((), ())), preferred_element_type=F32)


def iota(shape, dim):
    return lax.broadcasted_iota(jnp.int32, shape, dim)


def one_hot(mask):
    return jnp.where(mask, 1.0, 0.0).astype(BF)


def kernel(a_ref, co_ref, cv_ref, o1_ref, o2_ref,
           abuf, tbuf, sg, rg, rs, sb, p1, z2, p2, k1, k4, k4c, v1k, e6, coin, cvin, cot, cvt, cv,
           asem, csem, sgsem, rgsem, ssem, rssem, p1s, p1r, p2s, p2r):
    me = lax.axis_index('dev')
    frag = lax.axis_index('frag')
    core = lax.rem(me, 2)
    mx = lax.rem(me // 2, 2)
    my = me // 4
    sib = me + 1 - 2 * core
    xn = me + 2 - 4 * mx
    yn = me + 4 - 8 * my
    dg = xn + 4 - 8 * my
    cols = [me, xn, yn, dg]
    chips = [c // 2 for c in cols]
    peers = [(3, 0), (3, 1), (1, 0), (1, 1), (2, 0), (2, 1), (0, 1)]
    par = [core, 1 - core]

    def a_copies(p):
        slot = lax.rem(p, NBUF)
        step = ROWS // SPLIT
        return [pltpu.make_async_copy(a_ref.at[p, pl.ds(k * step, step)],
                                      abuf.at[slot, pl.ds(k * step, step)],
                                      asem.at[slot]) for k in range(SPLIT)]

    def a_start(p):
        for c in a_copies(p):
            c.start()

    def a_wait(p):
        slot = lax.rem(p, NBUF)
        pltpu.make_async_copy(a_ref.at[p], abuf.at[slot], asem.at[slot]).wait()

    cin = [pltpu.make_async_copy(co_ref, coin, csem.at[0]), pltpu.make_async_copy(cv_ref, cvin, csem.at[1])]
    for c in cin:
        c.start()
    for p in range(NBUF - 1):
        a_start(p)

    barrier = pltpu.get_barrier_semaphore()
    for k in range(1, ND):
        pl.semaphore_signal(barrier, inc=1, device_id=(frag, lax.rem(me + k, ND)), device_id_type=MESH)

    cot[...] = jnp.zeros(cot.shape, BF)
    cvt[...] = jnp.zeros(cvt.shape, BF)
    for c in cin:
        c.wait()
    cot[0:NO, 0:NQ] = coin[...]
    cvt[0:NV, 0:NQ] = cvin[...]
    cv[...] = mm_nt(one_hot(iota((128, 128), 0) == iota((128, 128), 1)), cvt[...]).astype(BF)
    xr = mm(one_hot((iota((64, 16), 0) >> 3) == iota((64, 16), 1)), cot[...]).astype(BF)
    diff = iota((128, 960), 1) - iota((128, 960), 0)
    hit = diff == 0
    for k in range(1, 8):
        hit = hit | (diff == 120 * k)
    off = iota((64, 960), 1) - 120 * (iota((64, 960), 0) & 7)
    k1[...] = jnp.where((off >= 0) & (off < 120), mm(xr, one_hot(hit)), 0.0).astype(BF)
    pi = mm(one_hot((iota((128, 16), 0) & 7) == iota((128, 16), 1)), cot[...]).astype(BF)
    for h, d in enumerate((me, sib)):
        col = iota((128, 240), 1)
        w = mm(pi, one_hot(iota((128, 240), 0) == (col >> 4) + NP * d))
        keep = (iota((128, 240), 0) >> 3) == (col & 15)
        k4c[h] = jnp.where(keep, w, 0.0).astype(BF)
    pl.semaphore_wait(barrier, ND - 1)

    def step1(p):
        slot = lax.rem(p, NBUF)
        tslot = lax.rem(p, 2)
        pad = jnp.zeros((960, 8), BF)
        for g in range(8):
            left = jnp.concatenate([abuf[slot, 1920 * g:1920 * g + 960, :], pad], axis=1)
            if g < 7:
                right = jnp.concatenate([abuf[slot, 1920 * g + 960:1920 * g + 1920, :], pad], axis=1)
                out = mm(k1[...], jnp.concatenate([left, right], axis=1))
                lo = out[:, :128].reshape(8, 8, 128)
                hi = out[:, 128:].reshape(8, 8, 128)
            else:
                lo = mm(k1[...], left).reshape(8, 8, 128)
                hi = jnp.zeros((8, 8, 128), F32)
            tbuf[tslot, :, 16 * g:16 * g + 16, :] = jnp.concatenate([lo, hi], axis=1).astype(BF)

    def step23(p):
        t = tbuf[lax.rem(p, 2)].reshape(1024, 128)
        h = mm(t, cv[...]).astype(BF).reshape(8, 128, 128)
        hoo = mm_nt(cot[...], t)
        lane = iota((16, 128), 1)
        for x in range(0, 8, 2):
            g = mm(cvt[0:112, :], jnp.concatenate([h[x], h[x + 1]], axis=1))
            for y in range(2):
                last = g[GR:GR + 16, 128 * y:128 * y + 128]
                tiles = [jnp.where(lane < NV, g[16 * k:16 * k + 16, 128 * y:128 * y + 128],
                                   pltpu.roll(last, (NV - GC * k) % 128, 1)) for k in range(VB)]
                tiles = jnp.concatenate(tiles, axis=0)
                sg[x // 2, y, p, 0:EX] = tiles[:EX].astype(BF)
                sg[x // 2, y, p, RS0:RS0 + RSA] = tiles[EX:].astype(BF)
        hoo = jnp.concatenate([hoo[0:8, 128 * x:128 * x + 128] for x in range(8)], axis=0).astype(BF)
        goo = mm(hoo, cv[...]).astype(BF).reshape(4, 2, 8, 128)
        for y in range(2):
            sg[:, y, p, GO:GO + 8] = goo[:, y]

    def sends(p):
        out = [pltpu.make_async_remote_copy(
            src_ref=sg.at[:, 1 - core, p, RS0:RS1], dst_ref=rs.at[:, p],
            send_sem=ssem, recv_sem=rssem, device_id=(frag, sib), device_id_type=MESH)]
        for k, (c, q) in enumerate(peers):
            out.append(pltpu.make_async_remote_copy(
                src_ref=sg.at[chips[c], par[q], p, 0:SENT], dst_ref=rg.at[me, p, 0:SENT],
                send_sem=sgsem.at[k], recv_sem=rgsem.at[me],
                device_id=(frag, 2 * chips[c] + par[q]), device_id_type=MESH))
        return out

    def send(p):
        for c in sends(p):
            c.start()
        rg[me, p, 0:SENT] = sg[chips[0], core, p, 0:SENT]

    if RS0 + RSA < RS1:
        sg[:, :, :, RS0 + RSA:RS1, :] = jnp.zeros((4, 2, NP, RS1 - RS0 - RSA, 128), BF)
    a_wait(0)
    a_start(NBUF - 1)
    step1(0)

    def body(p, carry):
        @pl.when(p + NBUF - 1 < NP)
        def _():
            a_start(p + NBUF - 1)

        @pl.when(p >= 2)
        def _():
            send(p - 2)

        a_wait(p)
        step23(p - 1)
        step1(p)
        return carry

    lax.fori_loop(1, NP, body, 0)
    send(NP - 2)
    step23(NP - 1)
    send(NP - 1)

    def rcopy(src, dst, ss, rr, dev):
        return pltpu.make_async_remote_copy(src_ref=src, dst_ref=dst, send_sem=ss, recv_sem=rr,
                                            device_id=(frag, dev), device_id_type=MESH)

    def bwait(view, sem):
        pltpu.make_async_copy(view, view, sem).wait()

    units = [(3, 0), (3, 1), (1, 0), (2, 0), (2, 1), (1, 1), (0, 0), (0, 1)]

    def part(buf, at, kc):
        return mm(kc, jnp.concatenate([buf[at + (slice(None), slice(r, r + 16))].reshape(240, 128)
                                       for r in range(0, 16 * HB, 16)], axis=1))

    for c, half in units:
        r = RS0 + 16 * HB * half
        w = part(sg.at[:, :, :, r:r + 16 * HB], (chips[c], core), k4c[0])
        for b in range(HB):
            sb[c, 128 * (HB * half + b):128 * (HB * half + b) + 128, :] = w[:, 128 * b:128 * b + 128]

    def half_rows(half):
        return slice(HALF * half, HALF * half + HALF)

    def rows(half, c):
        return slice(HALF * half + CH * c, HALF * half + CH * c + CH)

    def first(c, half):
        m = 1 if c == 3 else 0
        return rcopy(sb.at[c, half_rows(half)], p1.at[m, half_rows(half)], p1s.at[half, m], p1r.at[half, m],
                     (xn, yn)[half])

    sent_after = {1: (3, 0), 2: (3, 1), 3: (1, 0), 5: (2, 1)}
    bwait(rs, rssem)
    for n, (c, half) in enumerate(units):
        r = 16 * HB * half
        w = part(rs.at[:, :, r:r + 16 * HB], (chips[c],), k4c[1])
        for b in range(HB):
            at = slice(128 * (HB * half + b), 128 * (HB * half + b) + 128)
            sb[c, at, :] = sb[c, at, :] + w[:, 128 * b:128 * b + 128]
        if n in sent_after:
            first(*sent_after[n]).start()

    def put(w, a0):
        o2_ref[a0:a0 + w.shape[0]] = w[:, :, :NV]
        for k in range(VB):
            lo, hi = max(a0, 16 * k), min(a0 + w.shape[0], 16 * k + NV - GR)
            if lo < hi:
                n = min(GC, NV - GC * k)
                o2_ref[GR + lo - 16 * k:GR + hi - 16 * k, :, GC * k:GC * k + n] = w[lo - a0:hi - a0, :, NV:NV + n]

    for c in range(15):
        col = iota((128, 128), 1)
        w = mm(pi, one_hot(iota((128, 128), 0) == (col >> 4) + 8 * c))
        k4[:, c * 128:(c + 1) * 128] = jnp.where((iota((128, 128), 0) >> 3) == (col & 15), w, 0.0).astype(BF)
    e6[...] = one_hot((iota((128, 960), 1) >> 3) == iota((128, 960), 0))

    def v1_rows(t):
        row = iota((96, 128), 0) + 96 * t
        z = mm(one_hot((row >> 3) == iota((96, 128), 1)), cvt[...]).astype(BF)
        w = mm(z, e6[...])
        keep = (iota((96, 960), 0) & 7) == (iota((96, 960), 1) & 7)
        v1k[pl.ds(pl.multiple_of(96 * t, 96), 96), :] = jnp.where(keep, w, 0.0).astype(BF)

    def v1_build(t, carry):
        v1_rows(t)
        return carry

    lax.fori_loop(0, 9, v1_build, 0)
    for k in range(1, ND):
        src = lax.rem(me + k, ND)
        bwait(rg.at[src, :, 0:SENT], rgsem.at[src])

    v = rg[:, :, GO:GO + 8, :].reshape(960, 128)

    def v1_out(t, carry):
        w = mm(v1k[pl.ds(pl.multiple_of(96 * t, 96), 96), :], v)
        o1_ref[pl.ds(12 * t, 12)] = w.reshape(12, 8, 128)[:, :, :NV]
        return carry

    lax.fori_loop(0, 9, v1_out, 0)

    nx = -(-EX // 16)
    for ab in range(0, nx, 2):
        n = min(2, nx - ab)
        w = mm(k4[...], jnp.concatenate([rg[:, :, 16 * (ab + u):16 * (ab + u) + 16, :].reshape(1920, 128)
                                         for u in range(n)], axis=1)).reshape(16, 8, 128 * n)
        for u in range(n):
            put(w[:min(16, EX - 16 * (ab + u)), :, 128 * u:128 * u + 128], 16 * (ab + u))

    for half in range(2):
        bwait(p1.at[1, half_rows(half)], p1r.at[half, 1])
        z2[half_rows(half), :] = sb[2 - half, half_rows(half), :] + p1[1, half_rows(half), :]
    for c in range(NCH):
        for half in range(2):
            rcopy(z2.at[rows(half, c)], p2.at[rows(half, c)], p2s.at[half, c], p2r.at[half, c],
                  (yn, xn)[half]).start()
    for half in range(2):
        bwait(p1.at[0, half_rows(half)], p1r.at[half, 0])
        sb[0, half_rows(half), :] = sb[0, half_rows(half), :] + p1[0, half_rows(half), :]
    for c in range(NCH):
        for half in range(2):
            bwait(p2.at[rows(half, c)], p2r.at[half, c])
            w = sb[0, rows(half, c), :] + p2[rows(half, c), :]
            put(w.reshape(-1, 8, 128), EX + (HALF * half + CH * c) // 8)

    for k in range(ND - 1):
        bwait(rg.at[0, :, 0:SENT], sgsem.at[k])
    bwait(rs, ssem)
    for c in range(NCH):
        for half in range(2):
            bwait(p2.at[rows(half, c)], p2s.at[half, c])
    for m in range(2):
        for half in range(2):
            bwait(p1.at[m, half_rows(half)], p1s.at[half, m])


def write_out(x1_ref, x2_ref, y1_ref, y2_ref, sem):
    copies = [pltpu.make_async_copy(x1_ref, y1_ref, sem.at[0]), pltpu.make_async_copy(x2_ref, y2_ref, sem.at[1])]
    for c in copies:
        c.start()
    for c in copies:
        c.wait()


def solution(mesh):
    def local_part(ao, co, cv):
        a = ao.reshape(NP, ROWS, NQ)
        co, cv = (pltpu.with_memory_space_constraint(t.T, pltpu.HBM) for t in (co, cv))
        vm = pl.BlockSpec(memory_space=pltpu.VMEM)
        o1, o2 = pl.pallas_call(
            kernel,
            out_shape=[jax.ShapeDtypeStruct((NV, NO, NV), F32), jax.ShapeDtypeStruct((NV, NO, NV), F32)],
            in_specs=[pl.BlockSpec(memory_space=pltpu.HBM)] * 3,
            out_specs=[vm, vm],
            scratch_shapes=[
                pltpu.VMEM((NBUF, ROWS, NQ), BF),
                pltpu.VMEM((2, 8, 128, 128), BF),
                pltpu.VMEM((4, 2, NP, RS1, 128), BF),
                pltpu.VMEM((8, NP, RS0, 128), BF),
                pltpu.VMEM((4, NP, RS1 - RS0, 128), BF),
                pltpu.VMEM((4, 128 * RSB, 128), F32),
                pltpu.VMEM((2, RSR, 128), F32),
                pltpu.VMEM((RSR, 128), F32),
                pltpu.VMEM((RSR, 128), F32),
                pltpu.VMEM((64, 960), BF),
                pltpu.VMEM((128, 1920), BF),
                pltpu.VMEM((2, 128, 240), BF),
                pltpu.VMEM((864, 960), BF),
                pltpu.VMEM((128, 960), BF),
                pltpu.VMEM((NO, NQ), BF),
                pltpu.VMEM((NV, NQ), BF),
                pltpu.VMEM((16, 128), BF),
                pltpu.VMEM((128, 128), BF),
                pltpu.VMEM((128, 128), BF),
                pltpu.SemaphoreType.DMA((NBUF,)),
                pltpu.SemaphoreType.DMA((2,)),
                pltpu.SemaphoreType.DMA((ND,)),
                pltpu.SemaphoreType.DMA((ND,)),
                pltpu.SemaphoreType.DMA,
                pltpu.SemaphoreType.DMA,
                pltpu.SemaphoreType.DMA((2, 2)),
                pltpu.SemaphoreType.DMA((2, 2)),
                pltpu.SemaphoreType.DMA((2, NCH)),
                pltpu.SemaphoreType.DMA((2, NCH)),
            ],
            compiler_params=pltpu.CompilerParams(collective_id=0, has_side_effects=True,
                                                 vmem_limit_bytes=34 * 1024 * 1024),
            name='mo_blocks',
        )(a, co, cv)
        o1, o2 = pl.pallas_call(
            write_out,
            out_shape=[jax.ShapeDtypeStruct((NV, NO, NV), F32), jax.ShapeDtypeStruct((NV, NO, NV), F32)],
            in_specs=[vm, vm],
            out_specs=[pl.BlockSpec(memory_space=pltpu.HBM)] * 2,
            scratch_shapes=[pltpu.SemaphoreType.DMA((2,))],
            compiler_params=pltpu.CompilerParams(vmem_limit_bytes=2 * 1024 * 1024),
            name='write_out',
        )(o1, o2)
        return o1.transpose(0, 2, 1), o2.transpose(1, 0, 2)

    return jax.shard_map(local_part, mesh=mesh,
                         in_specs=(P(('frag', 'dev')), P('frag'), P('frag')),
                         out_specs=(P('frag', None, 'dev'), P('frag', None, 'dev')),
                         check_vma=False)
```

```python
import jax
import jax.numpy as jnp
from jax import lax
from jax.experimental import pallas as pl
from jax.experimental.pallas import tpu as pltpu
from jax.sharding import PartitionSpec as P

MESH = pl.DeviceIdType.MESH
BF = jnp.bfloat16
F32 = jnp.float32
ND = 8
NP = 15
NQ = 120
NO = 8
NV = 108
ROWS = NQ * NQ
NBUF = 4
SPLIT = 5
VB = 6
GR = 16 * VB
GC = 20
EX = 40
VB = 6
GR = 16 * VB
GC = 20
GO = EX
SENT = EX + 8
RS0 = -(-SENT // 16) * 16
RSA = GR - EX
RSB = -(-RSA // 16)
RS1 = RS0 + 16 * RSB
RSR = 8 * RSA
NCH = 2
HB = RSB // 2
HALF = RSR // 2
CH = HALF // NCH


def mm(a, b):
    return jnp.dot(a, b, preferred_element_type=F32)


def mm_nt(a, b):
    return lax.dot_general(a, b, (((1,), (1,)), ((), ())), preferred_element_type=F32)


def iota(shape, dim):
    return lax.broadcasted_iota(jnp.int32, shape, dim)


def one_hot(mask):
    return jnp.where(mask, 1.0, 0.0).astype(BF)


def kernel(a_ref, co_ref, cv_ref, o1_ref, o2_ref,
           abuf, tbuf, sg, rg, rs, sb, p1, z2, p2, k1, k4, k4c, v1k, e6, coin, cvin, cot, cvt, cv,
           asem, csem, sgsem, rgsem, ssem, rssem, p1s, p1r, p2s, p2r):
    me = lax.axis_index('dev')
    frag = lax.axis_index('frag')
    core = lax.rem(me, 2)
    mx = lax.rem(me // 2, 2)
    my = me // 4
    sib = me + 1 - 2 * core
    xn = me + 2 - 4 * mx
    yn = me + 4 - 8 * my
    dg = xn + 4 - 8 * my
    cols = [me, xn, yn, dg]
    chips = [c // 2 for c in cols]
    peers = [(3, 0), (3, 1), (1, 0), (1, 1), (2, 0), (2, 1), (0, 1)]
    par = [core, 1 - core]

    def a_copies(p):
        slot = lax.rem(p, NBUF)
        step = ROWS // SPLIT
        return [pltpu.make_async_copy(a_ref.at[p, pl.ds(k * step, step)],
                                      abuf.at[slot, pl.ds(k * step, step)],
                                      asem.at[slot]) for k in range(SPLIT)]

    def a_start(p):
        for c in a_copies(p):
            c.start()

    def a_wait(p):
        slot = lax.rem(p, NBUF)
        pltpu.make_async_copy(a_ref.at[p], abuf.at[slot], asem.at[slot]).wait()

    cin = [pltpu.make_async_copy(co_ref, coin, csem.at[0]), pltpu.make_async_copy(cv_ref, cvin, csem.at[1])]
    for c in cin:
        c.start()
    for p in range(NBUF - 1):
        a_start(p)

    barrier = pltpu.get_barrier_semaphore()
    for k in range(1, ND):
        pl.semaphore_signal(barrier, inc=1, device_id=(frag, lax.rem(me + k, ND)), device_id_type=MESH)

    cot[...] = jnp.zeros(cot.shape, BF)
    cvt[...] = jnp.zeros(cvt.shape, BF)
    for c in cin:
        c.wait()
    cot[0:NO, 0:NQ] = coin[...]
    cvt[0:NV, 0:NQ] = cvin[...]
    cv[...] = mm_nt(one_hot(iota((128, 128), 0) == iota((128, 128), 1)), cvt[...]).astype(BF)
    xr = mm(one_hot((iota((64, 16), 0) >> 3) == iota((64, 16), 1)), cot[...]).astype(BF)
    diff = iota((128, 960), 1) - iota((128, 960), 0)
    hit = diff == 0
    for k in range(1, 8):
        hit = hit | (diff == 120 * k)
    off = iota((64, 960), 1) - 120 * (iota((64, 960), 0) & 7)
    k1[...] = jnp.where((off >= 0) & (off < 120), mm(xr, one_hot(hit)), 0.0).astype(BF)
    pi = mm(one_hot((iota((128, 16), 0) & 7) == iota((128, 16), 1)), cot[...]).astype(BF)
    for h, d in enumerate((me, sib)):
        col = iota((128, 240), 1)
        w = mm(pi, one_hot(iota((128, 240), 0) == (col >> 4) + NP * d))
        keep = (iota((128, 240), 0) >> 3) == (col & 15)
        k4c[h] = jnp.where(keep, w, 0.0).astype(BF)
    pl.semaphore_wait(barrier, ND - 1)

    def step1(p):
        slot = lax.rem(p, NBUF)
        tslot = lax.rem(p, 2)
        pad = jnp.zeros((960, 8), BF)
        for g in range(8):
            left = jnp.concatenate([abuf[slot, 1920 * g:1920 * g + 960, :], pad], axis=1)
            if g < 7:
                right = jnp.concatenate([abuf[slot, 1920 * g + 960:1920 * g + 1920, :], pad], axis=1)
                out = mm(k1[...], jnp.concatenate([left, right], axis=1))
                lo = out[:, :128].reshape(8, 8, 128)
                hi = out[:, 128:].reshape(8, 8, 128)
            else:
                lo = mm(k1[...], left).reshape(8, 8, 128)
                hi = jnp.zeros((8, 8, 128), F32)
            tbuf[tslot, :, 16 * g:16 * g + 16, :] = jnp.concatenate([lo, hi], axis=1).astype(BF)

    def step23(p):
        t = tbuf[lax.rem(p, 2)].reshape(1024, 128)
        h = mm(t, cv[...]).astype(BF).reshape(8, 128, 128)
        hoo = mm_nt(cot[...], t)
        lane = iota((16, 128), 1)
        for x in range(0, 8, 2):
            g = mm(cvt[0:112, :], jnp.concatenate([h[x], h[x + 1]], axis=1))
            for y in range(2):
                last = g[GR:GR + 16, 128 * y:128 * y + 128]
                tiles = [jnp.where(lane < NV, g[16 * k:16 * k + 16, 128 * y:128 * y + 128],
                                   pltpu.roll(last, (NV - GC * k) % 128, 1)) for k in range(VB)]
                tiles = jnp.concatenate(tiles, axis=0)
                sg[x // 2, y, p, 0:EX] = tiles[:EX].astype(BF)
                sg[x // 2, y, p, RS0:RS0 + RSA] = tiles[EX:].astype(BF)
        hoo = jnp.concatenate([hoo[0:8, 128 * x:128 * x + 128] for x in range(8)], axis=0).astype(BF)
        goo = mm(hoo, cv[...]).astype(BF).reshape(4, 2, 8, 128)
        for y in range(2):
            sg[:, y, p, GO:GO + 8] = goo[:, y]

    def sends(p, n):
        ps = pl.ds(p, n)
        out = [pltpu.make_async_remote_copy(
            src_ref=sg.at[:, 1 - core, ps, RS0:RS1], dst_ref=rs.at[:, ps],
            send_sem=ssem, recv_sem=rssem, device_id=(frag, sib), device_id_type=MESH)]
        for k, (c, q) in enumerate(peers):
            out.append(pltpu.make_async_remote_copy(
                src_ref=sg.at[chips[c], par[q], ps, 0:SENT], dst_ref=rg.at[me, ps, 0:SENT],
                send_sem=sgsem.at[k], recv_sem=rgsem.at[me],
                device_id=(frag, 2 * chips[c] + par[q]), device_id_type=MESH))
        return out

    def send(p, n):
        for c in sends(p, n):
            c.start()
        for q in range(n):
            rg[me, p + q, 0:SENT] = sg[chips[0], core, p + q, 0:SENT]

    if RS0 + RSA < RS1:
        sg[:, :, :, RS0 + RSA:RS1, :] = jnp.zeros((4, 2, NP, RS1 - RS0 - RSA, 128), BF)
    a_wait(0)
    a_start(NBUF - 1)
    step1(0)

    def body(p, carry):
        @pl.when(p + NBUF - 1 < NP)
        def _():
            a_start(p + NBUF - 1)

        @pl.when(p == 2)
        def _():
            send(0, 1)

        @pl.when((p > 2) & (lax.rem(p, 2) == 0))
        def _():
            send(p - 3, 2)

        a_wait(p)
        step23(p - 1)
        step1(p)
        return carry

    lax.fori_loop(1, NP, body, 0)
    send(NP - 2, 1)
    step23(NP - 1)
    send(NP - 1, 1)

    def rcopy(src, dst, ss, rr, dev):
        return pltpu.make_async_remote_copy(src_ref=src, dst_ref=dst, send_sem=ss, recv_sem=rr,
                                            device_id=(frag, dev), device_id_type=MESH)

    def bwait(view, sem):
        pltpu.make_async_copy(view, view, sem).wait()

    units = [(3, 0), (3, 1), (1, 0), (2, 0), (2, 1), (1, 1), (0, 0), (0, 1)]

    def part(buf, at, kc):
        return mm(kc, jnp.concatenate([buf[at + (slice(None), slice(r, r + 16))].reshape(240, 128)
                                       for r in range(0, 16 * HB, 16)], axis=1))

    for c, half in units:
        r = RS0 + 16 * HB * half
        w = part(sg.at[:, :, :, r:r + 16 * HB], (chips[c], core), k4c[0])
        for b in range(HB):
            sb[c, 128 * (HB * half + b):128 * (HB * half + b) + 128, :] = w[:, 128 * b:128 * b + 128]

    def half_rows(half):
        return slice(HALF * half, HALF * half + HALF)

    def rows(half, c):
        return slice(HALF * half + CH * c, HALF * half + CH * c + CH)

    def first(c, half):
        m = 1 if c == 3 else 0
        return rcopy(sb.at[c, half_rows(half)], p1.at[m, half_rows(half)], p1s.at[half, m], p1r.at[half, m],
                     (xn, yn)[half])

    sent_after = {1: (3, 0), 2: (3, 1), 3: (1, 0), 5: (2, 1)}
    bwait(rs, rssem)
    for n, (c, half) in enumerate(units):
        r = 16 * HB * half
        w = part(rs.at[:, :, r:r + 16 * HB], (chips[c],), k4c[1])
        for b in range(HB):
            at = slice(128 * (HB * half + b), 128 * (HB * half + b) + 128)
            sb[c, at, :] = sb[c, at, :] + w[:, 128 * b:128 * b + 128]
        if n in sent_after:
            first(*sent_after[n]).start()

    def put(w, a0):
        o2_ref[a0:a0 + w.shape[0]] = w[:, :, :NV]
        for k in range(VB):
            lo, hi = max(a0, 16 * k), min(a0 + w.shape[0], 16 * k + NV - GR)
            if lo < hi:
                n = min(GC, NV - GC * k)
                o2_ref[GR + lo - 16 * k:GR + hi - 16 * k, :, GC * k:GC * k + n] = w[lo - a0:hi - a0, :, NV:NV + n]

    for c in range(15):
        col = iota((128, 128), 1)
        w = mm(pi, one_hot(iota((128, 128), 0) == (col >> 4) + 8 * c))
        k4[:, c * 128:(c + 1) * 128] = jnp.where((iota((128, 128), 0) >> 3) == (col & 15), w, 0.0).astype(BF)
    e6[...] = one_hot((iota((128, 960), 1) >> 3) == iota((128, 960), 0))

    def v1_rows(t):
        row = iota((96, 128), 0) + 96 * t
        z = mm(one_hot((row >> 3) == iota((96, 128), 1)), cvt[...]).astype(BF)
        w = mm(z, e6[...])
        keep = (iota((96, 960), 0) & 7) == (iota((96, 960), 1) & 7)
        v1k[pl.ds(pl.multiple_of(96 * t, 96), 96), :] = jnp.where(keep, w, 0.0).astype(BF)

    def v1_build(t, carry):
        v1_rows(t)
        return carry

    lax.fori_loop(0, 9, v1_build, 0)
    for k in range(1, ND):
        src = lax.rem(me + k, ND)
        bwait(rg.at[src, :, 0:SENT], rgsem.at[src])

    v = rg[:, :, GO:GO + 8, :].reshape(960, 128)

    def v1_out(t, carry):
        w = mm(v1k[pl.ds(pl.multiple_of(96 * t, 96), 96), :], v)
        o1_ref[pl.ds(12 * t, 12)] = w.reshape(12, 8, 128)[:, :, :NV]
        return carry

    lax.fori_loop(0, 9, v1_out, 0)

    nx = -(-EX // 16)
    for ab in range(0, nx, 2):
        n = min(2, nx - ab)
        w = mm(k4[...], jnp.concatenate([rg[:, :, 16 * (ab + u):16 * (ab + u) + 16, :].reshape(1920, 128)
                                         for u in range(n)], axis=1)).reshape(16, 8, 128 * n)
        for u in range(n):
            put(w[:min(16, EX - 16 * (ab + u)), :, 128 * u:128 * u + 128], 16 * (ab + u))

    for half in range(2):
        bwait(p1.at[1, half_rows(half)], p1r.at[half, 1])
        z2[half_rows(half), :] = sb[2 - half, half_rows(half), :] + p1[1, half_rows(half), :]
    for c in range(NCH):
        for half in range(2):
            rcopy(z2.at[rows(half, c)], p2.at[rows(half, c)], p2s.at[half, c], p2r.at[half, c],
                  (yn, xn)[half]).start()
    for half in range(2):
        bwait(p1.at[0, half_rows(half)], p1r.at[half, 0])
        sb[0, half_rows(half), :] = sb[0, half_rows(half), :] + p1[0, half_rows(half), :]
    for c in range(NCH):
        for half in range(2):
            bwait(p2.at[rows(half, c)], p2r.at[half, c])
            w = sb[0, rows(half, c), :] + p2[rows(half, c), :]
            put(w.reshape(-1, 8, 128), EX + (HALF * half + CH * c) // 8)

    for k in range(ND - 1):
        bwait(rg.at[0, :, 0:SENT], sgsem.at[k])
    bwait(rs, ssem)
    for c in range(NCH):
        for half in range(2):
            bwait(p2.at[rows(half, c)], p2s.at[half, c])
    for m in range(2):
        for half in range(2):
            bwait(p1.at[m, half_rows(half)], p1s.at[half, m])


def write_out(x1_ref, x2_ref, y1_ref, y2_ref, sem):
    copies = [pltpu.make_async_copy(x1_ref, y1_ref, sem.at[0]), pltpu.make_async_copy(x2_ref, y2_ref, sem.at[1])]
    for c in copies:
        c.start()
    for c in copies:
        c.wait()


def solution(mesh):
    def local_part(ao, co, cv):
        a = ao.reshape(NP, ROWS, NQ)
        co, cv = (pltpu.with_memory_space_constraint(t.T, pltpu.HBM) for t in (co, cv))
        vm = pl.BlockSpec(memory_space=pltpu.VMEM)
        o1, o2 = pl.pallas_call(
            kernel,
            out_shape=[jax.ShapeDtypeStruct((NV, NO, NV), F32), jax.ShapeDtypeStruct((NV, NO, NV), F32)],
            in_specs=[pl.BlockSpec(memory_space=pltpu.HBM)] * 3,
            out_specs=[vm, vm],
            scratch_shapes=[
                pltpu.VMEM((NBUF, ROWS, NQ), BF),
                pltpu.VMEM((2, 8, 128, 128), BF),
                pltpu.VMEM((4, 2, NP, RS1, 128), BF),
                pltpu.VMEM((8, NP, RS0, 128), BF),
                pltpu.VMEM((4, NP, RS1 - RS0, 128), BF),
                pltpu.VMEM((4, 128 * RSB, 128), F32),
                pltpu.VMEM((2, RSR, 128), F32),
                pltpu.VMEM((RSR, 128), F32),
                pltpu.VMEM((RSR, 128), F32),
                pltpu.VMEM((64, 960), BF),
                pltpu.VMEM((128, 1920), BF),
                pltpu.VMEM((2, 128, 240), BF),
                pltpu.VMEM((864, 960), BF),
                pltpu.VMEM((128, 960), BF),
                pltpu.VMEM((NO, NQ), BF),
                pltpu.VMEM((NV, NQ), BF),
                pltpu.VMEM((16, 128), BF),
                pltpu.VMEM((128, 128), BF),
                pltpu.VMEM((128, 128), BF),
                pltpu.SemaphoreType.DMA((NBUF,)),
                pltpu.SemaphoreType.DMA((2,)),
                pltpu.SemaphoreType.DMA((ND,)),
                pltpu.SemaphoreType.DMA((ND,)),
                pltpu.SemaphoreType.DMA,
                pltpu.SemaphoreType.DMA,
                pltpu.SemaphoreType.DMA((2, 2)),
                pltpu.SemaphoreType.DMA((2, 2)),
                pltpu.SemaphoreType.DMA((2, NCH)),
                pltpu.SemaphoreType.DMA((2, NCH)),
            ],
            compiler_params=pltpu.CompilerParams(collective_id=0, has_side_effects=True,
                                                 vmem_limit_bytes=34 * 1024 * 1024),
            name='mo_blocks',
        )(a, co, cv)
        o1, o2 = pl.pallas_call(
            write_out,
            out_shape=[jax.ShapeDtypeStruct((NV, NO, NV), F32), jax.ShapeDtypeStruct((NV, NO, NV), F32)],
            in_specs=[vm, vm],
            out_specs=[pl.BlockSpec(memory_space=pltpu.HBM)] * 2,
            scratch_shapes=[pltpu.SemaphoreType.DMA((2,))],
            compiler_params=pltpu.CompilerParams(vmem_limit_bytes=2 * 1024 * 1024),
            name='write_out',
        )(o1, o2)
        return o1.transpose(0, 2, 1), o2.transpose(1, 0, 2)

    return jax.shard_map(local_part, mesh=mesh,
                         in_specs=(P(('frag', 'dev')), P('frag'), P('frag')),
                         out_specs=(P('frag', None, 'dev'), P('frag', None, 'dev')),
                         check_vma=False)
```

```python
import jax
import jax.numpy as jnp
from jax import lax
from jax.experimental import pallas as pl
from jax.experimental.pallas import tpu as pltpu
from jax.sharding import PartitionSpec as P

MESH = pl.DeviceIdType.MESH
BF = jnp.bfloat16
F32 = jnp.float32
ND = 8
NP = 15
NQ = 120
NO = 8
NV = 108
ROWS = NQ * NQ
NBUF = 4
SPLIT = 5
VB = 6
GR = 16 * VB
GC = 20
EX = 40
VB = 6
GR = 16 * VB
GC = 20
GO = EX
SENT = EX + 8
RS0 = -(-SENT // 16) * 16
RSA = GR - EX
RSB = -(-RSA // 16)
RS1 = RS0 + 16 * RSB
RSR = 8 * RSA
NCH = 2
HB = RSB // 2
HALF = RSR // 2
CH = HALF // NCH


def mm(a, b):
    return jnp.dot(a, b, preferred_element_type=F32)


def mm_nt(a, b):
    return lax.dot_general(a, b, (((1,), (1,)), ((), ())), preferred_element_type=F32)


def iota(shape, dim):
    return lax.broadcasted_iota(jnp.int32, shape, dim)


def one_hot(mask):
    return jnp.where(mask, 1.0, 0.0).astype(BF)


def kernel(a_ref, co_ref, cv_ref, o1_ref, o2_ref,
           abuf, tbuf, sg, rg, rs, sb, p1, z2, p2, k1, k4, k4c, v1k, e6, coin, cvin, cot, cvt, cv,
           asem, csem, sgsem, rgsem, ssem, rssem, p1s, p1r, p2s, p2r):
    me = lax.axis_index('dev')
    frag = lax.axis_index('frag')
    core = lax.rem(me, 2)
    mx = lax.rem(me // 2, 2)
    my = me // 4
    sib = me + 1 - 2 * core
    xn = me + 2 - 4 * mx
    yn = me + 4 - 8 * my
    dg = xn + 4 - 8 * my
    cols = [me, xn, yn, dg]
    chips = [c // 2 for c in cols]
    one = core * chips[1] + (1 - core) * chips[3]
    two = core * chips[3] + (1 - core) * chips[1]
    peers = [(one, 0), (chips[2], 0), (two, 0), (one, 1), (chips[2], 1), (two, 1), (chips[0], 1)]
    par = [core, 1 - core]

    def a_copies(p):
        slot = lax.rem(p, NBUF)
        step = ROWS // SPLIT
        return [pltpu.make_async_copy(a_ref.at[p, pl.ds(k * step, step)],
                                      abuf.at[slot, pl.ds(k * step, step)],
                                      asem.at[slot]) for k in range(SPLIT)]

    def a_start(p):
        for c in a_copies(p):
            c.start()

    def a_wait(p):
        slot = lax.rem(p, NBUF)
        pltpu.make_async_copy(a_ref.at[p], abuf.at[slot], asem.at[slot]).wait()

    cin = [pltpu.make_async_copy(co_ref, coin, csem.at[0]), pltpu.make_async_copy(cv_ref, cvin, csem.at[1])]
    for c in cin:
        c.start()
    for p in range(NBUF - 1):
        a_start(p)

    barrier = pltpu.get_barrier_semaphore()
    for k in range(1, ND):
        pl.semaphore_signal(barrier, inc=1, device_id=(frag, lax.rem(me + k, ND)), device_id_type=MESH)

    cot[...] = jnp.zeros(cot.shape, BF)
    cvt[...] = jnp.zeros(cvt.shape, BF)
    for c in cin:
        c.wait()
    cot[0:NO, 0:NQ] = coin[...]
    cvt[0:NV, 0:NQ] = cvin[...]
    cv[...] = mm_nt(one_hot(iota((128, 128), 0) == iota((128, 128), 1)), cvt[...]).astype(BF)
    xr = mm(one_hot((iota((64, 16), 0) >> 3) == iota((64, 16), 1)), cot[...]).astype(BF)
    diff = iota((128, 960), 1) - iota((128, 960), 0)
    hit = diff == 0
    for k in range(1, 8):
        hit = hit | (diff == 120 * k)
    off = iota((64, 960), 1) - 120 * (iota((64, 960), 0) & 7)
    k1[...] = jnp.where((off >= 0) & (off < 120), mm(xr, one_hot(hit)), 0.0).astype(BF)
    pi = mm(one_hot((iota((128, 16), 0) & 7) == iota((128, 16), 1)), cot[...]).astype(BF)
    for h, d in enumerate((me, sib)):
        col = iota((128, 240), 1)
        w = mm(pi, one_hot(iota((128, 240), 0) == (col >> 4) + NP * d))
        keep = (iota((128, 240), 0) >> 3) == (col & 15)
        k4c[h] = jnp.where(keep, w, 0.0).astype(BF)
    pl.semaphore_wait(barrier, ND - 1)

    def step1(p):
        slot = lax.rem(p, NBUF)
        tslot = lax.rem(p, 2)
        pad = jnp.zeros((960, 8), BF)
        for g in range(8):
            left = jnp.concatenate([abuf[slot, 1920 * g:1920 * g + 960, :], pad], axis=1)
            if g < 7:
                right = jnp.concatenate([abuf[slot, 1920 * g + 960:1920 * g + 1920, :], pad], axis=1)
                out = mm(k1[...], jnp.concatenate([left, right], axis=1))
                lo = out[:, :128].reshape(8, 8, 128)
                hi = out[:, 128:].reshape(8, 8, 128)
            else:
                lo = mm(k1[...], left).reshape(8, 8, 128)
                hi = jnp.zeros((8, 8, 128), F32)
            tbuf[tslot, :, 16 * g:16 * g + 16, :] = jnp.concatenate([lo, hi], axis=1).astype(BF)

    def step23(p):
        t = tbuf[lax.rem(p, 2)].reshape(1024, 128)
        h = mm(t, cv[...]).astype(BF).reshape(8, 128, 128)
        hoo = mm_nt(cot[...], t)
        lane = iota((16, 128), 1)
        for x in range(0, 8, 2):
            g = mm(cvt[0:112, :], jnp.concatenate([h[x], h[x + 1]], axis=1))
            for y in range(2):
                last = g[GR:GR + 16, 128 * y:128 * y + 128]
                tiles = [jnp.where(lane < NV, g[16 * k:16 * k + 16, 128 * y:128 * y + 128],
                                   pltpu.roll(last, (NV - GC * k) % 128, 1)) for k in range(VB)]
                tiles = jnp.concatenate(tiles, axis=0)
                sg[x // 2, y, p, 0:EX] = tiles[:EX].astype(BF)
                sg[x // 2, y, p, RS0:RS0 + RSA] = tiles[EX:].astype(BF)
        hoo = jnp.concatenate([hoo[0:8, 128 * x:128 * x + 128] for x in range(8)], axis=0).astype(BF)
        goo = mm(hoo, cv[...]).astype(BF).reshape(4, 2, 8, 128)
        for y in range(2):
            sg[:, y, p, GO:GO + 8] = goo[:, y]

    def sends(p):
        out = [pltpu.make_async_remote_copy(
            src_ref=sg.at[:, 1 - core, p, RS0:RS1], dst_ref=rs.at[:, p],
            send_sem=ssem, recv_sem=rssem, device_id=(frag, sib), device_id_type=MESH)]
        for k, (chip, q) in enumerate(peers):
            out.append(pltpu.make_async_remote_copy(
                src_ref=sg.at[chip, par[q], p, 0:SENT], dst_ref=rg.at[me, p, 0:SENT],
                send_sem=sgsem.at[k], recv_sem=rgsem.at[me],
                device_id=(frag, 2 * chip + par[q]), device_id_type=MESH))
        return out

    def send(p):
        for c in sends(p):
            c.start()
        rg[me, p, 0:SENT] = sg[chips[0], core, p, 0:SENT]

    if RS0 + RSA < RS1:
        sg[:, :, :, RS0 + RSA:RS1, :] = jnp.zeros((4, 2, NP, RS1 - RS0 - RSA, 128), BF)
    a_wait(0)
    a_start(NBUF - 1)
    step1(0)

    def body(p, carry):
        @pl.when(p + NBUF - 1 < NP)
        def _():
            a_start(p + NBUF - 1)

        @pl.when(p >= 2)
        def _():
            send(p - 2)

        a_wait(p)
        step23(p - 1)
        step1(p)
        return carry

    lax.fori_loop(1, NP, body, 0)
    send(NP - 2)
    step23(NP - 1)
    send(NP - 1)

    def rcopy(src, dst, ss, rr, dev):
        return pltpu.make_async_remote_copy(src_ref=src, dst_ref=dst, send_sem=ss, recv_sem=rr,
                                            device_id=(frag, dev), device_id_type=MESH)

    def bwait(view, sem):
        pltpu.make_async_copy(view, view, sem).wait()

    units = [(3, 0), (3, 1), (1, 0), (2, 0), (2, 1), (1, 1), (0, 0), (0, 1)]

    def part(buf, at, kc):
        return mm(kc, jnp.concatenate([buf[at + (slice(None), slice(r, r + 16))].reshape(240, 128)
                                       for r in range(0, 16 * HB, 16)], axis=1))

    for c, half in units:
        r = RS0 + 16 * HB * half
        w = part(sg.at[:, :, :, r:r + 16 * HB], (chips[c], core), k4c[0])
        for b in range(HB):
            sb[c, 128 * (HB * half + b):128 * (HB * half + b) + 128, :] = w[:, 128 * b:128 * b + 128]

    def half_rows(half):
        return slice(HALF * half, HALF * half + HALF)

    def rows(half, c):
        return slice(HALF * half + CH * c, HALF * half + CH * c + CH)

    def first(c, half):
        m = 1 if c == 3 else 0
        return rcopy(sb.at[c, half_rows(half)], p1.at[m, half_rows(half)], p1s.at[half, m], p1r.at[half, m],
                     (xn, yn)[half])

    sent_after = {1: (3, 0), 2: (3, 1), 3: (1, 0), 5: (2, 1)}
    bwait(rs, rssem)
    for n, (c, half) in enumerate(units):
        r = 16 * HB * half
        w = part(rs.at[:, :, r:r + 16 * HB], (chips[c],), k4c[1])
        for b in range(HB):
            at = slice(128 * (HB * half + b), 128 * (HB * half + b) + 128)
            sb[c, at, :] = sb[c, at, :] + w[:, 128 * b:128 * b + 128]
        if n in sent_after:
            first(*sent_after[n]).start()

    def put(w, a0):
        o2_ref[a0:a0 + w.shape[0]] = w[:, :, :NV]
        for k in range(VB):
            lo, hi = max(a0, 16 * k), min(a0 + w.shape[0], 16 * k + NV - GR)
            if lo < hi:
                n = min(GC, NV - GC * k)
                o2_ref[GR + lo - 16 * k:GR + hi - 16 * k, :, GC * k:GC * k + n] = w[lo - a0:hi - a0, :, NV:NV + n]

    for c in range(15):
        col = iota((128, 128), 1)
        w = mm(pi, one_hot(iota((128, 128), 0) == (col >> 4) + 8 * c))
        k4[:, c * 128:(c + 1) * 128] = jnp.where((iota((128, 128), 0) >> 3) == (col & 15), w, 0.0).astype(BF)
    e6[...] = one_hot((iota((128, 960), 1) >> 3) == iota((128, 960), 0))

    def v1_rows(t):
        row = iota((96, 128), 0) + 96 * t
        z = mm(one_hot((row >> 3) == iota((96, 128), 1)), cvt[...]).astype(BF)
        w = mm(z, e6[...])
        keep = (iota((96, 960), 0) & 7) == (iota((96, 960), 1) & 7)
        v1k[pl.ds(pl.multiple_of(96 * t, 96), 96), :] = jnp.where(keep, w, 0.0).astype(BF)

    def v1_build(t, carry):
        v1_rows(t)
        return carry

    lax.fori_loop(0, 9, v1_build, 0)
    for k in range(1, ND):
        src = lax.rem(me + k, ND)
        bwait(rg.at[src, :, 0:SENT], rgsem.at[src])

    v = rg[:, :, GO:GO + 8, :].reshape(960, 128)

    def v1_out(t, carry):
        w = mm(v1k[pl.ds(pl.multiple_of(96 * t, 96), 96), :], v)
        o1_ref[pl.ds(12 * t, 12)] = w.reshape(12, 8, 128)[:, :, :NV]
        return carry

    lax.fori_loop(0, 9, v1_out, 0)

    nx = -(-EX // 16)
    for ab in range(0, nx, 2):
        n = min(2, nx - ab)
        w = mm(k4[...], jnp.concatenate([rg[:, :, 16 * (ab + u):16 * (ab + u) + 16, :].reshape(1920, 128)
                                         for u in range(n)], axis=1)).reshape(16, 8, 128 * n)
        for u in range(n):
            put(w[:min(16, EX - 16 * (ab + u)), :, 128 * u:128 * u + 128], 16 * (ab + u))

    for half in range(2):
        bwait(p1.at[1, half_rows(half)], p1r.at[half, 1])
        z2[half_rows(half), :] = sb[2 - half, half_rows(half), :] + p1[1, half_rows(half), :]
    for c in range(NCH):
        for half in range(2):
            rcopy(z2.at[rows(half, c)], p2.at[rows(half, c)], p2s.at[half, c], p2r.at[half, c],
                  (yn, xn)[half]).start()
    for half in range(2):
        bwait(p1.at[0, half_rows(half)], p1r.at[half, 0])
        sb[0, half_rows(half), :] = sb[0, half_rows(half), :] + p1[0, half_rows(half), :]
    for c in range(NCH):
        for half in range(2):
            bwait(p2.at[rows(half, c)], p2r.at[half, c])
            w = sb[0, rows(half, c), :] + p2[rows(half, c), :]
            put(w.reshape(-1, 8, 128), EX + (HALF * half + CH * c) // 8)

    for k in range(ND - 1):
        bwait(rg.at[0, :, 0:SENT], sgsem.at[k])
    bwait(rs, ssem)
    for c in range(NCH):
        for half in range(2):
            bwait(p2.at[rows(half, c)], p2s.at[half, c])
    for m in range(2):
        for half in range(2):
            bwait(p1.at[m, half_rows(half)], p1s.at[half, m])


def write_out(x1_ref, x2_ref, y1_ref, y2_ref, sem):
    copies = [pltpu.make_async_copy(x1_ref, y1_ref, sem.at[0]), pltpu.make_async_copy(x2_ref, y2_ref, sem.at[1])]
    for c in copies:
        c.start()
    for c in copies:
        c.wait()


def solution(mesh):
    def local_part(ao, co, cv):
        a = ao.reshape(NP, ROWS, NQ)
        co, cv = (pltpu.with_memory_space_constraint(t.T, pltpu.HBM) for t in (co, cv))
        vm = pl.BlockSpec(memory_space=pltpu.VMEM)
        o1, o2 = pl.pallas_call(
            kernel,
            out_shape=[jax.ShapeDtypeStruct((NV, NO, NV), F32), jax.ShapeDtypeStruct((NV, NO, NV), F32)],
            in_specs=[pl.BlockSpec(memory_space=pltpu.HBM)] * 3,
            out_specs=[vm, vm],
            scratch_shapes=[
                pltpu.VMEM((NBUF, ROWS, NQ), BF),
                pltpu.VMEM((2, 8, 128, 128), BF),
                pltpu.VMEM((4, 2, NP, RS1, 128), BF),
                pltpu.VMEM((8, NP, RS0, 128), BF),
                pltpu.VMEM((4, NP, RS1 - RS0, 128), BF),
                pltpu.VMEM((4, 128 * RSB, 128), F32),
                pltpu.VMEM((2, RSR, 128), F32),
                pltpu.VMEM((RSR, 128), F32),
                pltpu.VMEM((RSR, 128), F32),
                pltpu.VMEM((64, 960), BF),
                pltpu.VMEM((128, 1920), BF),
                pltpu.VMEM((2, 128, 240), BF),
                pltpu.VMEM((864, 960), BF),
                pltpu.VMEM((128, 960), BF),
                pltpu.VMEM((NO, NQ), BF),
                pltpu.VMEM((NV, NQ), BF),
                pltpu.VMEM((16, 128), BF),
                pltpu.VMEM((128, 128), BF),
                pltpu.VMEM((128, 128), BF),
                pltpu.SemaphoreType.DMA((NBUF,)),
                pltpu.SemaphoreType.DMA((2,)),
                pltpu.SemaphoreType.DMA((ND,)),
                pltpu.SemaphoreType.DMA((ND,)),
                pltpu.SemaphoreType.DMA,
                pltpu.SemaphoreType.DMA,
                pltpu.SemaphoreType.DMA((2, 2)),
                pltpu.SemaphoreType.DMA((2, 2)),
                pltpu.SemaphoreType.DMA((2, NCH)),
                pltpu.SemaphoreType.DMA((2, NCH)),
            ],
            compiler_params=pltpu.CompilerParams(collective_id=0, has_side_effects=True,
                                                 vmem_limit_bytes=34 * 1024 * 1024),
            name='mo_blocks',
        )(a, co, cv)
        o1, o2 = pl.pallas_call(
            write_out,
            out_shape=[jax.ShapeDtypeStruct((NV, NO, NV), F32), jax.ShapeDtypeStruct((NV, NO, NV), F32)],
            in_specs=[vm, vm],
            out_specs=[pl.BlockSpec(memory_space=pltpu.HBM)] * 2,
            scratch_shapes=[pltpu.SemaphoreType.DMA((2,))],
            compiler_params=pltpu.CompilerParams(vmem_limit_bytes=2 * 1024 * 1024),
            name='write_out',
        )(o1, o2)
        return o1.transpose(0, 2, 1), o2.transpose(1, 0, 2)

    return jax.shard_map(local_part, mesh=mesh,
                         in_specs=(P(('frag', 'dev')), P('frag'), P('frag')),
                         out_specs=(P('frag', None, 'dev'), P('frag', None, 'dev')),
                         check_vma=False)
```

```python
import jax
import jax.numpy as jnp
from jax import lax
from jax.experimental import pallas as pl
from jax.experimental.pallas import tpu as pltpu
from jax.sharding import PartitionSpec as P

MESH = pl.DeviceIdType.MESH
BF = jnp.bfloat16
F32 = jnp.float32
ND = 8
NP = 15
NQ = 120
NO = 8
NV = 108
ROWS = NQ * NQ
NBUF = 4
SPLIT = 5
VB = 6
GR = 16 * VB
GC = 20
EX = 40
VB = 6
GR = 16 * VB
GC = 20
GO = EX
SENT = EX + 8
RS0 = -(-SENT // 16) * 16
RSA = GR - EX
RSB = -(-RSA // 16)
RS1 = RS0 + 16 * RSB
RSR = 8 * RSA
NCH = 2
HB = RSB // 2
HALF = RSR // 2
CH = HALF // NCH


def mm(a, b):
    return jnp.dot(a, b, preferred_element_type=F32)


def mm_nt(a, b):
    return lax.dot_general(a, b, (((1,), (1,)), ((), ())), preferred_element_type=F32)


def iota(shape, dim):
    return lax.broadcasted_iota(jnp.int32, shape, dim)


def one_hot(mask):
    return jnp.where(mask, 1.0, 0.0).astype(BF)


def kernel(a_ref, co_ref, cv_ref, o1_ref, o2_ref,
           abuf, tbuf, sg, rg, rs, sb, p1, z2, p2, k1, k4, k4c, v1k, e6, coin, cvin, cot, cvt, cv,
           asem, csem, sgsem, rgsem, ssem, rssem, p1s, p1r, p2s, p2r):
    me = lax.axis_index('dev')
    frag = lax.axis_index('frag')
    core = lax.rem(me, 2)
    mx = lax.rem(me // 2, 2)
    my = me // 4
    sib = me + 1 - 2 * core
    xn = me + 2 - 4 * mx
    yn = me + 4 - 8 * my
    dg = xn + 4 - 8 * my
    cols = [me, xn, yn, dg]
    chips = [c // 2 for c in cols]
    one = core * chips[1] + (1 - core) * chips[3]
    two = core * chips[3] + (1 - core) * chips[1]
    peers = [(one, 0), (chips[2], 0), (two, 0), (one, 1), (chips[2], 1), (two, 1), (chips[0], 1)]
    par = [core, 1 - core]

    def a_copies(p):
        slot = lax.rem(p, NBUF)
        step = ROWS // SPLIT
        return [pltpu.make_async_copy(a_ref.at[p, pl.ds(k * step, step)],
                                      abuf.at[slot, pl.ds(k * step, step)],
                                      asem.at[slot]) for k in range(SPLIT)]

    def a_start(p):
        for c in a_copies(p):
            c.start()

    def a_wait(p):
        slot = lax.rem(p, NBUF)
        pltpu.make_async_copy(a_ref.at[p], abuf.at[slot], asem.at[slot]).wait()

    cin = [pltpu.make_async_copy(co_ref, coin, csem.at[0]), pltpu.make_async_copy(cv_ref, cvin, csem.at[1])]
    for c in cin:
        c.start()
    for p in range(NBUF - 1):
        a_start(p)

    barrier = pltpu.get_barrier_semaphore()
    for k in range(1, ND):
        pl.semaphore_signal(barrier, inc=1, device_id=(frag, lax.rem(me + k, ND)), device_id_type=MESH)

    cot[...] = jnp.zeros(cot.shape, BF)
    cvt[...] = jnp.zeros(cvt.shape, BF)
    for c in cin:
        c.wait()
    cot[0:NO, 0:NQ] = coin[...]
    cvt[0:NV, 0:NQ] = cvin[...]
    cv[...] = mm_nt(one_hot(iota((128, 128), 0) == iota((128, 128), 1)), cvt[...]).astype(BF)
    xr = mm(one_hot((iota((64, 16), 0) >> 3) == iota((64, 16), 1)), cot[...]).astype(BF)
    diff = iota((128, 960), 1) - iota((128, 960), 0)
    hit = diff == 0
    for k in range(1, 8):
        hit = hit | (diff == 120 * k)
    off = iota((64, 960), 1) - 120 * (iota((64, 960), 0) & 7)
    k1[...] = jnp.where((off >= 0) & (off < 120), mm(xr, one_hot(hit)), 0.0).astype(BF)
    pi = mm(one_hot((iota((128, 16), 0) & 7) == iota((128, 16), 1)), cot[...]).astype(BF)
    for h, d in enumerate((me, sib)):
        col = iota((128, 240), 1)
        w = mm(pi, one_hot(iota((128, 240), 0) == (col >> 4) + NP * d))
        keep = (iota((128, 240), 0) >> 3) == (col & 15)
        k4c[h] = jnp.where(keep, w, 0.0).astype(BF)
    pl.semaphore_wait(barrier, ND - 1)

    def step1(p):
        slot = lax.rem(p, NBUF)
        tslot = lax.rem(p, 2)
        pad = jnp.zeros((960, 8), BF)
        for g in range(8):
            left = jnp.concatenate([abuf[slot, 1920 * g:1920 * g + 960, :], pad], axis=1)
            if g < 7:
                right = jnp.concatenate([abuf[slot, 1920 * g + 960:1920 * g + 1920, :], pad], axis=1)
                out = mm(k1[...], jnp.concatenate([left, right], axis=1))
                lo = out[:, :128].reshape(8, 8, 128)
                hi = out[:, 128:].reshape(8, 8, 128)
            else:
                lo = mm(k1[...], left).reshape(8, 8, 128)
                hi = jnp.zeros((8, 8, 128), F32)
            tbuf[tslot, :, 16 * g:16 * g + 16, :] = jnp.concatenate([lo, hi], axis=1).astype(BF)

    def step23(p):
        t = tbuf[lax.rem(p, 2)].reshape(1024, 128)
        h = mm(t, cv[...]).astype(BF).reshape(8, 128, 128)
        hoo = mm_nt(cot[...], t)
        lane = iota((16, 128), 1)
        for x in range(0, 8, 2):
            g = mm(cvt[0:112, :], jnp.concatenate([h[x], h[x + 1]], axis=1))
            for y in range(2):
                last = g[GR:GR + 16, 128 * y:128 * y + 128]
                tiles = [jnp.where(lane < NV, g[16 * k:16 * k + 16, 128 * y:128 * y + 128],
                                   pltpu.roll(last, (NV - GC * k) % 128, 1)) for k in range(VB)]
                tiles = jnp.concatenate(tiles, axis=0)
                sg[x // 2, y, p, 0:EX] = tiles[:EX].astype(BF)
                sg[x // 2, y, p, RS0:RS0 + RSA] = tiles[EX:].astype(BF)
        hoo = jnp.concatenate([hoo[0:8, 128 * x:128 * x + 128] for x in range(8)], axis=0).astype(BF)
        goo = mm(hoo, cv[...]).astype(BF).reshape(4, 2, 8, 128)
        for y in range(2):
            sg[:, y, p, GO:GO + 8] = goo[:, y]

    def sends(p):
        out = [pltpu.make_async_remote_copy(
            src_ref=sg.at[:, 1 - core, p, RS0:RS1], dst_ref=rs.at[:, p],
            send_sem=ssem, recv_sem=rssem, device_id=(frag, sib), device_id_type=MESH)]
        for k, (chip, q) in enumerate(peers):
            out.append(pltpu.make_async_remote_copy(
                src_ref=sg.at[chip, par[q], p, 0:SENT], dst_ref=rg.at[me, p, 0:SENT],
                send_sem=sgsem.at[k], recv_sem=rgsem.at[me],
                device_id=(frag, 2 * chip + par[q]), device_id_type=MESH))
        return out

    def send(p):
        for c in sends(p):
            c.start()
        rg[me, p, 0:SENT] = sg[chips[0], core, p, 0:SENT]

    if RS0 + RSA < RS1:
        sg[:, :, :, RS0 + RSA:RS1, :] = jnp.zeros((4, 2, NP, RS1 - RS0 - RSA, 128), BF)
    a_wait(0)
    a_start(NBUF - 1)
    step1(0)

    def body(p, carry):
        @pl.when(p + NBUF - 1 < NP)
        def _():
            a_start(p + NBUF - 1)

        @pl.when(p >= 2)
        def _():
            send(p - 2)

        a_wait(p)
        step23(p - 1)
        step1(p)
        return carry

    lax.fori_loop(1, NP, body, 0)
    send(NP - 2)
    step23(NP - 1)
    send(NP - 1)

    def rcopy(src, dst, ss, rr, dev):
        return pltpu.make_async_remote_copy(src_ref=src, dst_ref=dst, send_sem=ss, recv_sem=rr,
                                            device_id=(frag, dev), device_id_type=MESH)

    def bwait(view, sem):
        pltpu.make_async_copy(view, view, sem).wait()

    units = [(3, 0), (3, 1), (1, 0), (2, 0), (2, 1), (1, 1), (0, 0), (0, 1)]

    def part(buf, at, kc):
        return mm(kc, jnp.concatenate([buf[at + (slice(None), slice(r, r + 16))].reshape(240, 128)
                                       for r in range(0, 16 * HB, 16)], axis=1))

    for c, half in units:
        r = RS0 + 16 * HB * half
        w = part(sg.at[:, :, :, r:r + 16 * HB], (chips[c], core), k4c[0])
        for b in range(HB):
            sb[c, 128 * (HB * half + b):128 * (HB * half + b) + 128, :] = w[:, 128 * b:128 * b + 128]

    def half_rows(half):
        return slice(HALF * half, HALF * half + HALF)

    def rows(half, c):
        return slice(HALF * half + CH * c, HALF * half + CH * c + CH)

    def first(c, half):
        m = 1 if c == 3 else 0
        return rcopy(sb.at[c, half_rows(half)], p1.at[m, half_rows(half)], p1s.at[half, m], p1r.at[half, m],
                     (xn, yn)[half])

    sent_after = {1: (3, 0), 2: (3, 1)}
    bwait(rs, rssem)
    for n, (c, half) in enumerate(units):
        r = 16 * HB * half
        w = part(rs.at[:, :, r:r + 16 * HB], (chips[c],), k4c[1])
        for b in range(HB):
            at = slice(128 * (HB * half + b), 128 * (HB * half + b) + 128)
            sb[c, at, :] = sb[c, at, :] + w[:, 128 * b:128 * b + 128]
        if n in sent_after:
            first(*sent_after[n]).start()

    def put(w, a0):
        o2_ref[a0:a0 + w.shape[0]] = w[:, :, :NV]
        for k in range(VB):
            lo, hi = max(a0, 16 * k), min(a0 + w.shape[0], 16 * k + NV - GR)
            if lo < hi:
                n = min(GC, NV - GC * k)
                o2_ref[GR + lo - 16 * k:GR + hi - 16 * k, :, GC * k:GC * k + n] = w[lo - a0:hi - a0, :, NV:NV + n]

    for c in range(15):
        col = iota((128, 128), 1)
        w = mm(pi, one_hot(iota((128, 128), 0) == (col >> 4) + 8 * c))
        k4[:, c * 128:(c + 1) * 128] = jnp.where((iota((128, 128), 0) >> 3) == (col & 15), w, 0.0).astype(BF)
    e6[...] = one_hot((iota((128, 960), 1) >> 3) == iota((128, 960), 0))

    def v1_rows(t):
        row = iota((96, 128), 0) + 96 * t
        z = mm(one_hot((row >> 3) == iota((96, 128), 1)), cvt[...]).astype(BF)
        w = mm(z, e6[...])
        keep = (iota((96, 960), 0) & 7) == (iota((96, 960), 1) & 7)
        v1k[pl.ds(pl.multiple_of(96 * t, 96), 96), :] = jnp.where(keep, w, 0.0).astype(BF)

    def v1_build(t, carry):
        v1_rows(t)
        return carry

    lax.fori_loop(0, 9, v1_build, 0)
    for half, col in ((0, 1), (1, 2)):
        bwait(p1.at[1, half_rows(half)], p1s.at[half, 1])
        first(col, half).start()
    for k in range(1, ND):
        src = lax.rem(me + k, ND)
        bwait(rg.at[src, :, 0:SENT], rgsem.at[src])

    v = rg[:, :, GO:GO + 8, :].reshape(960, 128)

    def v1_out(t, carry):
        w = mm(v1k[pl.ds(pl.multiple_of(96 * t, 96), 96), :], v)
        o1_ref[pl.ds(12 * t, 12)] = w.reshape(12, 8, 128)[:, :, :NV]
        return carry

    lax.fori_loop(0, 9, v1_out, 0)

    nx = -(-EX // 16)
    for ab in range(0, nx, 2):
        n = min(2, nx - ab)
        w = mm(k4[...], jnp.concatenate([rg[:, :, 16 * (ab + u):16 * (ab + u) + 16, :].reshape(1920, 128)
                                         for u in range(n)], axis=1)).reshape(16, 8, 128 * n)
        for u in range(n):
            put(w[:min(16, EX - 16 * (ab + u)), :, 128 * u:128 * u + 128], 16 * (ab + u))

    for half in range(2):
        bwait(p1.at[1, half_rows(half)], p1r.at[half, 1])
        z2[half_rows(half), :] = sb[2 - half, half_rows(half), :] + p1[1, half_rows(half), :]
    for c in range(NCH):
        for half in range(2):
            rcopy(z2.at[rows(half, c)], p2.at[rows(half, c)], p2s.at[half, c], p2r.at[half, c],
                  (yn, xn)[half]).start()
    for half in range(2):
        bwait(p1.at[0, half_rows(half)], p1r.at[half, 0])
        sb[0, half_rows(half), :] = sb[0, half_rows(half), :] + p1[0, half_rows(half), :]
    for c in range(NCH):
        for half in range(2):
            bwait(p2.at[rows(half, c)], p2r.at[half, c])
            w = sb[0, rows(half, c), :] + p2[rows(half, c), :]
            put(w.reshape(-1, 8, 128), EX + (HALF * half + CH * c) // 8)

    for k in range(ND - 1):
        bwait(rg.at[0, :, 0:SENT], sgsem.at[k])
    bwait(rs, ssem)
    for c in range(NCH):
        for half in range(2):
            bwait(p2.at[rows(half, c)], p2s.at[half, c])
    for half in range(2):
        bwait(p1.at[0, half_rows(half)], p1s.at[half, 0])


def write_out(x1_ref, x2_ref, y1_ref, y2_ref, sem):
    copies = [pltpu.make_async_copy(x1_ref, y1_ref, sem.at[0]), pltpu.make_async_copy(x2_ref, y2_ref, sem.at[1])]
    for c in copies:
        c.start()
    for c in copies:
        c.wait()


def solution(mesh):
    def local_part(ao, co, cv):
        a = ao.reshape(NP, ROWS, NQ)
        co, cv = (pltpu.with_memory_space_constraint(t.T, pltpu.HBM) for t in (co, cv))
        vm = pl.BlockSpec(memory_space=pltpu.VMEM)
        o1, o2 = pl.pallas_call(
            kernel,
            out_shape=[jax.ShapeDtypeStruct((NV, NO, NV), F32), jax.ShapeDtypeStruct((NV, NO, NV), F32)],
            in_specs=[pl.BlockSpec(memory_space=pltpu.HBM)] * 3,
            out_specs=[vm, vm],
            scratch_shapes=[
                pltpu.VMEM((NBUF, ROWS, NQ), BF),
                pltpu.VMEM((2, 8, 128, 128), BF),
                pltpu.VMEM((4, 2, NP, RS1, 128), BF),
                pltpu.VMEM((8, NP, RS0, 128), BF),
                pltpu.VMEM((4, NP, RS1 - RS0, 128), BF),
                pltpu.VMEM((4, 128 * RSB, 128), F32),
                pltpu.VMEM((2, RSR, 128), F32),
                pltpu.VMEM((RSR, 128), F32),
                pltpu.VMEM((RSR, 128), F32),
                pltpu.VMEM((64, 960), BF),
                pltpu.VMEM((128, 1920), BF),
                pltpu.VMEM((2, 128, 240), BF),
                pltpu.VMEM((864, 960), BF),
                pltpu.VMEM((128, 960), BF),
                pltpu.VMEM((NO, NQ), BF),
                pltpu.VMEM((NV, NQ), BF),
                pltpu.VMEM((16, 128), BF),
                pltpu.VMEM((128, 128), BF),
                pltpu.VMEM((128, 128), BF),
                pltpu.SemaphoreType.DMA((NBUF,)),
                pltpu.SemaphoreType.DMA((2,)),
                pltpu.SemaphoreType.DMA((ND,)),
                pltpu.SemaphoreType.DMA((ND,)),
                pltpu.SemaphoreType.DMA,
                pltpu.SemaphoreType.DMA,
                pltpu.SemaphoreType.DMA((2, 2)),
                pltpu.SemaphoreType.DMA((2, 2)),
                pltpu.SemaphoreType.DMA((2, NCH)),
                pltpu.SemaphoreType.DMA((2, NCH)),
            ],
            compiler_params=pltpu.CompilerParams(collective_id=0, has_side_effects=True,
                                                 vmem_limit_bytes=34 * 1024 * 1024),
            name='mo_blocks',
        )(a, co, cv)
        o1, o2 = pl.pallas_call(
            write_out,
            out_shape=[jax.ShapeDtypeStruct((NV, NO, NV), F32), jax.ShapeDtypeStruct((NV, NO, NV), F32)],
            in_specs=[vm, vm],
            out_specs=[pl.BlockSpec(memory_space=pltpu.HBM)] * 2,
            scratch_shapes=[pltpu.SemaphoreType.DMA((2,))],
            compiler_params=pltpu.CompilerParams(vmem_limit_bytes=2 * 1024 * 1024),
            name='write_out',
        )(o1, o2)
        return o1.transpose(0, 2, 1), o2.transpose(1, 0, 2)

    return jax.shard_map(local_part, mesh=mesh,
                         in_specs=(P(('frag', 'dev')), P('frag'), P('frag')),
                         out_specs=(P('frag', None, 'dev'), P('frag', None, 'dev')),
                         check_vma=False)
```

```python
import jax
import jax.numpy as jnp
from jax import lax
from jax.experimental import pallas as pl
from jax.experimental.pallas import tpu as pltpu
from jax.sharding import PartitionSpec as P

MESH = pl.DeviceIdType.MESH
BF = jnp.bfloat16
F32 = jnp.float32
ND = 8
NP = 15
NQ = 120
NO = 8
NV = 108
ROWS = NQ * NQ
NBUF = 4
SPLIT = 5
VB = 6
GR = 16 * VB
GC = 20
EX = 40
VB = 6
GR = 16 * VB
GC = 20
GO = EX
SENT = EX + 8
RS0 = -(-SENT // 16) * 16
RSA = GR - EX
RSB = -(-RSA // 16)
RS1 = RS0 + 16 * RSB
RSR = 8 * RSA
NCH = 2
HB = RSB // 2
HALF = RSR // 2
CH = HALF // NCH


def mm(a, b):
    return jnp.dot(a, b, preferred_element_type=F32)


def mm_nt(a, b):
    return lax.dot_general(a, b, (((1,), (1,)), ((), ())), preferred_element_type=F32)


def iota(shape, dim):
    return lax.broadcasted_iota(jnp.int32, shape, dim)


def one_hot(mask):
    return jnp.where(mask, 1.0, 0.0).astype(BF)


def kernel(a_ref, co_ref, cv_ref, o1_ref, o2_ref,
           abuf, ta, tb, sg, rg, rs, sb, p1, z2, p2, k1, k4, k4c, v1k, e6, coin, cvin, cot, cvt, cv,
           asem, csem, sgsem, rgsem, ssem, rssem, p1s, p1r, p2s, p2r):
    me = lax.axis_index('dev')
    frag = lax.axis_index('frag')
    core = lax.rem(me, 2)
    mx = lax.rem(me // 2, 2)
    my = me // 4
    sib = me + 1 - 2 * core
    xn = me + 2 - 4 * mx
    yn = me + 4 - 8 * my
    dg = xn + 4 - 8 * my
    cols = [me, xn, yn, dg]
    chips = [c // 2 for c in cols]
    one = core * chips[1] + (1 - core) * chips[3]
    two = core * chips[3] + (1 - core) * chips[1]
    peers = [(one, 0), (chips[2], 0), (two, 0), (one, 1), (chips[2], 1), (two, 1), (chips[0], 1)]
    par = [core, 1 - core]

    def a_copies(p):
        slot = lax.rem(p, NBUF)
        step = ROWS // SPLIT
        return [pltpu.make_async_copy(a_ref.at[p, pl.ds(k * step, step)],
                                      abuf.at[slot, pl.ds(k * step, step)],
                                      asem.at[slot]) for k in range(SPLIT)]

    def a_start(p):
        for c in a_copies(p):
            c.start()

    def a_wait(p):
        slot = lax.rem(p, NBUF)
        pltpu.make_async_copy(a_ref.at[p], abuf.at[slot], asem.at[slot]).wait()

    cin = [pltpu.make_async_copy(co_ref, coin, csem.at[0]), pltpu.make_async_copy(cv_ref, cvin, csem.at[1])]
    for c in cin:
        c.start()
    for p in range(NBUF - 1):
        a_start(p)

    barrier = pltpu.get_barrier_semaphore()
    for k in range(1, ND):
        pl.semaphore_signal(barrier, inc=1, device_id=(frag, lax.rem(me + k, ND)), device_id_type=MESH)

    cot[...] = jnp.zeros(cot.shape, BF)
    cvt[...] = jnp.zeros(cvt.shape, BF)
    for c in cin:
        c.wait()
    cot[0:NO, 0:NQ] = coin[...]
    cvt[0:NV, 0:NQ] = cvin[...]
    cv[...] = mm_nt(one_hot(iota((128, 128), 0) == iota((128, 128), 1)), cvt[...]).astype(BF)
    xr = mm(one_hot((iota((64, 16), 0) >> 3) == iota((64, 16), 1)), cot[...]).astype(BF)
    diff = iota((128, 960), 1) - iota((128, 960), 0)
    hit = diff == 0
    for k in range(1, 8):
        hit = hit | (diff == 120 * k)
    off = iota((64, 960), 1) - 120 * (iota((64, 960), 0) & 7)
    k1[...] = jnp.where((off >= 0) & (off < 120), mm(xr, one_hot(hit)), 0.0).astype(BF)
    pi = mm(one_hot((iota((128, 16), 0) & 7) == iota((128, 16), 1)), cot[...]).astype(BF)
    for h, d in enumerate((me, sib)):
        col = iota((128, 240), 1)
        w = mm(pi, one_hot(iota((128, 240), 0) == (col >> 4) + NP * d))
        keep = (iota((128, 240), 0) >> 3) == (col & 15)
        k4c[h] = jnp.where(keep, w, 0.0).astype(BF)
    pl.semaphore_wait(barrier, ND - 1)

    pad = jnp.zeros((960, 8), BF)
    lane = iota((16, 128), 1)

    def step1(p, t, g):
        slot = lax.rem(p, NBUF)
        left = jnp.concatenate([abuf[slot, 1920 * g:1920 * g + 960, :], pad], axis=1)
        if g < 7:
            right = jnp.concatenate([abuf[slot, 1920 * g + 960:1920 * g + 1920, :], pad], axis=1)
            out = mm(k1[...], jnp.concatenate([left, right], axis=1))
            lo = out[:, :128].reshape(8, 8, 128)
            hi = out[:, 128:].reshape(8, 8, 128)
        else:
            lo = mm(k1[...], left).reshape(8, 8, 128)
            hi = jnp.zeros((8, 8, 128), F32)
        t[:, 16 * g:16 * g + 16, :] = jnp.concatenate([lo, hi], axis=1).astype(BF)

    def step2(t, x):
        h = mm(t[x:x + 2].reshape(256, 128), cv[...]).astype(BF)
        return jnp.concatenate([h[:128], h[128:]], axis=1)

    def step3(p, x, h):
        g = mm(cvt[0:112, :], h)
        for y in range(2):
            last = g[GR:GR + 16, 128 * y:128 * y + 128]
            tiles = [jnp.where(lane < NV, g[16 * k:16 * k + 16, 128 * y:128 * y + 128],
                               pltpu.roll(last, (NV - GC * k) % 128, 1)) for k in range(VB)]
            tiles = jnp.concatenate(tiles, axis=0)
            sg[x // 2, y, p, 0:EX] = tiles[:EX].astype(BF)
            sg[x // 2, y, p, RS0:RS0 + RSA] = tiles[EX:].astype(BF)

    def step2o(t):
        hoo = mm_nt(cot[...], t[...].reshape(1024, 128))
        return jnp.concatenate([hoo[0:8, 128 * x:128 * x + 128] for x in range(8)], axis=0).astype(BF)

    def step3o(p, hoo):
        goo = mm(hoo, cv[...]).astype(BF).reshape(4, 2, 8, 128)
        for y in range(2):
            sg[:, y, p, GO:GO + 8] = goo[:, y]

    def work(p, told, tnew):
        def one(g):
            if tnew is not None:
                step1(p, tnew, g)

        h0 = step2(told, 0)
        one(0)
        h1 = step2(told, 2)
        one(1)
        step3(p - 1, 0, h0)
        h2 = step2(told, 4)
        one(2)
        step3(p - 1, 2, h1)
        h3 = step2(told, 6)
        one(3)
        step3(p - 1, 4, h2)
        hoo = step2o(told)
        one(4)
        step3(p - 1, 6, h3)
        one(5)
        step3o(p - 1, hoo)
        one(6)
        one(7)

    def sends(p):
        out = [pltpu.make_async_remote_copy(
            src_ref=sg.at[:, 1 - core, p, RS0:RS1], dst_ref=rs.at[:, p],
            send_sem=ssem, recv_sem=rssem, device_id=(frag, sib), device_id_type=MESH)]
        for k, (chip, q) in enumerate(peers):
            out.append(pltpu.make_async_remote_copy(
                src_ref=sg.at[chip, par[q], p, 0:SENT], dst_ref=rg.at[me, p, 0:SENT],
                send_sem=sgsem.at[k], recv_sem=rgsem.at[me],
                device_id=(frag, 2 * chip + par[q]), device_id_type=MESH))
        return out

    def send(p):
        for c in sends(p):
            c.start()
        rg[me, p, 0:SENT] = sg[chips[0], core, p, 0:SENT]

    if RS0 + RSA < RS1:
        sg[:, :, :, RS0 + RSA:RS1, :] = jnp.zeros((4, 2, NP, RS1 - RS0 - RSA, 128), BF)
    a_wait(0)
    a_start(NBUF - 1)
    for g in range(8):
        step1(0, ta, g)

    def body(k, carry):
        for p, told, tnew in ((2 * k + 1, ta, tb), (2 * k + 2, tb, ta)):
            @pl.when(p + NBUF - 1 < NP)
            def _():
                a_start(p + NBUF - 1)

            @pl.when(p >= 2)
            def _():
                send(p - 2)

            a_wait(p)
            work(p, told, tnew)
        return carry

    lax.fori_loop(0, NP // 2, body, 0)
    send(NP - 2)
    work(NP, ta, None)
    send(NP - 1)

    def rcopy(src, dst, ss, rr, dev):
        return pltpu.make_async_remote_copy(src_ref=src, dst_ref=dst, send_sem=ss, recv_sem=rr,
                                            device_id=(frag, dev), device_id_type=MESH)

    def bwait(view, sem):
        pltpu.make_async_copy(view, view, sem).wait()

    units = [(3, 0), (3, 1), (1, 0), (2, 0), (2, 1), (1, 1), (0, 0), (0, 1)]

    def part(buf, at, kc):
        return mm(kc, jnp.concatenate([buf[at + (slice(None), slice(r, r + 16))].reshape(240, 128)
                                       for r in range(0, 16 * HB, 16)], axis=1))

    for c, half in units:
        r = RS0 + 16 * HB * half
        w = part(sg.at[:, :, :, r:r + 16 * HB], (chips[c], core), k4c[0])
        for b in range(HB):
            sb[c, 128 * (HB * half + b):128 * (HB * half + b) + 128, :] = w[:, 128 * b:128 * b + 128]

    def half_rows(half):
        return slice(HALF * half, HALF * half + HALF)

    def rows(half, c):
        return slice(HALF * half + CH * c, HALF * half + CH * c + CH)

    def first(c, half):
        m = 1 if c == 3 else 0
        return rcopy(sb.at[c, half_rows(half)], p1.at[m, half_rows(half)], p1s.at[half, m], p1r.at[half, m],
                     (xn, yn)[half])

    sent_after = {1: (3, 0), 2: (3, 1)}
    bwait(rs, rssem)
    for n, (c, half) in enumerate(units):
        r = 16 * HB * half
        w = part(rs.at[:, :, r:r + 16 * HB], (chips[c],), k4c[1])
        for b in range(HB):
            at = slice(128 * (HB * half + b), 128 * (HB * half + b) + 128)
            sb[c, at, :] = sb[c, at, :] + w[:, 128 * b:128 * b + 128]
        if n in sent_after:
            first(*sent_after[n]).start()

    def put(w, a0):
        o2_ref[a0:a0 + w.shape[0]] = w[:, :, :NV]
        for k in range(VB):
            lo, hi = max(a0, 16 * k), min(a0 + w.shape[0], 16 * k + NV - GR)
            if lo < hi:
                n = min(GC, NV - GC * k)
                o2_ref[GR + lo - 16 * k:GR + hi - 16 * k, :, GC * k:GC * k + n] = w[lo - a0:hi - a0, :, NV:NV + n]

    for c in range(15):
        col = iota((128, 128), 1)
        w = mm(pi, one_hot(iota((128, 128), 0) == (col >> 4) + 8 * c))
        k4[:, c * 128:(c + 1) * 128] = jnp.where((iota((128, 128), 0) >> 3) == (col & 15), w, 0.0).astype(BF)
    e6[...] = one_hot((iota((128, 960), 1) >> 3) == iota((128, 960), 0))

    def v1_rows(t):
        row = iota((96, 128), 0) + 96 * t
        z = mm(one_hot((row >> 3) == iota((96, 128), 1)), cvt[...]).astype(BF)
        w = mm(z, e6[...])
        keep = (iota((96, 960), 0) & 7) == (iota((96, 960), 1) & 7)
        v1k[pl.ds(pl.multiple_of(96 * t, 96), 96), :] = jnp.where(keep, w, 0.0).astype(BF)

    def v1_build(t, carry):
        v1_rows(t)
        return carry

    lax.fori_loop(0, 9, v1_build, 0)
    for half, col in ((0, 1), (1, 2)):
        bwait(p1.at[1, half_rows(half)], p1s.at[half, 1])
        first(col, half).start()
    for k in range(1, ND):
        src = lax.rem(me + k, ND)
        bwait(rg.at[src, :, 0:SENT], rgsem.at[src])

    v = rg[:, :, GO:GO + 8, :].reshape(960, 128)

    def v1_out(t, carry):
        w = mm(v1k[pl.ds(pl.multiple_of(96 * t, 96), 96), :], v)
        o1_ref[pl.ds(12 * t, 12)] = w.reshape(12, 8, 128)[:, :, :NV]
        return carry

    lax.fori_loop(0, 9, v1_out, 0)

    nx = -(-EX // 16)
    for ab in range(0, nx, 2):
        n = min(2, nx - ab)
        w = mm(k4[...], jnp.concatenate([rg[:, :, 16 * (ab + u):16 * (ab + u) + 16, :].reshape(1920, 128)
                                         for u in range(n)], axis=1)).reshape(16, 8, 128 * n)
        for u in range(n):
            put(w[:min(16, EX - 16 * (ab + u)), :, 128 * u:128 * u + 128], 16 * (ab + u))

    for half in range(2):
        bwait(p1.at[1, half_rows(half)], p1r.at[half, 1])
        z2[half_rows(half), :] = sb[2 - half, half_rows(half), :] + p1[1, half_rows(half), :]
    for c in range(NCH):
        for half in range(2):
            rcopy(z2.at[rows(half, c)], p2.at[rows(half, c)], p2s.at[half, c], p2r.at[half, c],
                  (yn, xn)[half]).start()
    for half in range(2):
        bwait(p1.at[0, half_rows(half)], p1r.at[half, 0])
        sb[0, half_rows(half), :] = sb[0, half_rows(half), :] + p1[0, half_rows(half), :]
    for c in range(NCH):
        for half in range(2):
            bwait(p2.at[rows(half, c)], p2r.at[half, c])
            w = sb[0, rows(half, c), :] + p2[rows(half, c), :]
            put(w.reshape(-1, 8, 128), EX + (HALF * half + CH * c) // 8)

    for k in range(ND - 1):
        bwait(rg.at[0, :, 0:SENT], sgsem.at[k])
    bwait(rs, ssem)
    for c in range(NCH):
        for half in range(2):
            bwait(p2.at[rows(half, c)], p2s.at[half, c])
    for half in range(2):
        bwait(p1.at[0, half_rows(half)], p1s.at[half, 0])


def write_out(x1_ref, x2_ref, y1_ref, y2_ref, sem):
    copies = [pltpu.make_async_copy(x1_ref, y1_ref, sem.at[0]), pltpu.make_async_copy(x2_ref, y2_ref, sem.at[1])]
    for c in copies:
        c.start()
    for c in copies:
        c.wait()


def solution(mesh):
    def local_part(ao, co, cv):
        a = ao.reshape(NP, ROWS, NQ)
        co, cv = (pltpu.with_memory_space_constraint(t.T, pltpu.HBM) for t in (co, cv))
        vm = pl.BlockSpec(memory_space=pltpu.VMEM)
        o1, o2 = pl.pallas_call(
            kernel,
            out_shape=[jax.ShapeDtypeStruct((NV, NO, NV), F32), jax.ShapeDtypeStruct((NV, NO, NV), F32)],
            in_specs=[pl.BlockSpec(memory_space=pltpu.HBM)] * 3,
            out_specs=[vm, vm],
            scratch_shapes=[
                pltpu.VMEM((NBUF, ROWS, NQ), BF),
                pltpu.VMEM((8, 128, 128), BF),
                pltpu.VMEM((8, 128, 128), BF),
                pltpu.VMEM((4, 2, NP, RS1, 128), BF),
                pltpu.VMEM((8, NP, RS0, 128), BF),
                pltpu.VMEM((4, NP, RS1 - RS0, 128), BF),
                pltpu.VMEM((4, 128 * RSB, 128), F32),
                pltpu.VMEM((2, RSR, 128), F32),
                pltpu.VMEM((RSR, 128), F32),
                pltpu.VMEM((RSR, 128), F32),
                pltpu.VMEM((64, 960), BF),
                pltpu.VMEM((128, 1920), BF),
                pltpu.VMEM((2, 128, 240), BF),
                pltpu.VMEM((864, 960), BF),
                pltpu.VMEM((128, 960), BF),
                pltpu.VMEM((NO, NQ), BF),
                pltpu.VMEM((NV, NQ), BF),
                pltpu.VMEM((16, 128), BF),
                pltpu.VMEM((128, 128), BF),
                pltpu.VMEM((128, 128), BF),
                pltpu.SemaphoreType.DMA((NBUF,)),
                pltpu.SemaphoreType.DMA((2,)),
                pltpu.SemaphoreType.DMA((ND,)),
                pltpu.SemaphoreType.DMA((ND,)),
                pltpu.SemaphoreType.DMA,
                pltpu.SemaphoreType.DMA,
                pltpu.SemaphoreType.DMA((2, 2)),
                pltpu.SemaphoreType.DMA((2, 2)),
                pltpu.SemaphoreType.DMA((2, NCH)),
                pltpu.SemaphoreType.DMA((2, NCH)),
            ],
            compiler_params=pltpu.CompilerParams(collective_id=0, has_side_effects=True,
                                                 vmem_limit_bytes=34 * 1024 * 1024),
            name='mo_blocks',
        )(a, co, cv)
        o1, o2 = pl.pallas_call(
            write_out,
            out_shape=[jax.ShapeDtypeStruct((NV, NO, NV), F32), jax.ShapeDtypeStruct((NV, NO, NV), F32)],
            in_specs=[vm, vm],
            out_specs=[pl.BlockSpec(memory_space=pltpu.HBM)] * 2,
            scratch_shapes=[pltpu.SemaphoreType.DMA((2,))],
            compiler_params=pltpu.CompilerParams(vmem_limit_bytes=2 * 1024 * 1024),
            name='write_out',
        )(o1, o2)
        return o1.transpose(0, 2, 1), o2.transpose(1, 0, 2)

    return jax.shard_map(local_part, mesh=mesh,
                         in_specs=(P(('frag', 'dev')), P('frag'), P('frag')),
                         out_specs=(P('frag', None, 'dev'), P('frag', None, 'dev')),
                         check_vma=False)
```

```python
import jax
import jax.numpy as jnp
from jax import lax
from jax.experimental import pallas as pl
from jax.experimental.pallas import tpu as pltpu
from jax.sharding import PartitionSpec as P

MESH = pl.DeviceIdType.MESH
BF = jnp.bfloat16
F32 = jnp.float32
ND = 8
NP = 15
NQ = 120
NO = 8
NV = 108
ROWS = NQ * NQ
NBUF = 4
PIECES = [0, 3840, 7680, 11520, ROWS]
VB = 6
GR = 16 * VB
GC = 20
EX = 40
VB = 6
GR = 16 * VB
GC = 20
GO = EX
SENT = EX + 8
RS0 = -(-SENT // 16) * 16
RSA = GR - EX
RSB = -(-RSA // 16)
RS1 = RS0 + 16 * RSB
RSR = 8 * RSA
NCH = 2
HB = RSB // 2
HALF = RSR // 2
CH = HALF // NCH


def mm(a, b):
    return jnp.dot(a, b, preferred_element_type=F32)


def mm_nt(a, b):
    return lax.dot_general(a, b, (((1,), (1,)), ((), ())), preferred_element_type=F32)


def iota(shape, dim):
    return lax.broadcasted_iota(jnp.int32, shape, dim)


def one_hot(mask):
    return jnp.where(mask, 1.0, 0.0).astype(BF)


def kernel(a_ref, co_ref, cv_ref, o1_ref, o2_ref,
           abuf, ta, tb, sg, rg, rs, sb, p1, z2, p2, k1, k4, k4c, v1k, e6, coin, cvin, cot, cvt, cv,
           asem, csem, sgsem, rgsem, ssem, rssem, p1s, p1r, p2s, p2r):
    me = lax.axis_index('dev')
    frag = lax.axis_index('frag')
    core = lax.rem(me, 2)
    mx = lax.rem(me // 2, 2)
    my = me // 4
    sib = me + 1 - 2 * core
    xn = me + 2 - 4 * mx
    yn = me + 4 - 8 * my
    dg = xn + 4 - 8 * my
    cols = [me, xn, yn, dg]
    chips = [c // 2 for c in cols]
    one = core * chips[1] + (1 - core) * chips[3]
    two = core * chips[3] + (1 - core) * chips[1]
    peers = [(one, 0), (chips[2], 0), (two, 0), (one, 1), (chips[2], 1), (two, 1), (chips[0], 1)]
    par = [core, 1 - core]

    def a_copy(p, k):
        slot = lax.rem(p, NBUF)
        r = slice(PIECES[k], PIECES[k + 1])
        return pltpu.make_async_copy(a_ref.at[p, r], abuf.at[slot, r], asem.at[slot, k])

    def a_start(p):
        for k in range(4):
            a_copy(p, k).start()

    def a_wait(p, parts=range(4)):
        for k in parts:
            a_copy(p, k).wait()

    cin = [pltpu.make_async_copy(co_ref, coin, csem.at[0]), pltpu.make_async_copy(cv_ref, cvin, csem.at[1])]
    for c in cin:
        c.start()
    for p in range(NBUF - 1):
        a_start(p)

    barrier = pltpu.get_barrier_semaphore()
    for k in range(1, ND):
        pl.semaphore_signal(barrier, inc=1, device_id=(frag, lax.rem(me + k, ND)), device_id_type=MESH)

    cot[...] = jnp.zeros(cot.shape, BF)
    cvt[...] = jnp.zeros(cvt.shape, BF)
    for c in cin:
        c.wait()
    cot[0:NO, 0:NQ] = coin[...]
    cvt[0:NV, 0:NQ] = cvin[...]
    cv[...] = mm_nt(one_hot(iota((128, 128), 0) == iota((128, 128), 1)), cvt[...]).astype(BF)
    xr = mm(one_hot((iota((64, 16), 0) >> 3) == iota((64, 16), 1)), cot[...]).astype(BF)
    diff = iota((128, 960), 1) - iota((128, 960), 0)
    hit = diff == 0
    for k in range(1, 8):
        hit = hit | (diff == 120 * k)
    off = iota((64, 960), 1) - 120 * (iota((64, 960), 0) & 7)
    k1[...] = jnp.where((off >= 0) & (off < 120), mm(xr, one_hot(hit)), 0.0).astype(BF)
    pi = mm(one_hot((iota((128, 16), 0) & 7) == iota((128, 16), 1)), cot[...]).astype(BF)
    for h, d in enumerate((me, sib)):
        col = iota((128, 240), 1)
        w = mm(pi, one_hot(iota((128, 240), 0) == (col >> 4) + NP * d))
        keep = (iota((128, 240), 0) >> 3) == (col & 15)
        k4c[h] = jnp.where(keep, w, 0.0).astype(BF)
    pl.semaphore_wait(barrier, ND - 1)

    pad = jnp.zeros((960, 8), BF)
    lane = iota((16, 128), 1)

    def step1(p, t, g):
        slot = lax.rem(p, NBUF)
        left = jnp.concatenate([abuf[slot, 1920 * g:1920 * g + 960, :], pad], axis=1)
        if g < 7:
            right = jnp.concatenate([abuf[slot, 1920 * g + 960:1920 * g + 1920, :], pad], axis=1)
            out = mm(k1[...], jnp.concatenate([left, right], axis=1))
            lo = out[:, :128].reshape(8, 8, 128)
            hi = out[:, 128:].reshape(8, 8, 128)
        else:
            lo = mm(k1[...], left).reshape(8, 8, 128)
            hi = jnp.zeros((8, 8, 128), F32)
        t[:, 16 * g:16 * g + 16, :] = jnp.concatenate([lo, hi], axis=1).astype(BF)

    def step2(t, x):
        h = mm(t[x:x + 2].reshape(256, 128), cv[...]).astype(BF)
        return jnp.concatenate([h[:128], h[128:]], axis=1)

    def step3(p, x, h):
        g = mm(cvt[0:112, :], h)
        for y in range(2):
            last = g[GR:GR + 16, 128 * y:128 * y + 128]
            tiles = [jnp.where(lane < NV, g[16 * k:16 * k + 16, 128 * y:128 * y + 128],
                               pltpu.roll(last, (NV - GC * k) % 128, 1)) for k in range(VB)]
            tiles = jnp.concatenate(tiles, axis=0)
            sg[x // 2, y, p, 0:EX] = tiles[:EX].astype(BF)
            sg[x // 2, y, p, RS0:RS0 + RSA] = tiles[EX:].astype(BF)

    def step2o(t):
        hoo = mm_nt(cot[...], t[...].reshape(1024, 128))
        return jnp.concatenate([hoo[0:8, 128 * x:128 * x + 128] for x in range(8)], axis=0).astype(BF)

    def step3o(p, hoo):
        goo = mm(hoo, cv[...]).astype(BF).reshape(4, 2, 8, 128)
        for y in range(2):
            sg[:, y, p, GO:GO + 8] = goo[:, y]

    def work(p, told, tnew, late=False):
        def one(g):
            if tnew is not None:
                step1(p, tnew, g)

        h0 = step2(told, 0)
        one(0)
        h1 = step2(told, 2)
        one(1)
        step3(p - 1, 0, h0)
        h2 = step2(told, 4)
        one(2)
        step3(p - 1, 2, h1)
        h3 = step2(told, 6)
        one(3)
        step3(p - 1, 4, h2)
        hoo = step2o(told)
        if late:
            a_wait(p, (2, 3))
        one(4)
        step3(p - 1, 6, h3)
        one(5)
        step3o(p - 1, hoo)
        one(6)
        one(7)

    def pair_copy(p):
        return pltpu.make_async_remote_copy(
            src_ref=sg.at[:, 1 - core, p, RS0:RS1], dst_ref=rs.at[:, p],
            send_sem=ssem, recv_sem=rssem, device_id=(frag, sib), device_id_type=MESH)

    def exchange(p):
        for k, (chip, q) in enumerate(peers):
            pltpu.make_async_remote_copy(
                src_ref=sg.at[chip, par[q], p, 0:SENT], dst_ref=rg.at[me, p, 0:SENT],
                send_sem=sgsem.at[k], recv_sem=rgsem.at[me],
                device_id=(frag, 2 * chip + par[q]), device_id_type=MESH).start()
        rg[me, p, 0:SENT] = sg[chips[0], core, p, 0:SENT]

    def send(p):
        pair_copy(p).start()
        exchange(p)

    if RS0 + RSA < RS1:
        sg[:, :, :, RS0 + RSA:RS1, :] = jnp.zeros((4, 2, NP, RS1 - RS0 - RSA, 128), BF)
    a_wait(0)
    a_start(NBUF - 1)
    for g in range(8):
        step1(0, ta, g)

    def body(k, carry):
        for p, told, tnew in ((2 * k + 1, ta, tb), (2 * k + 2, tb, ta)):
            a_start(p + NBUF - 1)
            if told is ta:
                @pl.when(k > 0)
                def _():
                    send(p - 2)
            else:
                send(p - 2)
            a_wait(p)
            work(p, told, tnew)
        return carry

    lax.fori_loop(0, (NP - NBUF) // 2, body, 0)
    for p in range((NP - NBUF) // 2 * 2 + 1, NP):
        told, tnew = (ta, tb) if p % 2 else (tb, ta)
        if p + NBUF - 1 < NP:
            a_start(p + NBUF - 1)
        send(p - 2)
        if p < NP - 1:
            a_wait(p)
            work(p, told, tnew)
        else:
            a_wait(p, (0, 1))
            work(p, told, tnew, late=True)
    pair_copy(NP - 2).start()
    work(NP, ta, None)
    pair_copy(NP - 1).start()
    exchange(NP - 2)
    exchange(NP - 1)

    def rcopy(src, dst, ss, rr, dev):
        return pltpu.make_async_remote_copy(src_ref=src, dst_ref=dst, send_sem=ss, recv_sem=rr,
                                            device_id=(frag, dev), device_id_type=MESH)

    def bwait(view, sem):
        pltpu.make_async_copy(view, view, sem).wait()

    units = [(3, 0), (3, 1), (1, 0), (2, 0), (2, 1), (1, 1), (0, 0), (0, 1)]

    def part(buf, at, kc):
        return mm(kc, jnp.concatenate([buf[at + (slice(None), slice(r, r + 16))].reshape(240, 128)
                                       for r in range(0, 16 * HB, 16)], axis=1))

    for c, half in units:
        r = RS0 + 16 * HB * half
        w = part(sg.at[:, :, :, r:r + 16 * HB], (chips[c], core), k4c[0])
        for b in range(HB):
            sb[c, 128 * (HB * half + b):128 * (HB * half + b) + 128, :] = w[:, 128 * b:128 * b + 128]

    def half_rows(half):
        return slice(HALF * half, HALF * half + HALF)

    def rows(half, c):
        return slice(HALF * half + CH * c, HALF * half + CH * c + CH)

    def first(c, half):
        m = 1 if c == 3 else 0
        return rcopy(sb.at[c, half_rows(half)], p1.at[m, half_rows(half)], p1s.at[half, m], p1r.at[half, m],
                     (xn, yn)[half])

    sent_after = {1: (3, 0), 2: (3, 1)}
    bwait(rs, rssem)
    for n, (c, half) in enumerate(units):
        r = 16 * HB * half
        w = part(rs.at[:, :, r:r + 16 * HB], (chips[c],), k4c[1])
        for b in range(HB):
            at = slice(128 * (HB * half + b), 128 * (HB * half + b) + 128)
            sb[c, at, :] = sb[c, at, :] + w[:, 128 * b:128 * b + 128]
        if n in sent_after:
            first(*sent_after[n]).start()

    def put(w, a0):
        o2_ref[a0:a0 + w.shape[0]] = w[:, :, :NV]
        for k in range(VB):
            lo, hi = max(a0, 16 * k), min(a0 + w.shape[0], 16 * k + NV - GR)
            if lo < hi:
                n = min(GC, NV - GC * k)
                o2_ref[GR + lo - 16 * k:GR + hi - 16 * k, :, GC * k:GC * k + n] = w[lo - a0:hi - a0, :, NV:NV + n]

    for c in range(15):
        col = iota((128, 128), 1)
        w = mm(pi, one_hot(iota((128, 128), 0) == (col >> 4) + 8 * c))
        k4[:, c * 128:(c + 1) * 128] = jnp.where((iota((128, 128), 0) >> 3) == (col & 15), w, 0.0).astype(BF)
    e6[...] = one_hot((iota((128, 960), 1) >> 3) == iota((128, 960), 0))

    def v1_rows(t):
        row = iota((96, 128), 0) + 96 * t
        z = mm(one_hot((row >> 3) == iota((96, 128), 1)), cvt[...]).astype(BF)
        w = mm(z, e6[...])
        keep = (iota((96, 960), 0) & 7) == (iota((96, 960), 1) & 7)
        v1k[pl.ds(pl.multiple_of(96 * t, 96), 96), :] = jnp.where(keep, w, 0.0).astype(BF)

    def v1_build(t, carry):
        v1_rows(t)
        return carry

    lax.fori_loop(0, 9, v1_build, 0)
    for half, col in ((0, 1), (1, 2)):
        bwait(p1.at[1, half_rows(half)], p1s.at[half, 1])
        first(col, half).start()
    for k in range(1, ND):
        src = lax.rem(me + k, ND)
        bwait(rg.at[src, :, 0:SENT], rgsem.at[src])

    v = rg[:, :, GO:GO + 8, :].reshape(960, 128)

    def v1_out(t, carry):
        w = mm(v1k[pl.ds(pl.multiple_of(96 * t, 96), 96), :], v)
        o1_ref[pl.ds(12 * t, 12)] = w.reshape(12, 8, 128)[:, :, :NV]
        return carry

    lax.fori_loop(0, 9, v1_out, 0)

    nx = -(-EX // 16)
    for ab in range(0, nx, 2):
        n = min(2, nx - ab)
        w = mm(k4[...], jnp.concatenate([rg[:, :, 16 * (ab + u):16 * (ab + u) + 16, :].reshape(1920, 128)
                                         for u in range(n)], axis=1)).reshape(16, 8, 128 * n)
        for u in range(n):
            put(w[:min(16, EX - 16 * (ab + u)), :, 128 * u:128 * u + 128], 16 * (ab + u))

    for half in range(2):
        bwait(p1.at[1, half_rows(half)], p1r.at[half, 1])
        z2[half_rows(half), :] = sb[2 - half, half_rows(half), :] + p1[1, half_rows(half), :]
    for c in range(NCH):
        for half in range(2):
            rcopy(z2.at[rows(half, c)], p2.at[rows(half, c)], p2s.at[half, c], p2r.at[half, c],
                  (yn, xn)[half]).start()
    for half in range(2):
        bwait(p1.at[0, half_rows(half)], p1r.at[half, 0])
        sb[0, half_rows(half), :] = sb[0, half_rows(half), :] + p1[0, half_rows(half), :]
    for c in range(NCH):
        for half in range(2):
            bwait(p2.at[rows(half, c)], p2r.at[half, c])
            w = sb[0, rows(half, c), :] + p2[rows(half, c), :]
            put(w.reshape(-1, 8, 128), EX + (HALF * half + CH * c) // 8)

    for k in range(ND - 1):
        bwait(rg.at[0, :, 0:SENT], sgsem.at[k])
    bwait(rs, ssem)
    for c in range(NCH):
        for half in range(2):
            bwait(p2.at[rows(half, c)], p2s.at[half, c])
    for half in range(2):
        bwait(p1.at[0, half_rows(half)], p1s.at[half, 0])


def write_out(x1_ref, x2_ref, y1_ref, y2_ref, sem):
    copies = [pltpu.make_async_copy(x1_ref, y1_ref, sem.at[0]), pltpu.make_async_copy(x2_ref, y2_ref, sem.at[1])]
    for c in copies:
        c.start()
    for c in copies:
        c.wait()


def solution(mesh):
    def local_part(ao, co, cv):
        a = ao.reshape(NP, ROWS, NQ)
        co, cv = (pltpu.with_memory_space_constraint(t.T, pltpu.HBM) for t in (co, cv))
        vm = pl.BlockSpec(memory_space=pltpu.VMEM)
        o1, o2 = pl.pallas_call(
            kernel,
            out_shape=[jax.ShapeDtypeStruct((NV, NO, NV), F32), jax.ShapeDtypeStruct((NV, NO, NV), F32)],
            in_specs=[pl.BlockSpec(memory_space=pltpu.HBM)] * 3,
            out_specs=[vm, vm],
            scratch_shapes=[
                pltpu.VMEM((NBUF, ROWS, NQ), BF),
                pltpu.VMEM((8, 128, 128), BF),
                pltpu.VMEM((8, 128, 128), BF),
                pltpu.VMEM((4, 2, NP, RS1, 128), BF),
                pltpu.VMEM((8, NP, RS0, 128), BF),
                pltpu.VMEM((4, NP, RS1 - RS0, 128), BF),
                pltpu.VMEM((4, 128 * RSB, 128), F32),
                pltpu.VMEM((2, RSR, 128), F32),
                pltpu.VMEM((RSR, 128), F32),
                pltpu.VMEM((RSR, 128), F32),
                pltpu.VMEM((64, 960), BF),
                pltpu.VMEM((128, 1920), BF),
                pltpu.VMEM((2, 128, 240), BF),
                pltpu.VMEM((864, 960), BF),
                pltpu.VMEM((128, 960), BF),
                pltpu.VMEM((NO, NQ), BF),
                pltpu.VMEM((NV, NQ), BF),
                pltpu.VMEM((16, 128), BF),
                pltpu.VMEM((128, 128), BF),
                pltpu.VMEM((128, 128), BF),
                pltpu.SemaphoreType.DMA((NBUF, 4)),
                pltpu.SemaphoreType.DMA((2,)),
                pltpu.SemaphoreType.DMA((ND,)),
                pltpu.SemaphoreType.DMA((ND,)),
                pltpu.SemaphoreType.DMA,
                pltpu.SemaphoreType.DMA,
                pltpu.SemaphoreType.DMA((2, 2)),
                pltpu.SemaphoreType.DMA((2, 2)),
                pltpu.SemaphoreType.DMA((2, NCH)),
                pltpu.SemaphoreType.DMA((2, NCH)),
            ],
            compiler_params=pltpu.CompilerParams(collective_id=0, has_side_effects=True,
                                                 vmem_limit_bytes=34 * 1024 * 1024),
            name='mo_blocks',
        )(a, co, cv)
        o1, o2 = pl.pallas_call(
            write_out,
            out_shape=[jax.ShapeDtypeStruct((NV, NO, NV), F32), jax.ShapeDtypeStruct((NV, NO, NV), F32)],
            in_specs=[vm, vm],
            out_specs=[pl.BlockSpec(memory_space=pltpu.HBM)] * 2,
            scratch_shapes=[pltpu.SemaphoreType.DMA((2,))],
            compiler_params=pltpu.CompilerParams(vmem_limit_bytes=2 * 1024 * 1024),
            name='write_out',
        )(o1, o2)
        return o1.transpose(0, 2, 1), o2.transpose(1, 0, 2)

    return jax.shard_map(local_part, mesh=mesh,
                         in_specs=(P(('frag', 'dev')), P('frag'), P('frag')),
                         out_specs=(P('frag', None, 'dev'), P('frag', None, 'dev')),
                         check_vma=False)
```

```python
import jax
import jax.numpy as jnp
from jax import lax
from jax.experimental import pallas as pl
from jax.experimental.pallas import tpu as pltpu
from jax.sharding import PartitionSpec as P

MESH = pl.DeviceIdType.MESH
BF = jnp.bfloat16
F32 = jnp.float32
ND = 8
NP = 15
NQ = 120
NO = 8
NV = 108
ROWS = NQ * NQ
NBUF = 4
SPLIT = 5
VB = 6
GR = 16 * VB
GC = 20
EX = 32
VB = 6
GR = 16 * VB
GC = 20
GO = EX
SENT = EX + 8
RS0 = -(-SENT // 16) * 16
RSA = GR - EX
RSB = -(-RSA // 16)
RS1 = RS0 + 16 * RSB
RSR = 8 * RSA
NCH = 2
HB = RSB // 2
HALF = RSR // 2
CH = HALF // NCH


def mm(a, b):
    return jnp.dot(a, b, preferred_element_type=F32)


def mm_nt(a, b):
    return lax.dot_general(a, b, (((1,), (1,)), ((), ())), preferred_element_type=F32)


def iota(shape, dim):
    return lax.broadcasted_iota(jnp.int32, shape, dim)


def one_hot(mask):
    return jnp.where(mask, 1.0, 0.0).astype(BF)


def kernel(a_ref, co_ref, cv_ref, o1_ref, o2_ref,
           abuf, ta, tb, sg, rg, rs, sb, p1, z2, p2, k1, k4, k4c, v1k, e6, coin, cvin, cot, cvt, cv,
           asem, csem, sgsem, rgsem, ssem, rssem, p1s, p1r, p2s, p2r):
    me = lax.axis_index('dev')
    frag = lax.axis_index('frag')
    core = lax.rem(me, 2)
    mx = lax.rem(me // 2, 2)
    my = me // 4
    sib = me + 1 - 2 * core
    xn = me + 2 - 4 * mx
    yn = me + 4 - 8 * my
    dg = xn + 4 - 8 * my
    cols = [me, xn, yn, dg]
    chips = [c // 2 for c in cols]
    one = core * chips[1] + (1 - core) * chips[3]
    two = core * chips[3] + (1 - core) * chips[1]
    peers = [(one, 0), (chips[2], 0), (two, 0), (one, 1), (chips[2], 1), (two, 1), (chips[0], 1)]
    par = [core, 1 - core]

    def a_copies(p):
        slot = lax.rem(p, NBUF)
        step = ROWS // SPLIT
        return [pltpu.make_async_copy(a_ref.at[p, pl.ds(k * step, step)],
                                      abuf.at[slot, pl.ds(k * step, step)],
                                      asem.at[slot]) for k in range(SPLIT)]

    def a_start(p):
        for c in a_copies(p):
            c.start()

    def a_wait(p):
        slot = lax.rem(p, NBUF)
        pltpu.make_async_copy(a_ref.at[p], abuf.at[slot], asem.at[slot]).wait()

    cin = [pltpu.make_async_copy(co_ref, coin, csem.at[0]), pltpu.make_async_copy(cv_ref, cvin, csem.at[1])]
    for c in cin:
        c.start()
    for p in range(NBUF - 1):
        a_start(p)

    barrier = pltpu.get_barrier_semaphore()
    for k in range(1, ND):
        pl.semaphore_signal(barrier, inc=1, device_id=(frag, lax.rem(me + k, ND)), device_id_type=MESH)

    cot[...] = jnp.zeros(cot.shape, BF)
    cvt[...] = jnp.zeros(cvt.shape, BF)
    for c in cin:
        c.wait()
    cot[0:NO, 0:NQ] = coin[...]
    cvt[0:NV, 0:NQ] = cvin[...]
    cv[...] = mm_nt(one_hot(iota((128, 128), 0) == iota((128, 128), 1)), cvt[...]).astype(BF)
    xr = mm(one_hot((iota((64, 16), 0) >> 3) == iota((64, 16), 1)), cot[...]).astype(BF)
    diff = iota((128, 960), 1) - iota((128, 960), 0)
    hit = diff == 0
    for k in range(1, 8):
        hit = hit | (diff == 120 * k)
    off = iota((64, 960), 1) - 120 * (iota((64, 960), 0) & 7)
    k1[...] = jnp.where((off >= 0) & (off < 120), mm(xr, one_hot(hit)), 0.0).astype(BF)
    pi = mm(one_hot((iota((128, 16), 0) & 7) == iota((128, 16), 1)), cot[...]).astype(BF)
    for h, d in enumerate((me, sib)):
        col = iota((128, 240), 1)
        w = mm(pi, one_hot(iota((128, 240), 0) == (col >> 4) + NP * d))
        keep = (iota((128, 240), 0) >> 3) == (col & 15)
        k4c[h] = jnp.where(keep, w, 0.0).astype(BF)
    pl.semaphore_wait(barrier, ND - 1)

    pad = jnp.zeros((960, 8), BF)
    lane = iota((16, 128), 1)

    def step1(p, t, g):
        slot = lax.rem(p, NBUF)
        left = jnp.concatenate([abuf[slot, 1920 * g:1920 * g + 960, :], pad], axis=1)
        if g < 7:
            right = jnp.concatenate([abuf[slot, 1920 * g + 960:1920 * g + 1920, :], pad], axis=1)
            out = mm(k1[...], jnp.concatenate([left, right], axis=1))
            lo = out[:, :128].reshape(8, 8, 128)
            hi = out[:, 128:].reshape(8, 8, 128)
        else:
            lo = mm(k1[...], left).reshape(8, 8, 128)
            hi = jnp.zeros((8, 8, 128), F32)
        t[:, 16 * g:16 * g + 16, :] = jnp.concatenate([lo, hi], axis=1).astype(BF)

    def step2(t, x):
        h = mm(t[x:x + 2].reshape(256, 128), cv[...]).astype(BF)
        return jnp.concatenate([h[:128], h[128:]], axis=1)

    def step3(p, x, h):
        g = mm(cvt[0:112, :], h)
        for y in range(2):
            last = g[GR:GR + 16, 128 * y:128 * y + 128]
            tiles = [jnp.where(lane < NV, g[16 * k:16 * k + 16, 128 * y:128 * y + 128],
                               pltpu.roll(last, (NV - GC * k) % 128, 1)) for k in range(VB)]
            tiles = jnp.concatenate(tiles, axis=0)
            sg[x // 2, y, p, 0:EX] = tiles[:EX].astype(BF)
            sg[x // 2, y, p, RS0:RS0 + RSA] = tiles[EX:].astype(BF)

    def step2o(t):
        hoo = mm_nt(cot[...], t[...].reshape(1024, 128))
        return jnp.concatenate([hoo[0:8, 128 * x:128 * x + 128] for x in range(8)], axis=0).astype(BF)

    def step3o(p, hoo):
        goo = mm(hoo, cv[...]).astype(BF).reshape(4, 2, 8, 128)
        for y in range(2):
            sg[:, y, p, GO:GO + 8] = goo[:, y]

    def work(p, told, tnew):
        def one(g):
            if tnew is not None:
                step1(p, tnew, g)

        h0 = step2(told, 0)
        one(0)
        h1 = step2(told, 2)
        one(1)
        step3(p - 1, 0, h0)
        h2 = step2(told, 4)
        one(2)
        step3(p - 1, 2, h1)
        h3 = step2(told, 6)
        one(3)
        step3(p - 1, 4, h2)
        hoo = step2o(told)
        one(4)
        step3(p - 1, 6, h3)
        one(5)
        step3o(p - 1, hoo)
        one(6)
        one(7)

    def sends(p):
        out = [pltpu.make_async_remote_copy(
            src_ref=sg.at[:, 1 - core, p, RS0:RS1], dst_ref=rs.at[:, p],
            send_sem=ssem, recv_sem=rssem, device_id=(frag, sib), device_id_type=MESH)]
        for k, (chip, q) in enumerate(peers):
            out.append(pltpu.make_async_remote_copy(
                src_ref=sg.at[chip, par[q], p, 0:SENT], dst_ref=rg.at[me, p, 0:SENT],
                send_sem=sgsem.at[k], recv_sem=rgsem.at[me],
                device_id=(frag, 2 * chip + par[q]), device_id_type=MESH))
        return out

    def send(p):
        for c in sends(p):
            c.start()
        rg[me, p, 0:SENT] = sg[chips[0], core, p, 0:SENT]

    if RS0 + RSA < RS1:
        sg[:, :, :, RS0 + RSA:RS1, :] = jnp.zeros((4, 2, NP, RS1 - RS0 - RSA, 128), BF)
    a_wait(0)
    a_start(NBUF - 1)
    for g in range(8):
        step1(0, ta, g)

    def body(k, carry):
        for p, told, tnew in ((2 * k + 1, ta, tb), (2 * k + 2, tb, ta)):
            @pl.when(p + NBUF - 1 < NP)
            def _():
                a_start(p + NBUF - 1)

            @pl.when(p >= 2)
            def _():
                send(p - 2)

            a_wait(p)
            work(p, told, tnew)
        return carry

    lax.fori_loop(0, NP // 2, body, 0)
    send(NP - 2)
    work(NP, ta, None)
    send(NP - 1)

    def rcopy(src, dst, ss, rr, dev):
        return pltpu.make_async_remote_copy(src_ref=src, dst_ref=dst, send_sem=ss, recv_sem=rr,
                                            device_id=(frag, dev), device_id_type=MESH)

    def bwait(view, sem):
        pltpu.make_async_copy(view, view, sem).wait()

    units = [(3, 0), (3, 1), (1, 0), (2, 0), (2, 1), (1, 1), (0, 0), (0, 1)]

    def part(buf, at, kc):
        return mm(kc, jnp.concatenate([buf[at + (slice(None), slice(r, r + 16))].reshape(240, 128)
                                       for r in range(0, 16 * HB, 16)], axis=1))

    for c, half in units:
        r = RS0 + 16 * HB * half
        w = part(sg.at[:, :, :, r:r + 16 * HB], (chips[c], core), k4c[0])
        for b in range(HB):
            sb[c, 128 * (HB * half + b):128 * (HB * half + b) + 128, :] = w[:, 128 * b:128 * b + 128]

    def half_rows(half):
        return slice(HALF * half, HALF * half + HALF)

    def rows(half, c):
        return slice(HALF * half + CH * c, HALF * half + CH * c + CH)

    def first(c, half):
        m = 1 if c == 3 else 0
        return rcopy(sb.at[c, half_rows(half)], p1.at[m, half_rows(half)], p1s.at[half, m], p1r.at[half, m],
                     (xn, yn)[half])

    sent_after = {1: (3, 0), 2: (3, 1)}
    bwait(rs, rssem)
    for n, (c, half) in enumerate(units):
        r = 16 * HB * half
        w = part(rs.at[:, :, r:r + 16 * HB], (chips[c],), k4c[1])
        for b in range(HB):
            at = slice(128 * (HB * half + b), 128 * (HB * half + b) + 128)
            sb[c, at, :] = sb[c, at, :] + w[:, 128 * b:128 * b + 128]
        if n in sent_after:
            first(*sent_after[n]).start()

    def put(w, a0):
        o2_ref[a0:a0 + w.shape[0]] = w[:, :, :NV]
        for k in range(VB):
            lo, hi = max(a0, 16 * k), min(a0 + w.shape[0], 16 * k + NV - GR)
            if lo < hi:
                n = min(GC, NV - GC * k)
                o2_ref[GR + lo - 16 * k:GR + hi - 16 * k, :, GC * k:GC * k + n] = w[lo - a0:hi - a0, :, NV:NV + n]

    for c in range(15):
        col = iota((128, 128), 1)
        w = mm(pi, one_hot(iota((128, 128), 0) == (col >> 4) + 8 * c))
        k4[:, c * 128:(c + 1) * 128] = jnp.where((iota((128, 128), 0) >> 3) == (col & 15), w, 0.0).astype(BF)
    e6[...] = one_hot((iota((128, 960), 1) >> 3) == iota((128, 960), 0))

    def v1_rows(t):
        row = iota((96, 128), 0) + 96 * t
        z = mm(one_hot((row >> 3) == iota((96, 128), 1)), cvt[...]).astype(BF)
        w = mm(z, e6[...])
        keep = (iota((96, 960), 0) & 7) == (iota((96, 960), 1) & 7)
        v1k[pl.ds(pl.multiple_of(96 * t, 96), 96), :] = jnp.where(keep, w, 0.0).astype(BF)

    def v1_build(t, carry):
        v1_rows(t)
        return carry

    lax.fori_loop(0, 9, v1_build, 0)
    for half, col in ((0, 1), (1, 2)):
        bwait(p1.at[1, half_rows(half)], p1s.at[half, 1])
        first(col, half).start()
    for k in range(1, ND):
        src = lax.rem(me + k, ND)
        bwait(rg.at[src, :, 0:SENT], rgsem.at[src])

    v = rg[:, :, GO:GO + 8, :].reshape(960, 128)

    def v1_out(t, carry):
        w = mm(v1k[pl.ds(pl.multiple_of(96 * t, 96), 96), :], v)
        o1_ref[pl.ds(12 * t, 12)] = w.reshape(12, 8, 128)[:, :, :NV]
        return carry

    lax.fori_loop(0, 9, v1_out, 0)

    nx = -(-EX // 16)
    for ab in range(0, nx, 2):
        n = min(2, nx - ab)
        w = mm(k4[...], jnp.concatenate([rg[:, :, 16 * (ab + u):16 * (ab + u) + 16, :].reshape(1920, 128)
                                         for u in range(n)], axis=1)).reshape(16, 8, 128 * n)
        for u in range(n):
            put(w[:min(16, EX - 16 * (ab + u)), :, 128 * u:128 * u + 128], 16 * (ab + u))

    for half in range(2):
        bwait(p1.at[1, half_rows(half)], p1r.at[half, 1])
        z2[half_rows(half), :] = sb[2 - half, half_rows(half), :] + p1[1, half_rows(half), :]
    for c in range(NCH):
        for half in range(2):
            rcopy(z2.at[rows(half, c)], p2.at[rows(half, c)], p2s.at[half, c], p2r.at[half, c],
                  (yn, xn)[half]).start()
    for half in range(2):
        bwait(p1.at[0, half_rows(half)], p1r.at[half, 0])
        sb[0, half_rows(half), :] = sb[0, half_rows(half), :] + p1[0, half_rows(half), :]
    for c in range(NCH):
        for half in range(2):
            bwait(p2.at[rows(half, c)], p2r.at[half, c])
            w = sb[0, rows(half, c), :] + p2[rows(half, c), :]
            put(w.reshape(-1, 8, 128), EX + (HALF * half + CH * c) // 8)

    for k in range(ND - 1):
        bwait(rg.at[0, :, 0:SENT], sgsem.at[k])
    bwait(rs, ssem)
    for c in range(NCH):
        for half in range(2):
            bwait(p2.at[rows(half, c)], p2s.at[half, c])
    for half in range(2):
        bwait(p1.at[0, half_rows(half)], p1s.at[half, 0])


def write_out(x1_ref, x2_ref, y1_ref, y2_ref, sem):
    copies = [pltpu.make_async_copy(x1_ref, y1_ref, sem.at[0]), pltpu.make_async_copy(x2_ref, y2_ref, sem.at[1])]
    for c in copies:
        c.start()
    for c in copies:
        c.wait()


def solution(mesh):
    def local_part(ao, co, cv):
        a = ao.reshape(NP, ROWS, NQ)
        co, cv = (pltpu.with_memory_space_constraint(t.T, pltpu.HBM) for t in (co, cv))
        vm = pl.BlockSpec(memory_space=pltpu.VMEM)
        o1, o2 = pl.pallas_call(
            kernel,
            out_shape=[jax.ShapeDtypeStruct((NV, NO, NV), F32), jax.ShapeDtypeStruct((NV, NO, NV), F32)],
            in_specs=[pl.BlockSpec(memory_space=pltpu.HBM)] * 3,
            out_specs=[vm, vm],
            scratch_shapes=[
                pltpu.VMEM((NBUF, ROWS, NQ), BF),
                pltpu.VMEM((8, 128, 128), BF),
                pltpu.VMEM((8, 128, 128), BF),
                pltpu.VMEM((4, 2, NP, RS1, 128), BF),
                pltpu.VMEM((8, NP, RS0, 128), BF),
                pltpu.VMEM((4, NP, RS1 - RS0, 128), BF),
                pltpu.VMEM((4, 128 * RSB, 128), F32),
                pltpu.VMEM((2, RSR, 128), F32),
                pltpu.VMEM((RSR, 128), F32),
                pltpu.VMEM((RSR, 128), F32),
                pltpu.VMEM((64, 960), BF),
                pltpu.VMEM((128, 1920), BF),
                pltpu.VMEM((2, 128, 240), BF),
                pltpu.VMEM((864, 960), BF),
                pltpu.VMEM((128, 960), BF),
                pltpu.VMEM((NO, NQ), BF),
                pltpu.VMEM((NV, NQ), BF),
                pltpu.VMEM((16, 128), BF),
                pltpu.VMEM((128, 128), BF),
                pltpu.VMEM((128, 128), BF),
                pltpu.SemaphoreType.DMA((NBUF,)),
                pltpu.SemaphoreType.DMA((2,)),
                pltpu.SemaphoreType.DMA((ND,)),
                pltpu.SemaphoreType.DMA((ND,)),
                pltpu.SemaphoreType.DMA,
                pltpu.SemaphoreType.DMA,
                pltpu.SemaphoreType.DMA((2, 2)),
                pltpu.SemaphoreType.DMA((2, 2)),
                pltpu.SemaphoreType.DMA((2, NCH)),
                pltpu.SemaphoreType.DMA((2, NCH)),
            ],
            compiler_params=pltpu.CompilerParams(collective_id=0, has_side_effects=True,
                                                 vmem_limit_bytes=34 * 1024 * 1024),
            name='mo_blocks',
        )(a, co, cv)
        o1, o2 = pl.pallas_call(
            write_out,
            out_shape=[jax.ShapeDtypeStruct((NV, NO, NV), F32), jax.ShapeDtypeStruct((NV, NO, NV), F32)],
            in_specs=[vm, vm],
            out_specs=[pl.BlockSpec(memory_space=pltpu.HBM)] * 2,
            scratch_shapes=[pltpu.SemaphoreType.DMA((2,))],
            compiler_params=pltpu.CompilerParams(vmem_limit_bytes=2 * 1024 * 1024),
            name='write_out',
        )(o1, o2)
        return o1.transpose(0, 2, 1), o2.transpose(1, 0, 2)

    return jax.shard_map(local_part, mesh=mesh,
                         in_specs=(P(('frag', 'dev')), P('frag'), P('frag')),
                         out_specs=(P('frag', None, 'dev'), P('frag', None, 'dev')),
                         check_vma=False)
```

```python
import jax
import jax.numpy as jnp
from jax import lax
from jax.experimental import pallas as pl
from jax.experimental.pallas import tpu as pltpu
from jax.sharding import PartitionSpec as P

MESH = pl.DeviceIdType.MESH
BF = jnp.bfloat16
F32 = jnp.float32
ND = 8
NP = 15
NQ = 120
NO = 8
NV = 108
ROWS = NQ * NQ
NBUF = 4
PIECE = 3840
VB = 6
GR = 16 * VB
GC = 20
EX = 40
VB = 6
GR = 16 * VB
GC = 20
GO = EX
SENT = EX + 8
RS0 = -(-SENT // 16) * 16
RSA = GR - EX
RSB = -(-RSA // 16)
RS1 = RS0 + 16 * RSB
RSR = 8 * RSA
NCH = 2
HB = RSB // 2
HALF = RSR // 2
CH = HALF // NCH


def mm(a, b):
    return jnp.dot(a, b, preferred_element_type=F32)


def mm_nt(a, b):
    return lax.dot_general(a, b, (((1,), (1,)), ((), ())), preferred_element_type=F32)


def iota(shape, dim):
    return lax.broadcasted_iota(jnp.int32, shape, dim)


def one_hot(mask):
    return jnp.where(mask, 1.0, 0.0).astype(BF)


def kernel(a_ref, co_ref, cv_ref, o1_ref, o2_ref,
           abuf, ta, tb, sg, rg, rs, sb, p1, z2, p2, k1, k4, k4c, v1k, e6, coin, cvin, cot, cvt, cv,
           asem, csem, sgsem, rgsem, ssem, rssem, p1s, p1r, p2s, p2r):
    me = lax.axis_index('dev')
    frag = lax.axis_index('frag')
    core = lax.rem(me, 2)
    mx = lax.rem(me // 2, 2)
    my = me // 4
    sib = me + 1 - 2 * core
    xn = me + 2 - 4 * mx
    yn = me + 4 - 8 * my
    dg = xn + 4 - 8 * my
    cols = [me, xn, yn, dg]
    chips = [c // 2 for c in cols]
    one = core * chips[1] + (1 - core) * chips[3]
    two = core * chips[3] + (1 - core) * chips[1]
    peers = [(one, 0), (chips[2], 0), (two, 0), (one, 1), (chips[2], 1), (two, 1), (chips[0], 1)]
    par = [core, 1 - core]

    def a_start(p):
        slot = lax.rem(p, NBUF)
        for k in range(4):
            r = slice(PIECE * k, min(PIECE * k + PIECE, ROWS))
            pltpu.make_async_copy(a_ref.at[p, r], abuf.at[slot, r], asem.at[slot, k // 2]).start()

    def a_wait(p, half):
        slot = lax.rem(p, NBUF)
        r = slice(0, 2 * PIECE) if half == 0 else slice(2 * PIECE, ROWS)
        pltpu.make_async_copy(a_ref.at[p, r], abuf.at[slot, r], asem.at[slot, half]).wait()

    cin = [pltpu.make_async_copy(co_ref, coin, csem.at[0]), pltpu.make_async_copy(cv_ref, cvin, csem.at[1])]
    for c in cin:
        c.start()
    for p in range(NBUF - 1):
        a_start(p)

    barrier = pltpu.get_barrier_semaphore()
    for k in range(1, ND):
        pl.semaphore_signal(barrier, inc=1, device_id=(frag, lax.rem(me + k, ND)), device_id_type=MESH)

    cot[...] = jnp.zeros(cot.shape, BF)
    cvt[...] = jnp.zeros(cvt.shape, BF)
    for c in cin:
        c.wait()
    cot[0:NO, 0:NQ] = coin[...]
    cvt[0:NV, 0:NQ] = cvin[...]
    cv[...] = mm_nt(one_hot(iota((128, 128), 0) == iota((128, 128), 1)), cvt[...]).astype(BF)
    xr = mm(one_hot((iota((64, 16), 0) >> 3) == iota((64, 16), 1)), cot[...]).astype(BF)
    diff = iota((128, 960), 1) - iota((128, 960), 0)
    hit = diff == 0
    for k in range(1, 8):
        hit = hit | (diff == 120 * k)
    off = iota((64, 960), 1) - 120 * (iota((64, 960), 0) & 7)
    k1[...] = jnp.where((off >= 0) & (off < 120), mm(xr, one_hot(hit)), 0.0).astype(BF)
    pi = mm(one_hot((iota((128, 16), 0) & 7) == iota((128, 16), 1)), cot[...]).astype(BF)
    for h, d in enumerate((me, sib)):
        col = iota((128, 240), 1)
        w = mm(pi, one_hot(iota((128, 240), 0) == (col >> 4) + NP * d))
        keep = (iota((128, 240), 0) >> 3) == (col & 15)
        k4c[h] = jnp.where(keep, w, 0.0).astype(BF)
    pl.semaphore_wait(barrier, ND - 1)

    pad = jnp.zeros((960, 8), BF)
    lane = iota((16, 128), 1)

    def step1(p, t, g):
        slot = lax.rem(p, NBUF)
        left = jnp.concatenate([abuf[slot, 1920 * g:1920 * g + 960, :], pad], axis=1)
        if g < 7:
            right = jnp.concatenate([abuf[slot, 1920 * g + 960:1920 * g + 1920, :], pad], axis=1)
            out = mm(k1[...], jnp.concatenate([left, right], axis=1))
            lo = out[:, :128].reshape(8, 8, 128)
            hi = out[:, 128:].reshape(8, 8, 128)
        else:
            lo = mm(k1[...], left).reshape(8, 8, 128)
            hi = jnp.zeros((8, 8, 128), F32)
        t[:, 16 * g:16 * g + 16, :] = jnp.concatenate([lo, hi], axis=1).astype(BF)

    def step2(t, x):
        h = mm(t[x:x + 2].reshape(256, 128), cv[...]).astype(BF)
        return jnp.concatenate([h[:128], h[128:]], axis=1)

    def step3(p, x, h):
        g = mm(cvt[0:112, :], h)
        for y in range(2):
            last = g[GR:GR + 16, 128 * y:128 * y + 128]
            tiles = [jnp.where(lane < NV, g[16 * k:16 * k + 16, 128 * y:128 * y + 128],
                               pltpu.roll(last, (NV - GC * k) % 128, 1)) for k in range(VB)]
            tiles = jnp.concatenate(tiles, axis=0)
            sg[x // 2, y, p, 0:EX] = tiles[:EX].astype(BF)
            sg[x // 2, y, p, RS0:RS0 + RSA] = tiles[EX:].astype(BF)

    def step2o(t):
        hoo = mm_nt(cot[...], t[...].reshape(1024, 128))
        return jnp.concatenate([hoo[0:8, 128 * x:128 * x + 128] for x in range(8)], axis=0).astype(BF)

    def step3o(p, hoo):
        goo = mm(hoo, cv[...]).astype(BF).reshape(4, 2, 8, 128)
        for y in range(2):
            sg[:, y, p, GO:GO + 8] = goo[:, y]

    def work(p, told, tnew):
        def one(g):
            if tnew is not None:
                step1(p, tnew, g)

        h0 = step2(told, 0)
        one(0)
        h1 = step2(told, 2)
        one(1)
        step3(p - 1, 0, h0)
        h2 = step2(told, 4)
        one(2)
        step3(p - 1, 2, h1)
        h3 = step2(told, 6)
        one(3)
        step3(p - 1, 4, h2)
        hoo = step2o(told)
        if tnew is not None:
            a_wait(p, 1)
        one(4)
        step3(p - 1, 6, h3)
        one(5)
        step3o(p - 1, hoo)
        one(6)
        one(7)

    def sends(p):
        out = [pltpu.make_async_remote_copy(
            src_ref=sg.at[:, 1 - core, p, RS0:RS1], dst_ref=rs.at[:, p],
            send_sem=ssem, recv_sem=rssem, device_id=(frag, sib), device_id_type=MESH)]
        for k, (chip, q) in enumerate(peers):
            out.append(pltpu.make_async_remote_copy(
                src_ref=sg.at[chip, par[q], p, 0:SENT], dst_ref=rg.at[me, p, 0:SENT],
                send_sem=sgsem.at[k], recv_sem=rgsem.at[me],
                device_id=(frag, 2 * chip + par[q]), device_id_type=MESH))
        return out

    def send(p):
        for c in sends(p):
            c.start()
        rg[me, p, 0:SENT] = sg[chips[0], core, p, 0:SENT]

    if RS0 + RSA < RS1:
        sg[:, :, :, RS0 + RSA:RS1, :] = jnp.zeros((4, 2, NP, RS1 - RS0 - RSA, 128), BF)
    a_wait(0, 0)
    a_start(NBUF - 1)
    for g in range(8):
        if g == 4:
            a_wait(0, 1)
        step1(0, ta, g)

    def body(k, carry):
        for p, told, tnew in ((2 * k + 1, ta, tb), (2 * k + 2, tb, ta)):
            @pl.when(p + NBUF - 1 < NP)
            def _():
                a_start(p + NBUF - 1)

            @pl.when(p >= 2)
            def _():
                send(p - 2)

            a_wait(p, 0)
            work(p, told, tnew)
        return carry

    lax.fori_loop(0, NP // 2, body, 0)
    send(NP - 2)
    work(NP, ta, None)
    send(NP - 1)

    def rcopy(src, dst, ss, rr, dev):
        return pltpu.make_async_remote_copy(src_ref=src, dst_ref=dst, send_sem=ss, recv_sem=rr,
                                            device_id=(frag, dev), device_id_type=MESH)

    def bwait(view, sem):
        pltpu.make_async_copy(view, view, sem).wait()

    units = [(3, 0), (3, 1), (1, 0), (2, 0), (2, 1), (1, 1), (0, 0), (0, 1)]

    def part(buf, at, kc):
        return mm(kc, jnp.concatenate([buf[at + (slice(None), slice(r, r + 16))].reshape(240, 128)
                                       for r in range(0, 16 * HB, 16)], axis=1))

    for c, half in units:
        r = RS0 + 16 * HB * half
        w = part(sg.at[:, :, :, r:r + 16 * HB], (chips[c], core), k4c[0])
        for b in range(HB):
            sb[c, 128 * (HB * half + b):128 * (HB * half + b) + 128, :] = w[:, 128 * b:128 * b + 128]

    def half_rows(half):
        return slice(HALF * half, HALF * half + HALF)

    def rows(half, c):
        return slice(HALF * half + CH * c, HALF * half + CH * c + CH)

    def first(c, half):
        m = 1 if c == 3 else 0
        return rcopy(sb.at[c, half_rows(half)], p1.at[m, half_rows(half)], p1s.at[half, m], p1r.at[half, m],
                     (xn, yn)[half])

    sent_after = {1: (3, 0), 2: (3, 1)}
    bwait(rs, rssem)
    for n, (c, half) in enumerate(units):
        r = 16 * HB * half
        w = part(rs.at[:, :, r:r + 16 * HB], (chips[c],), k4c[1])
        for b in range(HB):
            at = slice(128 * (HB * half + b), 128 * (HB * half + b) + 128)
            sb[c, at, :] = sb[c, at, :] + w[:, 128 * b:128 * b + 128]
        if n in sent_after:
            first(*sent_after[n]).start()

    def put(w, a0):
        o2_ref[a0:a0 + w.shape[0]] = w[:, :, :NV]
        for k in range(VB):
            lo, hi = max(a0, 16 * k), min(a0 + w.shape[0], 16 * k + NV - GR)
            if lo < hi:
                n = min(GC, NV - GC * k)
                o2_ref[GR + lo - 16 * k:GR + hi - 16 * k, :, GC * k:GC * k + n] = w[lo - a0:hi - a0, :, NV:NV + n]

    for c in range(15):
        col = iota((128, 128), 1)
        w = mm(pi, one_hot(iota((128, 128), 0) == (col >> 4) + 8 * c))
        k4[:, c * 128:(c + 1) * 128] = jnp.where((iota((128, 128), 0) >> 3) == (col & 15), w, 0.0).astype(BF)
    e6[...] = one_hot((iota((128, 960), 1) >> 3) == iota((128, 960), 0))

    def v1_rows(t):
        row = iota((96, 128), 0) + 96 * t
        z = mm(one_hot((row >> 3) == iota((96, 128), 1)), cvt[...]).astype(BF)
        w = mm(z, e6[...])
        keep = (iota((96, 960), 0) & 7) == (iota((96, 960), 1) & 7)
        v1k[pl.ds(pl.multiple_of(96 * t, 96), 96), :] = jnp.where(keep, w, 0.0).astype(BF)

    def v1_build(t, carry):
        v1_rows(t)
        return carry

    lax.fori_loop(0, 9, v1_build, 0)
    for half, col in ((0, 1), (1, 2)):
        bwait(p1.at[1, half_rows(half)], p1s.at[half, 1])
        first(col, half).start()
    for k in range(1, ND):
        src = lax.rem(me + k, ND)
        bwait(rg.at[src, :, 0:SENT], rgsem.at[src])

    v = rg[:, :, GO:GO + 8, :].reshape(960, 128)

    def v1_out(t, carry):
        w = mm(v1k[pl.ds(pl.multiple_of(96 * t, 96), 96), :], v)
        o1_ref[pl.ds(12 * t, 12)] = w.reshape(12, 8, 128)[:, :, :NV]
        return carry

    lax.fori_loop(0, 9, v1_out, 0)

    nx = -(-EX // 16)
    for ab in range(0, nx, 2):
        n = min(2, nx - ab)
        w = mm(k4[...], jnp.concatenate([rg[:, :, 16 * (ab + u):16 * (ab + u) + 16, :].reshape(1920, 128)
                                         for u in range(n)], axis=1)).reshape(16, 8, 128 * n)
        for u in range(n):
            put(w[:min(16, EX - 16 * (ab + u)), :, 128 * u:128 * u + 128], 16 * (ab + u))

    for half in range(2):
        bwait(p1.at[1, half_rows(half)], p1r.at[half, 1])
        z2[half_rows(half), :] = sb[2 - half, half_rows(half), :] + p1[1, half_rows(half), :]
    for c in range(NCH):
        for half in range(2):
            rcopy(z2.at[rows(half, c)], p2.at[rows(half, c)], p2s.at[half, c], p2r.at[half, c],
                  (yn, xn)[half]).start()
    for half in range(2):
        bwait(p1.at[0, half_rows(half)], p1r.at[half, 0])
        sb[0, half_rows(half), :] = sb[0, half_rows(half), :] + p1[0, half_rows(half), :]
    for c in range(NCH):
        for half in range(2):
            bwait(p2.at[rows(half, c)], p2r.at[half, c])
            w = sb[0, rows(half, c), :] + p2[rows(half, c), :]
            put(w.reshape(-1, 8, 128), EX + (HALF * half + CH * c) // 8)

    for k in range(ND - 1):
        bwait(rg.at[0, :, 0:SENT], sgsem.at[k])
    bwait(rs, ssem)
    for c in range(NCH):
        for half in range(2):
            bwait(p2.at[rows(half, c)], p2s.at[half, c])
    for half in range(2):
        bwait(p1.at[0, half_rows(half)], p1s.at[half, 0])


def write_out(x1_ref, x2_ref, y1_ref, y2_ref, sem):
    copies = [pltpu.make_async_copy(x1_ref, y1_ref, sem.at[0]), pltpu.make_async_copy(x2_ref, y2_ref, sem.at[1])]
    for c in copies:
        c.start()
    for c in copies:
        c.wait()


def solution(mesh):
    def local_part(ao, co, cv):
        a = ao.reshape(NP, ROWS, NQ)
        co, cv = (pltpu.with_memory_space_constraint(t.T, pltpu.HBM) for t in (co, cv))
        vm = pl.BlockSpec(memory_space=pltpu.VMEM)
        o1, o2 = pl.pallas_call(
            kernel,
            out_shape=[jax.ShapeDtypeStruct((NV, NO, NV), F32), jax.ShapeDtypeStruct((NV, NO, NV), F32)],
            in_specs=[pl.BlockSpec(memory_space=pltpu.HBM)] * 3,
            out_specs=[vm, vm],
            scratch_shapes=[
                pltpu.VMEM((NBUF, ROWS, NQ), BF),
                pltpu.VMEM((8, 128, 128), BF),
                pltpu.VMEM((8, 128, 128), BF),
                pltpu.VMEM((4, 2, NP, RS1, 128), BF),
                pltpu.VMEM((8, NP, RS0, 128), BF),
                pltpu.VMEM((4, NP, RS1 - RS0, 128), BF),
                pltpu.VMEM((4, 128 * RSB, 128), F32),
                pltpu.VMEM((2, RSR, 128), F32),
                pltpu.VMEM((RSR, 128), F32),
                pltpu.VMEM((RSR, 128), F32),
                pltpu.VMEM((64, 960), BF),
                pltpu.VMEM((128, 1920), BF),
                pltpu.VMEM((2, 128, 240), BF),
                pltpu.VMEM((864, 960), BF),
                pltpu.VMEM((128, 960), BF),
                pltpu.VMEM((NO, NQ), BF),
                pltpu.VMEM((NV, NQ), BF),
                pltpu.VMEM((16, 128), BF),
                pltpu.VMEM((128, 128), BF),
                pltpu.VMEM((128, 128), BF),
                pltpu.SemaphoreType.DMA((NBUF, 2)),
                pltpu.SemaphoreType.DMA((2,)),
                pltpu.SemaphoreType.DMA((ND,)),
                pltpu.SemaphoreType.DMA((ND,)),
                pltpu.SemaphoreType.DMA,
                pltpu.SemaphoreType.DMA,
                pltpu.SemaphoreType.DMA((2, 2)),
                pltpu.SemaphoreType.DMA((2, 2)),
                pltpu.SemaphoreType.DMA((2, NCH)),
                pltpu.SemaphoreType.DMA((2, NCH)),
            ],
            compiler_params=pltpu.CompilerParams(collective_id=0, has_side_effects=True,
                                                 vmem_limit_bytes=34 * 1024 * 1024),
            name='mo_blocks',
        )(a, co, cv)
        o1, o2 = pl.pallas_call(
            write_out,
            out_shape=[jax.ShapeDtypeStruct((NV, NO, NV), F32), jax.ShapeDtypeStruct((NV, NO, NV), F32)],
            in_specs=[vm, vm],
            out_specs=[pl.BlockSpec(memory_space=pltpu.HBM)] * 2,
            scratch_shapes=[pltpu.SemaphoreType.DMA((2,))],
            compiler_params=pltpu.CompilerParams(vmem_limit_bytes=2 * 1024 * 1024),
            name='write_out',
        )(o1, o2)
        return o1.transpose(0, 2, 1), o2.transpose(1, 0, 2)

    return jax.shard_map(local_part, mesh=mesh,
                         in_specs=(P(('frag', 'dev')), P('frag'), P('frag')),
                         out_specs=(P('frag', None, 'dev'), P('frag', None, 'dev')),
                         check_vma=False)
```

```python
import jax
import jax.numpy as jnp
from jax import lax
from jax.experimental import pallas as pl
from jax.experimental.pallas import tpu as pltpu
from jax.sharding import PartitionSpec as P

MESH = pl.DeviceIdType.MESH
BF = jnp.bfloat16
F32 = jnp.float32
ND = 8
NP = 15
NQ = 120
NO = 8
NV = 108
ROWS = NQ * NQ
NBUF = 4
SPLIT = 5
VB = 6
GR = 16 * VB
GC = 20
EX = 40
VB = 6
GR = 16 * VB
GC = 20
GO = EX
SENT = EX + 8
RS0 = -(-SENT // 16) * 16
RSA = GR - EX
RSB = -(-RSA // 16)
RS1 = RS0 + 16 * RSB
RSR = 8 * RSA
NCH = 2
HB = RSB // 2
HALF = RSR // 2
CH = HALF // NCH


def mm(a, b):
    return jnp.dot(a, b, preferred_element_type=F32)


def mm_nt(a, b):
    return lax.dot_general(a, b, (((1,), (1,)), ((), ())), preferred_element_type=F32)


def iota(shape, dim):
    return lax.broadcasted_iota(jnp.int32, shape, dim)


def one_hot(mask):
    return jnp.where(mask, 1.0, 0.0).astype(BF)


def kernel(a_ref, co_ref, cv_ref, o1_ref, o2_ref,
           abuf, ta, tb, sg, rg, rs, sb, p1, z2, p2, k1, k4, k4c, v1k, e6, coin, cvin, cot, cvt, cv,
           asem, csem, sgsem, rgsem, ssem, rssem, p1s, p1r, p2s, p2r):
    me = lax.axis_index('dev')
    frag = lax.axis_index('frag')
    core = lax.rem(me, 2)
    mx = lax.rem(me // 2, 2)
    my = me // 4
    sib = me + 1 - 2 * core
    xn = me + 2 - 4 * mx
    yn = me + 4 - 8 * my
    dg = xn + 4 - 8 * my
    cols = [me, xn, yn, dg]
    chips = [c // 2 for c in cols]
    one = core * chips[1] + (1 - core) * chips[3]
    two = core * chips[3] + (1 - core) * chips[1]
    peers = [(one, 0), (chips[2], 0), (two, 0), (one, 1), (chips[2], 1), (two, 1), (chips[0], 1)]
    par = [core, 1 - core]

    def a_copies(p):
        slot = lax.rem(p, NBUF)
        step = ROWS // SPLIT
        return [pltpu.make_async_copy(a_ref.at[p, pl.ds(k * step, step)],
                                      abuf.at[slot, pl.ds(k * step, step)],
                                      asem.at[slot]) for k in range(SPLIT)]

    def a_start(p):
        for c in a_copies(p):
            c.start()

    def a_wait(p):
        slot = lax.rem(p, NBUF)
        pltpu.make_async_copy(a_ref.at[p], abuf.at[slot], asem.at[slot]).wait()

    cin = [pltpu.make_async_copy(co_ref, coin, csem.at[0]), pltpu.make_async_copy(cv_ref, cvin, csem.at[1])]
    for c in cin:
        c.start()
    for p in range(NBUF - 1):
        a_start(p)

    barrier = pltpu.get_barrier_semaphore()
    for k in range(1, ND):
        pl.semaphore_signal(barrier, inc=1, device_id=(frag, lax.rem(me + k, ND)), device_id_type=MESH)

    cot[...] = jnp.zeros(cot.shape, BF)
    cvt[...] = jnp.zeros(cvt.shape, BF)
    for c in cin:
        c.wait()
    cot[0:NO, 0:NQ] = coin[...]
    cvt[0:NV, 0:NQ] = cvin[...]
    cv[...] = mm_nt(one_hot(iota((128, 128), 0) == iota((128, 128), 1)), cvt[...]).astype(BF)
    xr = mm(one_hot((iota((64, 16), 0) >> 3) == iota((64, 16), 1)), cot[...]).astype(BF)
    diff = iota((128, 960), 1) - iota((128, 960), 0)
    hit = diff == 0
    for k in range(1, 8):
        hit = hit | (diff == 120 * k)
    off = iota((64, 960), 1) - 120 * (iota((64, 960), 0) & 7)
    k1[...] = jnp.where((off >= 0) & (off < 120), mm(xr, one_hot(hit)), 0.0).astype(BF)
    pi = mm(one_hot((iota((128, 16), 0) & 7) == iota((128, 16), 1)), cot[...]).astype(BF)
    for h, d in enumerate((me, sib)):
        col = iota((128, 240), 1)
        w = mm(pi, one_hot(iota((128, 240), 0) == (col >> 4) + NP * d))
        keep = (iota((128, 240), 0) >> 3) == (col & 15)
        k4c[h] = jnp.where(keep, w, 0.0).astype(BF)
    pl.semaphore_wait(barrier, ND - 1)

    pad = jnp.zeros((960, 8), BF)
    lane = iota((16, 128), 1)

    def step1(p, t, g):
        slot = lax.rem(p, NBUF)
        left = jnp.concatenate([abuf[slot, 1920 * g:1920 * g + 960, :], pad], axis=1)
        if g < 7:
            right = jnp.concatenate([abuf[slot, 1920 * g + 960:1920 * g + 1920, :], pad], axis=1)
            out = mm(k1[...], jnp.concatenate([left, right], axis=1))
            lo = out[:, :128].reshape(8, 8, 128)
            hi = out[:, 128:].reshape(8, 8, 128)
        else:
            lo = mm(k1[...], left).reshape(8, 8, 128)
            hi = jnp.zeros((8, 8, 128), F32)
        t[:, 16 * g:16 * g + 16, :] = jnp.concatenate([lo, hi], axis=1).astype(BF)

    def step2(t, x):
        h = mm(t[x:x + 2].reshape(256, 128), cv[...]).astype(BF)
        return jnp.concatenate([h[:128], h[128:]], axis=1)

    def step3(p, x, h):
        g = mm(cvt[0:112, :], h)
        for y in range(2):
            last = g[GR:GR + 16, 128 * y:128 * y + 128]
            tiles = [jnp.where(lane < NV, g[16 * k:16 * k + 16, 128 * y:128 * y + 128],
                               pltpu.roll(last, (NV - GC * k) % 128, 1)) for k in range(VB)]
            tiles = jnp.concatenate(tiles, axis=0)
            sg[x // 2, y, p, 0:EX] = tiles[:EX].astype(BF)
            sg[x // 2, y, p, RS0:RS0 + RSA] = tiles[EX:].astype(BF)

    def step2o(t):
        hoo = mm_nt(cot[...], t[...].reshape(1024, 128))
        return jnp.concatenate([hoo[0:8, 128 * x:128 * x + 128] for x in range(8)], axis=0).astype(BF)

    def step3o(p, hoo):
        goo = mm(hoo, cv[...]).astype(BF).reshape(4, 2, 8, 128)
        for y in range(2):
            sg[:, y, p, GO:GO + 8] = goo[:, y]

    def work(p, told, tnew):
        def one(g):
            if tnew is not None:
                step1(p, tnew, g)

        h0 = step2(told, 0)
        one(0)
        h1 = step2(told, 2)
        one(1)
        step3(p - 1, 0, h0)
        h2 = step2(told, 4)
        one(2)
        step3(p - 1, 2, h1)
        h3 = step2(told, 6)
        one(3)
        step3(p - 1, 4, h2)
        hoo = step2o(told)
        one(4)
        step3(p - 1, 6, h3)
        one(5)
        step3o(p - 1, hoo)
        one(6)
        one(7)

    def sends(p):
        out = [pltpu.make_async_remote_copy(
            src_ref=sg.at[:, 1 - core, p, RS0:RS1], dst_ref=rs.at[:, p],
            send_sem=ssem, recv_sem=rssem, device_id=(frag, sib), device_id_type=MESH)]
        for k, (chip, q) in enumerate(peers):
            out.append(pltpu.make_async_remote_copy(
                src_ref=sg.at[chip, par[q], p, 0:SENT], dst_ref=rg.at[me, p, 0:SENT],
                send_sem=sgsem.at[k], recv_sem=rgsem.at[me],
                device_id=(frag, 2 * chip + par[q]), device_id_type=MESH))
        return out

    def send(p):
        for c in sends(p):
            c.start()
        rg[me, p, 0:SENT] = sg[chips[0], core, p, 0:SENT]

    if RS0 + RSA < RS1:
        sg[:, :, :, RS0 + RSA:RS1, :] = jnp.zeros((4, 2, NP, RS1 - RS0 - RSA, 128), BF)
    a_wait(0)
    a_start(NBUF - 1)
    for g in range(8):
        step1(0, ta, g)

    def body(k, carry):
        for p, told, tnew in ((2 * k + 1, ta, tb), (2 * k + 2, tb, ta)):
            @pl.when(p + NBUF - 1 < NP)
            def _():
                a_start(p + NBUF - 1)

            if told is ta:
                @pl.when(k > 0)
                def _():
                    send(p - 2)
            else:
                send(p - 2)

            a_wait(p)
            work(p, told, tnew)
        return carry

    lax.fori_loop(0, NP // 2, body, 0)
    send(NP - 2)
    work(NP, ta, None)
    send(NP - 1)

    def rcopy(src, dst, ss, rr, dev):
        return pltpu.make_async_remote_copy(src_ref=src, dst_ref=dst, send_sem=ss, recv_sem=rr,
                                            device_id=(frag, dev), device_id_type=MESH)

    def bwait(view, sem):
        pltpu.make_async_copy(view, view, sem).wait()

    units = [(3, 0), (3, 1), (1, 0), (2, 0), (2, 1), (1, 1), (0, 0), (0, 1)]

    def part(buf, at, kc):
        return mm(kc, jnp.concatenate([buf[at + (slice(None), slice(r, r + 16))].reshape(240, 128)
                                       for r in range(0, 16 * HB, 16)], axis=1))

    for c, half in units:
        r = RS0 + 16 * HB * half
        w = part(sg.at[:, :, :, r:r + 16 * HB], (chips[c], core), k4c[0])
        for b in range(HB):
            sb[c, 128 * (HB * half + b):128 * (HB * half + b) + 128, :] = w[:, 128 * b:128 * b + 128]

    def half_rows(half):
        return slice(HALF * half, HALF * half + HALF)

    def rows(half, c):
        return slice(HALF * half + CH * c, HALF * half + CH * c + CH)

    def first(c, half):
        m = 1 if c == 3 else 0
        return rcopy(sb.at[c, half_rows(half)], p1.at[m, half_rows(half)], p1s.at[half, m], p1r.at[half, m],
                     (xn, yn)[half])

    sent_after = {1: (3, 0), 2: (3, 1)}
    bwait(rs, rssem)
    for n, (c, half) in enumerate(units):
        r = 16 * HB * half
        w = part(rs.at[:, :, r:r + 16 * HB], (chips[c],), k4c[1])
        for b in range(HB):
            at = slice(128 * (HB * half + b), 128 * (HB * half + b) + 128)
            sb[c, at, :] = sb[c, at, :] + w[:, 128 * b:128 * b + 128]
        if n in sent_after:
            first(*sent_after[n]).start()

    def put(w, a0):
        o2_ref[a0:a0 + w.shape[0]] = w[:, :, :NV]
        for k in range(VB):
            lo, hi = max(a0, 16 * k), min(a0 + w.shape[0], 16 * k + NV - GR)
            if lo < hi:
                n = min(GC, NV - GC * k)
                o2_ref[GR + lo - 16 * k:GR + hi - 16 * k, :, GC * k:GC * k + n] = w[lo - a0:hi - a0, :, NV:NV + n]

    for c in range(15):
        col = iota((128, 128), 1)
        w = mm(pi, one_hot(iota((128, 128), 0) == (col >> 4) + 8 * c))
        k4[:, c * 128:(c + 1) * 128] = jnp.where((iota((128, 128), 0) >> 3) == (col & 15), w, 0.0).astype(BF)
    e6[...] = one_hot((iota((128, 960), 1) >> 3) == iota((128, 960), 0))

    def v1_rows(t):
        row = iota((96, 128), 0) + 96 * t
        z = mm(one_hot((row >> 3) == iota((96, 128), 1)), cvt[...]).astype(BF)
        w = mm(z, e6[...])
        keep = (iota((96, 960), 0) & 7) == (iota((96, 960), 1) & 7)
        v1k[pl.ds(pl.multiple_of(96 * t, 96), 96), :] = jnp.where(keep, w, 0.0).astype(BF)

    def v1_build(t, carry):
        v1_rows(t)
        return carry

    lax.fori_loop(0, 9, v1_build, 0)
    for half, col in ((0, 1), (1, 2)):
        bwait(p1.at[1, half_rows(half)], p1s.at[half, 1])
        first(col, half).start()
    for half in range(2):
        bwait(p1.at[1, half_rows(half)], p1r.at[half, 1])
        z2[half_rows(half), :] = sb[2 - half, half_rows(half), :] + p1[1, half_rows(half), :]
    for c in range(NCH):
        for half in range(2):
            rcopy(z2.at[rows(half, c)], p2.at[rows(half, c)], p2s.at[half, c], p2r.at[half, c],
                  (yn, xn)[half]).start()
    for k in range(1, ND):
        src = lax.rem(me + k, ND)
        bwait(rg.at[src, :, 0:SENT], rgsem.at[src])

    v = rg[:, :, GO:GO + 8, :].reshape(960, 128)

    def v1_out(t, carry):
        w = mm(v1k[pl.ds(pl.multiple_of(96 * t, 96), 96), :], v)
        o1_ref[pl.ds(12 * t, 12)] = w.reshape(12, 8, 128)[:, :, :NV]
        return carry

    lax.fori_loop(0, 9, v1_out, 0)

    nx = -(-EX // 16)
    for ab in range(0, nx, 2):
        n = min(2, nx - ab)
        w = mm(k4[...], jnp.concatenate([rg[:, :, 16 * (ab + u):16 * (ab + u) + 16, :].reshape(1920, 128)
                                         for u in range(n)], axis=1)).reshape(16, 8, 128 * n)
        for u in range(n):
            put(w[:min(16, EX - 16 * (ab + u)), :, 128 * u:128 * u + 128], 16 * (ab + u))

    for half in range(2):
        bwait(p1.at[0, half_rows(half)], p1r.at[half, 0])
        sb[0, half_rows(half), :] = sb[0, half_rows(half), :] + p1[0, half_rows(half), :]
    for c in range(NCH):
        for half in range(2):
            bwait(p2.at[rows(half, c)], p2r.at[half, c])
            w = sb[0, rows(half, c), :] + p2[rows(half, c), :]
            put(w.reshape(-1, 8, 128), EX + (HALF * half + CH * c) // 8)

    for k in range(ND - 1):
        bwait(rg.at[0, :, 0:SENT], sgsem.at[k])
    bwait(rs, ssem)
    for c in range(NCH):
        for half in range(2):
            bwait(p2.at[rows(half, c)], p2s.at[half, c])
    for half in range(2):
        bwait(p1.at[0, half_rows(half)], p1s.at[half, 0])


def write_out(x1_ref, x2_ref, y1_ref, y2_ref, sem):
    copies = [pltpu.make_async_copy(x1_ref, y1_ref, sem.at[0]), pltpu.make_async_copy(x2_ref, y2_ref, sem.at[1])]
    for c in copies:
        c.start()
    for c in copies:
        c.wait()


def solution(mesh):
    def local_part(ao, co, cv):
        a = ao.reshape(NP, ROWS, NQ)
        co, cv = (pltpu.with_memory_space_constraint(t.T, pltpu.HBM) for t in (co, cv))
        vm = pl.BlockSpec(memory_space=pltpu.VMEM)
        o1, o2 = pl.pallas_call(
            kernel,
            out_shape=[jax.ShapeDtypeStruct((NV, NO, NV), F32), jax.ShapeDtypeStruct((NV, NO, NV), F32)],
            in_specs=[pl.BlockSpec(memory_space=pltpu.HBM)] * 3,
            out_specs=[vm, vm],
            scratch_shapes=[
                pltpu.VMEM((NBUF, ROWS, NQ), BF),
                pltpu.VMEM((8, 128, 128), BF),
                pltpu.VMEM((8, 128, 128), BF),
                pltpu.VMEM((4, 2, NP, RS1, 128), BF),
                pltpu.VMEM((8, NP, RS0, 128), BF),
                pltpu.VMEM((4, NP, RS1 - RS0, 128), BF),
                pltpu.VMEM((4, 128 * RSB, 128), F32),
                pltpu.VMEM((2, RSR, 128), F32),
                pltpu.VMEM((RSR, 128), F32),
                pltpu.VMEM((RSR, 128), F32),
                pltpu.VMEM((64, 960), BF),
                pltpu.VMEM((128, 1920), BF),
                pltpu.VMEM((2, 128, 240), BF),
                pltpu.VMEM((864, 960), BF),
                pltpu.VMEM((128, 960), BF),
                pltpu.VMEM((NO, NQ), BF),
                pltpu.VMEM((NV, NQ), BF),
                pltpu.VMEM((16, 128), BF),
                pltpu.VMEM((128, 128), BF),
                pltpu.VMEM((128, 128), BF),
                pltpu.SemaphoreType.DMA((NBUF,)),
                pltpu.SemaphoreType.DMA((2,)),
                pltpu.SemaphoreType.DMA((ND,)),
                pltpu.SemaphoreType.DMA((ND,)),
                pltpu.SemaphoreType.DMA,
                pltpu.SemaphoreType.DMA,
                pltpu.SemaphoreType.DMA((2, 2)),
                pltpu.SemaphoreType.DMA((2, 2)),
                pltpu.SemaphoreType.DMA((2, NCH)),
                pltpu.SemaphoreType.DMA((2, NCH)),
            ],
            compiler_params=pltpu.CompilerParams(collective_id=0, has_side_effects=True,
                                                 vmem_limit_bytes=34 * 1024 * 1024),
            name='mo_blocks',
        )(a, co, cv)
        o1, o2 = pl.pallas_call(
            write_out,
            out_shape=[jax.ShapeDtypeStruct((NV, NO, NV), F32), jax.ShapeDtypeStruct((NV, NO, NV), F32)],
            in_specs=[vm, vm],
            out_specs=[pl.BlockSpec(memory_space=pltpu.HBM)] * 2,
            scratch_shapes=[pltpu.SemaphoreType.DMA((2,))],
            compiler_params=pltpu.CompilerParams(vmem_limit_bytes=2 * 1024 * 1024),
            name='write_out',
        )(o1, o2)
        return o1.transpose(0, 2, 1), o2.transpose(1, 0, 2)

    return jax.shard_map(local_part, mesh=mesh,
                         in_specs=(P(('frag', 'dev')), P('frag'), P('frag')),
                         out_specs=(P('frag', None, 'dev'), P('frag', None, 'dev')),
                         check_vma=False)
```

```python
import jax
import jax.numpy as jnp
from jax import lax
from jax.experimental import pallas as pl
from jax.experimental.pallas import tpu as pltpu
from jax.sharding import PartitionSpec as P

MESH = pl.DeviceIdType.MESH
BF = jnp.bfloat16
F32 = jnp.float32
ND = 8
NP = 15
NQ = 120
NO = 8
NV = 108
ROWS = NQ * NQ
NBUF = 4
SPLIT = 5
VB = 6
GR = 16 * VB
GC = 20
EX = 40
VB = 6
GR = 16 * VB
GC = 20
GO = EX
SENT = EX + 8
RS0 = -(-SENT // 16) * 16
RSA = GR - EX
RSB = -(-RSA // 16)
RS1 = RS0 + 16 * RSB
RSR = 8 * RSA
NCH = 2
HB = RSB // 2
XROWS = 192


def mm(a, b):
    return jnp.dot(a, b, preferred_element_type=F32)


def mm_nt(a, b):
    return lax.dot_general(a, b, (((1,), (1,)), ((), ())), preferred_element_type=F32)


def iota(shape, dim):
    return lax.broadcasted_iota(jnp.int32, shape, dim)


def one_hot(mask):
    return jnp.where(mask, 1.0, 0.0).astype(BF)


def kernel(a_ref, co_ref, cv_ref, o1_ref, o2_ref,
           abuf, ta, tb, sg, rg, rs, sb, p1, z2, p2, k1, k4, k4c, v1k, e6, coin, cvin, cot, cvt, cv,
           asem, csem, sgsem, rgsem, ssem, rssem, p1s, p1r, p2s, p2r):
    me = lax.axis_index('dev')
    frag = lax.axis_index('frag')
    core = lax.rem(me, 2)
    mx = lax.rem(me // 2, 2)
    my = me // 4
    sib = me + 1 - 2 * core
    xn = me + 2 - 4 * mx
    yn = me + 4 - 8 * my
    dg = xn + 4 - 8 * my
    cols = [me, xn, yn, dg]
    chips = [c // 2 for c in cols]
    one = core * chips[1] + (1 - core) * chips[3]
    two = core * chips[3] + (1 - core) * chips[1]
    peers = [(one, 0), (chips[2], 0), (two, 0), (one, 1), (chips[2], 1), (two, 1), (chips[0], 1)]
    par = [core, 1 - core]

    def a_copies(p):
        slot = lax.rem(p, NBUF)
        step = ROWS // SPLIT
        return [pltpu.make_async_copy(a_ref.at[p, pl.ds(k * step, step)],
                                      abuf.at[slot, pl.ds(k * step, step)],
                                      asem.at[slot]) for k in range(SPLIT)]

    def a_start(p):
        for c in a_copies(p):
            c.start()

    def a_wait(p):
        slot = lax.rem(p, NBUF)
        pltpu.make_async_copy(a_ref.at[p], abuf.at[slot], asem.at[slot]).wait()

    cin = [pltpu.make_async_copy(co_ref, coin, csem.at[0]), pltpu.make_async_copy(cv_ref, cvin, csem.at[1])]
    for c in cin:
        c.start()
    for p in range(NBUF - 1):
        a_start(p)

    barrier = pltpu.get_barrier_semaphore()
    for k in range(1, ND):
        pl.semaphore_signal(barrier, inc=1, device_id=(frag, lax.rem(me + k, ND)), device_id_type=MESH)

    cot[...] = jnp.zeros(cot.shape, BF)
    cvt[...] = jnp.zeros(cvt.shape, BF)
    for c in cin:
        c.wait()
    cot[0:NO, 0:NQ] = coin[...]
    cvt[0:NV, 0:NQ] = cvin[...]
    cv[...] = mm_nt(one_hot(iota((128, 128), 0) == iota((128, 128), 1)), cvt[...]).astype(BF)
    xr = mm(one_hot((iota((64, 16), 0) >> 3) == iota((64, 16), 1)), cot[...]).astype(BF)
    diff = iota((128, 960), 1) - iota((128, 960), 0)
    hit = diff == 0
    for k in range(1, 8):
        hit = hit | (diff == 120 * k)
    off = iota((64, 960), 1) - 120 * (iota((64, 960), 0) & 7)
    k1[...] = jnp.where((off >= 0) & (off < 120), mm(xr, one_hot(hit)), 0.0).astype(BF)
    pi = mm(one_hot((iota((128, 16), 0) & 7) == iota((128, 16), 1)), cot[...]).astype(BF)
    for h, d in enumerate((me, sib)):
        col = iota((128, 240), 1)
        w = mm(pi, one_hot(iota((128, 240), 0) == (col >> 4) + NP * d))
        keep = (iota((128, 240), 0) >> 3) == (col & 15)
        k4c[h] = jnp.where(keep, w, 0.0).astype(BF)
    pl.semaphore_wait(barrier, ND - 1)

    pad = jnp.zeros((960, 8), BF)
    lane = iota((16, 128), 1)

    def step1(p, t, g):
        slot = lax.rem(p, NBUF)
        left = jnp.concatenate([abuf[slot, 1920 * g:1920 * g + 960, :], pad], axis=1)
        if g < 7:
            right = jnp.concatenate([abuf[slot, 1920 * g + 960:1920 * g + 1920, :], pad], axis=1)
            out = mm(k1[...], jnp.concatenate([left, right], axis=1))
            lo = out[:, :128].reshape(8, 8, 128)
            hi = out[:, 128:].reshape(8, 8, 128)
        else:
            lo = mm(k1[...], left).reshape(8, 8, 128)
            hi = jnp.zeros((8, 8, 128), F32)
        t[:, 16 * g:16 * g + 16, :] = jnp.concatenate([lo, hi], axis=1).astype(BF)

    def step2(t, x):
        h = mm(t[x:x + 2].reshape(256, 128), cv[...]).astype(BF)
        return jnp.concatenate([h[:128], h[128:]], axis=1)

    def step3(p, x, h):
        g = mm(cvt[0:112, :], h)
        for y in range(2):
            last = g[GR:GR + 16, 128 * y:128 * y + 128]
            tiles = [jnp.where(lane < NV, g[16 * k:16 * k + 16, 128 * y:128 * y + 128],
                               pltpu.roll(last, (NV - GC * k) % 128, 1)) for k in range(VB)]
            tiles = jnp.concatenate(tiles, axis=0)
            sg[x // 2, y, p, 0:EX] = tiles[:EX].astype(BF)
            sg[x // 2, y, p, RS0:RS0 + RSA] = tiles[EX:].astype(BF)

    def step2o(t):
        hoo = mm_nt(cot[...], t[...].reshape(1024, 128))
        return jnp.concatenate([hoo[0:8, 128 * x:128 * x + 128] for x in range(8)], axis=0).astype(BF)

    def step3o(p, hoo):
        goo = mm(hoo, cv[...]).astype(BF).reshape(4, 2, 8, 128)
        for y in range(2):
            sg[:, y, p, GO:GO + 8] = goo[:, y]

    def work(p, told, tnew):
        def one(g):
            if tnew is not None:
                step1(p, tnew, g)

        h0 = step2(told, 0)
        one(0)
        h1 = step2(told, 2)
        one(1)
        step3(p - 1, 0, h0)
        h2 = step2(told, 4)
        one(2)
        step3(p - 1, 2, h1)
        h3 = step2(told, 6)
        one(3)
        step3(p - 1, 4, h2)
        hoo = step2o(told)
        one(4)
        step3(p - 1, 6, h3)
        one(5)
        step3o(p - 1, hoo)
        one(6)
        one(7)

    def sends(p):
        out = [pltpu.make_async_remote_copy(
            src_ref=sg.at[:, 1 - core, p, RS0:RS1], dst_ref=rs.at[:, p],
            send_sem=ssem, recv_sem=rssem, device_id=(frag, sib), device_id_type=MESH)]
        for k, (chip, q) in enumerate(peers):
            out.append(pltpu.make_async_remote_copy(
                src_ref=sg.at[chip, par[q], p, 0:SENT], dst_ref=rg.at[me, p, 0:SENT],
                send_sem=sgsem.at[k], recv_sem=rgsem.at[me],
                device_id=(frag, 2 * chip + par[q]), device_id_type=MESH))
        return out

    def send(p):
        for c in sends(p):
            c.start()
        rg[me, p, 0:SENT] = sg[chips[0], core, p, 0:SENT]

    if RS0 + RSA < RS1:
        sg[:, :, :, RS0 + RSA:RS1, :] = jnp.zeros((4, 2, NP, RS1 - RS0 - RSA, 128), BF)
    a_wait(0)
    a_start(NBUF - 1)
    for g in range(8):
        step1(0, ta, g)

    def body(k, carry):
        for p, told, tnew in ((2 * k + 1, ta, tb), (2 * k + 2, tb, ta)):
            @pl.when(p + NBUF - 1 < NP)
            def _():
                a_start(p + NBUF - 1)

            if told is ta:
                @pl.when(k > 0)
                def _():
                    send(p - 2)
            else:
                send(p - 2)

            a_wait(p)
            work(p, told, tnew)
        return carry

    lax.fori_loop(0, NP // 2, body, 0)
    send(NP - 2)
    work(NP, ta, None)
    send(NP - 1)

    def rcopy(src, dst, ss, rr, dev):
        return pltpu.make_async_remote_copy(src_ref=src, dst_ref=dst, send_sem=ss, recv_sem=rr,
                                            device_id=(frag, dev), device_id_type=MESH)

    def bwait(view, sem):
        pltpu.make_async_copy(view, view, sem).wait()

    units = [(3, 0), (3, 1), (1, 0), (2, 0), (2, 1), (1, 1), (0, 0), (0, 1)]

    def part(buf, at, kc):
        return mm(kc, jnp.concatenate([buf[at + (slice(None), slice(r, r + 16))].reshape(240, 128)
                                       for r in range(0, 16 * HB, 16)], axis=1))

    for c, half in units:
        r = RS0 + 16 * HB * half
        w = part(sg.at[:, :, :, r:r + 16 * HB], (chips[c], core), k4c[0])
        for b in range(HB):
            sb[c, 128 * (HB * half + b):128 * (HB * half + b) + 128, :] = w[:, 128 * b:128 * b + 128]

    def half_rows(half):
        return slice(XROWS, RSR) if half else slice(0, XROWS)

    def rows(half, c):
        h = half_rows(half)
        n = (h.stop - h.start) // NCH
        return slice(h.start + n * c, h.start + n * c + n)

    def first(c, half):
        m = 1 if c == 3 else 0
        return rcopy(sb.at[c, half_rows(half)], p1.at[m, half_rows(half)], p1s.at[half, m], p1r.at[half, m],
                     (xn, yn)[half])

    sent_after = {1: (3, 0), 2: (3, 1)}
    bwait(rs, rssem)
    for n, (c, half) in enumerate(units):
        r = 16 * HB * half
        w = part(rs.at[:, :, r:r + 16 * HB], (chips[c],), k4c[1])
        for b in range(HB):
            at = slice(128 * (HB * half + b), 128 * (HB * half + b) + 128)
            sb[c, at, :] = sb[c, at, :] + w[:, 128 * b:128 * b + 128]
        if n in sent_after:
            first(*sent_after[n]).start()

    def put(w, a0):
        o2_ref[a0:a0 + w.shape[0]] = w[:, :, :NV]
        for k in range(VB):
            lo, hi = max(a0, 16 * k), min(a0 + w.shape[0], 16 * k + NV - GR)
            if lo < hi:
                n = min(GC, NV - GC * k)
                o2_ref[GR + lo - 16 * k:GR + hi - 16 * k, :, GC * k:GC * k + n] = w[lo - a0:hi - a0, :, NV:NV + n]

    for c in range(15):
        col = iota((128, 128), 1)
        w = mm(pi, one_hot(iota((128, 128), 0) == (col >> 4) + 8 * c))
        k4[:, c * 128:(c + 1) * 128] = jnp.where((iota((128, 128), 0) >> 3) == (col & 15), w, 0.0).astype(BF)
    e6[...] = one_hot((iota((128, 960), 1) >> 3) == iota((128, 960), 0))

    def v1_rows(t):
        row = iota((96, 128), 0) + 96 * t
        z = mm(one_hot((row >> 3) == iota((96, 128), 1)), cvt[...]).astype(BF)
        w = mm(z, e6[...])
        keep = (iota((96, 960), 0) & 7) == (iota((96, 960), 1) & 7)
        v1k[pl.ds(pl.multiple_of(96 * t, 96), 96), :] = jnp.where(keep, w, 0.0).astype(BF)

    def v1_build(t, carry):
        v1_rows(t)
        return carry

    lax.fori_loop(0, 9, v1_build, 0)
    for half, col in ((0, 1), (1, 2)):
        bwait(p1.at[1, half_rows(half)], p1s.at[half, 1])
        first(col, half).start()
    for half in range(2):
        bwait(p1.at[1, half_rows(half)], p1r.at[half, 1])
        z2[half_rows(half), :] = sb[2 - half, half_rows(half), :] + p1[1, half_rows(half), :]
    for c in range(NCH):
        for half in range(2):
            rcopy(z2.at[rows(half, c)], p2.at[rows(half, c)], p2s.at[half, c], p2r.at[half, c],
                  (yn, xn)[half]).start()
    for k in range(1, ND):
        src = lax.rem(me + k, ND)
        bwait(rg.at[src, :, 0:SENT], rgsem.at[src])

    v = rg[:, :, GO:GO + 8, :].reshape(960, 128)

    def v1_out(t, carry):
        w = mm(v1k[pl.ds(pl.multiple_of(96 * t, 96), 96), :], v)
        o1_ref[pl.ds(12 * t, 12)] = w.reshape(12, 8, 128)[:, :, :NV]
        return carry

    lax.fori_loop(0, 9, v1_out, 0)

    nx = -(-EX // 16)
    for ab in range(0, nx, 2):
        n = min(2, nx - ab)
        w = mm(k4[...], jnp.concatenate([rg[:, :, 16 * (ab + u):16 * (ab + u) + 16, :].reshape(1920, 128)
                                         for u in range(n)], axis=1)).reshape(16, 8, 128 * n)
        for u in range(n):
            put(w[:min(16, EX - 16 * (ab + u)), :, 128 * u:128 * u + 128], 16 * (ab + u))

    for half in range(2):
        bwait(p1.at[0, half_rows(half)], p1r.at[half, 0])
        sb[0, half_rows(half), :] = sb[0, half_rows(half), :] + p1[0, half_rows(half), :]
    for c in range(NCH):
        for half in range(2):
            bwait(p2.at[rows(half, c)], p2r.at[half, c])
            w = sb[0, rows(half, c), :] + p2[rows(half, c), :]
            put(w.reshape(-1, 8, 128), EX + rows(half, c).start // 8)

    for k in range(ND - 1):
        bwait(rg.at[0, :, 0:SENT], sgsem.at[k])
    bwait(rs, ssem)
    for c in range(NCH):
        for half in range(2):
            bwait(p2.at[rows(half, c)], p2s.at[half, c])
    for half in range(2):
        bwait(p1.at[0, half_rows(half)], p1s.at[half, 0])


def write_out(x1_ref, x2_ref, y1_ref, y2_ref, sem):
    copies = [pltpu.make_async_copy(x1_ref, y1_ref, sem.at[0]), pltpu.make_async_copy(x2_ref, y2_ref, sem.at[1])]
    for c in copies:
        c.start()
    for c in copies:
        c.wait()


def solution(mesh):
    def local_part(ao, co, cv):
        a = ao.reshape(NP, ROWS, NQ)
        co, cv = (pltpu.with_memory_space_constraint(t.T, pltpu.HBM) for t in (co, cv))
        vm = pl.BlockSpec(memory_space=pltpu.VMEM)
        o1, o2 = pl.pallas_call(
            kernel,
            out_shape=[jax.ShapeDtypeStruct((NV, NO, NV), F32), jax.ShapeDtypeStruct((NV, NO, NV), F32)],
            in_specs=[pl.BlockSpec(memory_space=pltpu.HBM)] * 3,
            out_specs=[vm, vm],
            scratch_shapes=[
                pltpu.VMEM((NBUF, ROWS, NQ), BF),
                pltpu.VMEM((8, 128, 128), BF),
                pltpu.VMEM((8, 128, 128), BF),
                pltpu.VMEM((4, 2, NP, RS1, 128), BF),
                pltpu.VMEM((8, NP, RS0, 128), BF),
                pltpu.VMEM((4, NP, RS1 - RS0, 128), BF),
                pltpu.VMEM((4, 128 * RSB, 128), F32),
                pltpu.VMEM((2, RSR, 128), F32),
                pltpu.VMEM((RSR, 128), F32),
                pltpu.VMEM((RSR, 128), F32),
                pltpu.VMEM((64, 960), BF),
                pltpu.VMEM((128, 1920), BF),
                pltpu.VMEM((2, 128, 240), BF),
                pltpu.VMEM((864, 960), BF),
                pltpu.VMEM((128, 960), BF),
                pltpu.VMEM((NO, NQ), BF),
                pltpu.VMEM((NV, NQ), BF),
                pltpu.VMEM((16, 128), BF),
                pltpu.VMEM((128, 128), BF),
                pltpu.VMEM((128, 128), BF),
                pltpu.SemaphoreType.DMA((NBUF,)),
                pltpu.SemaphoreType.DMA((2,)),
                pltpu.SemaphoreType.DMA((ND,)),
                pltpu.SemaphoreType.DMA((ND,)),
                pltpu.SemaphoreType.DMA,
                pltpu.SemaphoreType.DMA,
                pltpu.SemaphoreType.DMA((2, 2)),
                pltpu.SemaphoreType.DMA((2, 2)),
                pltpu.SemaphoreType.DMA((2, NCH)),
                pltpu.SemaphoreType.DMA((2, NCH)),
            ],
            compiler_params=pltpu.CompilerParams(collective_id=0, has_side_effects=True,
                                                 vmem_limit_bytes=34 * 1024 * 1024),
            name='mo_blocks',
        )(a, co, cv)
        o1, o2 = pl.pallas_call(
            write_out,
            out_shape=[jax.ShapeDtypeStruct((NV, NO, NV), F32), jax.ShapeDtypeStruct((NV, NO, NV), F32)],
            in_specs=[vm, vm],
            out_specs=[pl.BlockSpec(memory_space=pltpu.HBM)] * 2,
            scratch_shapes=[pltpu.SemaphoreType.DMA((2,))],
            compiler_params=pltpu.CompilerParams(vmem_limit_bytes=2 * 1024 * 1024),
            name='write_out',
        )(o1, o2)
        return o1.transpose(0, 2, 1), o2.transpose(1, 0, 2)

    return jax.shard_map(local_part, mesh=mesh,
                         in_specs=(P(('frag', 'dev')), P('frag'), P('frag')),
                         out_specs=(P('frag', None, 'dev'), P('frag', None, 'dev')),
                         check_vma=False)
```

```python
import jax
import jax.numpy as jnp
from jax import lax
from jax.experimental import pallas as pl
from jax.experimental.pallas import tpu as pltpu
from jax.sharding import PartitionSpec as P

MESH = pl.DeviceIdType.MESH
BF = jnp.bfloat16
F32 = jnp.float32
ND = 8
NP = 15
NQ = 120
NO = 8
NV = 108
ROWS = NQ * NQ
NBUF = 4
SPLIT = 5
VB = 6
GR = 16 * VB
GC = 20
EX = 40
VB = 6
GR = 16 * VB
GC = 20
GO = EX
SENT = EX + 8
RS0 = -(-SENT // 16) * 16
RSA = GR - EX
RSB = -(-RSA // 16)
RS1 = RS0 + 16 * RSB
RSR = 8 * RSA
NCH = 2
HB = RSB // 2
XROWS = 240


def mm(a, b):
    return jnp.dot(a, b, preferred_element_type=F32)


def mm_nt(a, b):
    return lax.dot_general(a, b, (((1,), (1,)), ((), ())), preferred_element_type=F32)


def iota(shape, dim):
    return lax.broadcasted_iota(jnp.int32, shape, dim)


def one_hot(mask):
    return jnp.where(mask, 1.0, 0.0).astype(BF)


def kernel(a_ref, co_ref, cv_ref, o1_ref, o2_ref,
           abuf, ta, tb, sg, rg, rs, sb, p1, z2, p2, k1, k4, k4c, v1k, e6, coin, cvin, cot, cvt, cv,
           asem, csem, sgsem, rgsem, ssem, rssem, p1s, p1r, p2s, p2r):
    me = lax.axis_index('dev')
    frag = lax.axis_index('frag')
    core = lax.rem(me, 2)
    mx = lax.rem(me // 2, 2)
    my = me // 4
    sib = me + 1 - 2 * core
    xn = me + 2 - 4 * mx
    yn = me + 4 - 8 * my
    dg = xn + 4 - 8 * my
    cols = [me, xn, yn, dg]
    chips = [c // 2 for c in cols]
    one = core * chips[1] + (1 - core) * chips[3]
    two = core * chips[3] + (1 - core) * chips[1]
    peers = [(one, 0), (chips[2], 0), (two, 0), (one, 1), (chips[2], 1), (two, 1), (chips[0], 1)]
    par = [core, 1 - core]

    def a_copies(p):
        slot = lax.rem(p, NBUF)
        step = ROWS // SPLIT
        return [pltpu.make_async_copy(a_ref.at[p, pl.ds(k * step, step)],
                                      abuf.at[slot, pl.ds(k * step, step)],
                                      asem.at[slot]) for k in range(SPLIT)]

    def a_start(p):
        for c in a_copies(p):
            c.start()

    def a_wait(p):
        slot = lax.rem(p, NBUF)
        pltpu.make_async_copy(a_ref.at[p], abuf.at[slot], asem.at[slot]).wait()

    cin = [pltpu.make_async_copy(co_ref, coin, csem.at[0]), pltpu.make_async_copy(cv_ref, cvin, csem.at[1])]
    for c in cin:
        c.start()
    for p in range(NBUF - 1):
        a_start(p)

    barrier = pltpu.get_barrier_semaphore()
    for k in range(1, ND):
        pl.semaphore_signal(barrier, inc=1, device_id=(frag, lax.rem(me + k, ND)), device_id_type=MESH)

    cot[...] = jnp.zeros(cot.shape, BF)
    cvt[...] = jnp.zeros(cvt.shape, BF)
    for c in cin:
        c.wait()
    cot[0:NO, 0:NQ] = coin[...]
    cvt[0:NV, 0:NQ] = cvin[...]
    cv[...] = mm_nt(one_hot(iota((128, 128), 0) == iota((128, 128), 1)), cvt[...]).astype(BF)
    xr = mm(one_hot((iota((64, 16), 0) >> 3) == iota((64, 16), 1)), cot[...]).astype(BF)
    diff = iota((128, 960), 1) - iota((128, 960), 0)
    hit = diff == 0
    for k in range(1, 8):
        hit = hit | (diff == 120 * k)
    off = iota((64, 960), 1) - 120 * (iota((64, 960), 0) & 7)
    k1[...] = jnp.where((off >= 0) & (off < 120), mm(xr, one_hot(hit)), 0.0).astype(BF)
    pi = mm(one_hot((iota((128, 16), 0) & 7) == iota((128, 16), 1)), cot[...]).astype(BF)
    for h, d in enumerate((me, sib)):
        col = iota((128, 240), 1)
        w = mm(pi, one_hot(iota((128, 240), 0) == (col >> 4) + NP * d))
        keep = (iota((128, 240), 0) >> 3) == (col & 15)
        k4c[h] = jnp.where(keep, w, 0.0).astype(BF)
    pl.semaphore_wait(barrier, ND - 1)

    pad = jnp.zeros((960, 8), BF)
    lane = iota((16, 128), 1)

    def step1(p, t, g):
        slot = lax.rem(p, NBUF)
        left = jnp.concatenate([abuf[slot, 1920 * g:1920 * g + 960, :], pad], axis=1)
        if g < 7:
            right = jnp.concatenate([abuf[slot, 1920 * g + 960:1920 * g + 1920, :], pad], axis=1)
            out = mm(k1[...], jnp.concatenate([left, right], axis=1))
            lo = out[:, :128].reshape(8, 8, 128)
            hi = out[:, 128:].reshape(8, 8, 128)
        else:
            lo = mm(k1[...], left).reshape(8, 8, 128)
            hi = jnp.zeros((8, 8, 128), F32)
        t[:, 16 * g:16 * g + 16, :] = jnp.concatenate([lo, hi], axis=1).astype(BF)

    def step2(t, x):
        h = mm(t[x:x + 2].reshape(256, 128), cv[...]).astype(BF)
        return jnp.concatenate([h[:128], h[128:]], axis=1)

    def step3(p, x, h):
        g = mm(cvt[0:112, :], h)
        for y in range(2):
            last = g[GR:GR + 16, 128 * y:128 * y + 128]
            tiles = [jnp.where(lane < NV, g[16 * k:16 * k + 16, 128 * y:128 * y + 128],
                               pltpu.roll(last, (NV - GC * k) % 128, 1)) for k in range(VB)]
            tiles = jnp.concatenate(tiles, axis=0)
            sg[x // 2, y, p, 0:EX] = tiles[:EX].astype(BF)
            sg[x // 2, y, p, RS0:RS0 + RSA] = tiles[EX:].astype(BF)

    def step2o(t):
        hoo = mm_nt(cot[...], t[...].reshape(1024, 128))
        return jnp.concatenate([hoo[0:8, 128 * x:128 * x + 128] for x in range(8)], axis=0).astype(BF)

    def step3o(p, hoo):
        goo = mm(hoo, cv[...]).astype(BF).reshape(4, 2, 8, 128)
        for y in range(2):
            sg[:, y, p, GO:GO + 8] = goo[:, y]

    def work(p, told, tnew):
        def one(g):
            if tnew is not None:
                step1(p, tnew, g)

        h0 = step2(told, 0)
        one(0)
        h1 = step2(told, 2)
        one(1)
        step3(p - 1, 0, h0)
        h2 = step2(told, 4)
        one(2)
        step3(p - 1, 2, h1)
        h3 = step2(told, 6)
        one(3)
        step3(p - 1, 4, h2)
        hoo = step2o(told)
        one(4)
        step3(p - 1, 6, h3)
        one(5)
        step3o(p - 1, hoo)
        one(6)
        one(7)

    def sends(p):
        out = [pltpu.make_async_remote_copy(
            src_ref=sg.at[:, 1 - core, p, RS0:RS1], dst_ref=rs.at[:, p],
            send_sem=ssem, recv_sem=rssem, device_id=(frag, sib), device_id_type=MESH)]
        for k, (chip, q) in enumerate(peers):
            out.append(pltpu.make_async_remote_copy(
                src_ref=sg.at[chip, par[q], p, 0:SENT], dst_ref=rg.at[me, p, 0:SENT],
                send_sem=sgsem.at[k], recv_sem=rgsem.at[me],
                device_id=(frag, 2 * chip + par[q]), device_id_type=MESH))
        return out

    def send(p):
        for c in sends(p):
            c.start()
        rg[me, p, 0:SENT] = sg[chips[0], core, p, 0:SENT]

    if RS0 + RSA < RS1:
        sg[:, :, :, RS0 + RSA:RS1, :] = jnp.zeros((4, 2, NP, RS1 - RS0 - RSA, 128), BF)
    a_wait(0)
    a_start(NBUF - 1)
    for g in range(8):
        step1(0, ta, g)

    def body(k, carry):
        for p, told, tnew in ((2 * k + 1, ta, tb), (2 * k + 2, tb, ta)):
            @pl.when(p + NBUF - 1 < NP)
            def _():
                a_start(p + NBUF - 1)

            if told is ta:
                @pl.when(k > 0)
                def _():
                    send(p - 2)
            else:
                send(p - 2)

            a_wait(p)
            work(p, told, tnew)
        return carry

    lax.fori_loop(0, NP // 2, body, 0)
    send(NP - 2)
    work(NP, ta, None)
    send(NP - 1)

    def rcopy(src, dst, ss, rr, dev):
        return pltpu.make_async_remote_copy(src_ref=src, dst_ref=dst, send_sem=ss, recv_sem=rr,
                                            device_id=(frag, dev), device_id_type=MESH)

    def bwait(view, sem):
        pltpu.make_async_copy(view, view, sem).wait()

    units = [(3, 0), (3, 1), (1, 0), (2, 0), (2, 1), (1, 1), (0, 0), (0, 1)]

    def part(buf, at, kc):
        return mm(kc, jnp.concatenate([buf[at + (slice(None), slice(r, r + 16))].reshape(240, 128)
                                       for r in range(0, 16 * HB, 16)], axis=1))

    for c, half in units:
        r = RS0 + 16 * HB * half
        w = part(sg.at[:, :, :, r:r + 16 * HB], (chips[c], core), k4c[0])
        for b in range(HB):
            sb[c, 128 * (HB * half + b):128 * (HB * half + b) + 128, :] = w[:, 128 * b:128 * b + 128]

    def half_rows(half):
        return slice(XROWS, RSR) if half else slice(0, XROWS)

    def rows(half, c):
        h = half_rows(half)
        n = (h.stop - h.start) // NCH
        return slice(h.start + n * c, h.start + n * c + n)

    def first(c, half):
        m = 1 if c == 3 else 0
        return rcopy(sb.at[c, half_rows(half)], p1.at[m, half_rows(half)], p1s.at[half, m], p1r.at[half, m],
                     (xn, yn)[half])

    sent_after = {1: (3, 0), 2: (3, 1)}
    bwait(rs, rssem)
    for n, (c, half) in enumerate(units):
        r = 16 * HB * half
        w = part(rs.at[:, :, r:r + 16 * HB], (chips[c],), k4c[1])
        for b in range(HB):
            at = slice(128 * (HB * half + b), 128 * (HB * half + b) + 128)
            sb[c, at, :] = sb[c, at, :] + w[:, 128 * b:128 * b + 128]
        if n in sent_after:
            first(*sent_after[n]).start()

    def put(w, a0):
        o2_ref[a0:a0 + w.shape[0]] = w[:, :, :NV]
        for k in range(VB):
            lo, hi = max(a0, 16 * k), min(a0 + w.shape[0], 16 * k + NV - GR)
            if lo < hi:
                n = min(GC, NV - GC * k)
                o2_ref[GR + lo - 16 * k:GR + hi - 16 * k, :, GC * k:GC * k + n] = w[lo - a0:hi - a0, :, NV:NV + n]

    for c in range(15):
        col = iota((128, 128), 1)
        w = mm(pi, one_hot(iota((128, 128), 0) == (col >> 4) + 8 * c))
        k4[:, c * 128:(c + 1) * 128] = jnp.where((iota((128, 128), 0) >> 3) == (col & 15), w, 0.0).astype(BF)
    e6[...] = one_hot((iota((128, 960), 1) >> 3) == iota((128, 960), 0))

    def v1_rows(t):
        row = iota((96, 128), 0) + 96 * t
        z = mm(one_hot((row >> 3) == iota((96, 128), 1)), cvt[...]).astype(BF)
        w = mm(z, e6[...])
        keep = (iota((96, 960), 0) & 7) == (iota((96, 960), 1) & 7)
        v1k[pl.ds(pl.multiple_of(96 * t, 96), 96), :] = jnp.where(keep, w, 0.0).astype(BF)

    def v1_build(t, carry):
        v1_rows(t)
        return carry

    lax.fori_loop(0, 9, v1_build, 0)
    for half, col in ((0, 1), (1, 2)):
        bwait(p1.at[1, half_rows(half)], p1s.at[half, 1])
        first(col, half).start()
    for half in range(2):
        bwait(p1.at[1, half_rows(half)], p1r.at[half, 1])
        z2[half_rows(half), :] = sb[2 - half, half_rows(half), :] + p1[1, half_rows(half), :]
    for c in range(NCH):
        for half in range(2):
            rcopy(z2.at[rows(half, c)], p2.at[rows(half, c)], p2s.at[half, c], p2r.at[half, c],
                  (yn, xn)[half]).start()
    for k in range(1, ND):
        src = lax.rem(me + k, ND)
        bwait(rg.at[src, :, 0:SENT], rgsem.at[src])

    v = rg[:, :, GO:GO + 8, :].reshape(960, 128)

    def v1_out(t, carry):
        w = mm(v1k[pl.ds(pl.multiple_of(96 * t, 96), 96), :], v)
        o1_ref[pl.ds(12 * t, 12)] = w.reshape(12, 8, 128)[:, :, :NV]
        return carry

    lax.fori_loop(0, 9, v1_out, 0)

    nx = -(-EX // 16)
    for ab in range(0, nx, 2):
        n = min(2, nx - ab)
        w = mm(k4[...], jnp.concatenate([rg[:, :, 16 * (ab + u):16 * (ab + u) + 16, :].reshape(1920, 128)
                                         for u in range(n)], axis=1)).reshape(16, 8, 128 * n)
        for u in range(n):
            put(w[:min(16, EX - 16 * (ab + u)), :, 128 * u:128 * u + 128], 16 * (ab + u))

    for half in range(2):
        bwait(p1.at[0, half_rows(half)], p1r.at[half, 0])
        sb[0, half_rows(half), :] = sb[0, half_rows(half), :] + p1[0, half_rows(half), :]
    for c in range(NCH):
        for half in range(2):
            bwait(p2.at[rows(half, c)], p2r.at[half, c])
            w = sb[0, rows(half, c), :] + p2[rows(half, c), :]
            put(w.reshape(-1, 8, 128), EX + rows(half, c).start // 8)

    for k in range(ND - 1):
        bwait(rg.at[0, :, 0:SENT], sgsem.at[k])
    bwait(rs, ssem)
    for c in range(NCH):
        for half in range(2):
            bwait(p2.at[rows(half, c)], p2s.at[half, c])
    for half in range(2):
        bwait(p1.at[0, half_rows(half)], p1s.at[half, 0])


def write_out(x1_ref, x2_ref, y1_ref, y2_ref, sem):
    copies = [pltpu.make_async_copy(x1_ref, y1_ref, sem.at[0]), pltpu.make_async_copy(x2_ref, y2_ref, sem.at[1])]
    for c in copies:
        c.start()
    for c in copies:
        c.wait()


def solution(mesh):
    def local_part(ao, co, cv):
        a = ao.reshape(NP, ROWS, NQ)
        co, cv = (pltpu.with_memory_space_constraint(t.T, pltpu.HBM) for t in (co, cv))
        vm = pl.BlockSpec(memory_space=pltpu.VMEM)
        o1, o2 = pl.pallas_call(
            kernel,
            out_shape=[jax.ShapeDtypeStruct((NV, NO, NV), F32), jax.ShapeDtypeStruct((NV, NO, NV), F32)],
            in_specs=[pl.BlockSpec(memory_space=pltpu.HBM)] * 3,
            out_specs=[vm, vm],
            scratch_shapes=[
                pltpu.VMEM((NBUF, ROWS, NQ), BF),
                pltpu.VMEM((8, 128, 128), BF),
                pltpu.VMEM((8, 128, 128), BF),
                pltpu.VMEM((4, 2, NP, RS1, 128), BF),
                pltpu.VMEM((8, NP, RS0, 128), BF),
                pltpu.VMEM((4, NP, RS1 - RS0, 128), BF),
                pltpu.VMEM((4, 128 * RSB, 128), F32),
                pltpu.VMEM((2, RSR, 128), F32),
                pltpu.VMEM((RSR, 128), F32),
                pltpu.VMEM((RSR, 128), F32),
                pltpu.VMEM((64, 960), BF),
                pltpu.VMEM((128, 1920), BF),
                pltpu.VMEM((2, 128, 240), BF),
                pltpu.VMEM((864, 960), BF),
                pltpu.VMEM((128, 960), BF),
                pltpu.VMEM((NO, NQ), BF),
                pltpu.VMEM((NV, NQ), BF),
                pltpu.VMEM((16, 128), BF),
                pltpu.VMEM((128, 128), BF),
                pltpu.VMEM((128, 128), BF),
                pltpu.SemaphoreType.DMA((NBUF,)),
                pltpu.SemaphoreType.DMA((2,)),
                pltpu.SemaphoreType.DMA((ND,)),
                pltpu.SemaphoreType.DMA((ND,)),
                pltpu.SemaphoreType.DMA,
                pltpu.SemaphoreType.DMA,
                pltpu.SemaphoreType.DMA((2, 2)),
                pltpu.SemaphoreType.DMA((2, 2)),
                pltpu.SemaphoreType.DMA((2, NCH)),
                pltpu.SemaphoreType.DMA((2, NCH)),
            ],
            compiler_params=pltpu.CompilerParams(collective_id=0, has_side_effects=True,
                                                 vmem_limit_bytes=34 * 1024 * 1024),
            name='mo_blocks',
        )(a, co, cv)
        o1, o2 = pl.pallas_call(
            write_out,
            out_shape=[jax.ShapeDtypeStruct((NV, NO, NV), F32), jax.ShapeDtypeStruct((NV, NO, NV), F32)],
            in_specs=[vm, vm],
            out_specs=[pl.BlockSpec(memory_space=pltpu.HBM)] * 2,
            scratch_shapes=[pltpu.SemaphoreType.DMA((2,))],
            compiler_params=pltpu.CompilerParams(vmem_limit_bytes=2 * 1024 * 1024),
            name='write_out',
        )(o1, o2)
        return o1.transpose(0, 2, 1), o2.transpose(1, 0, 2)

    return jax.shard_map(local_part, mesh=mesh,
                         in_specs=(P(('frag', 'dev')), P('frag'), P('frag')),
                         out_specs=(P('frag', None, 'dev'), P('frag', None, 'dev')),
                         check_vma=False)
```

```python
import jax
import jax.numpy as jnp
from jax import lax
from jax.experimental import pallas as pl
from jax.experimental.pallas import tpu as pltpu
from jax.sharding import PartitionSpec as P

MESH = pl.DeviceIdType.MESH
BF = jnp.bfloat16
F32 = jnp.float32
ND = 8
NP = 15
NQ = 120
NO = 8
NV = 108
ROWS = NQ * NQ
NBUF = 4
SPLIT = 5
VB = 6
GR = 16 * VB
GC = 20
EX = 40
VB = 6
GR = 16 * VB
GC = 20
GO = EX
SENT = EX + 8
RS0 = -(-SENT // 16) * 16
RSA = GR - EX
RSB = -(-RSA // 16)
RS1 = RS0 + 16 * RSB
RSR = 8 * RSA
NCH = 2
HB = RSB // 2
XROWS = 256


def mm(a, b):
    return jnp.dot(a, b, preferred_element_type=F32)


def mm_nt(a, b):
    return lax.dot_general(a, b, (((1,), (1,)), ((), ())), preferred_element_type=F32)


def iota(shape, dim):
    return lax.broadcasted_iota(jnp.int32, shape, dim)


def one_hot(mask):
    return jnp.where(mask, 1.0, 0.0).astype(BF)


def kernel(a_ref, co_ref, cv_ref, o1_ref, o2_ref,
           abuf, ta, tb, sg, rg, rs, sb, p1, z2, p2, k1, k4, k4c, v1k, e6, coin, cvin, cot, cvt, cv,
           asem, csem, sgsem, rgsem, ssem, rssem, p1s, p1r, p2s, p2r):
    me = lax.axis_index('dev')
    frag = lax.axis_index('frag')
    core = lax.rem(me, 2)
    mx = lax.rem(me // 2, 2)
    my = me // 4
    sib = me + 1 - 2 * core
    xn = me + 2 - 4 * mx
    yn = me + 4 - 8 * my
    dg = xn + 4 - 8 * my
    cols = [me, xn, yn, dg]
    chips = [c // 2 for c in cols]
    one = core * chips[1] + (1 - core) * chips[3]
    two = core * chips[3] + (1 - core) * chips[1]
    peers = [(one, 0), (chips[2], 0), (two, 0), (one, 1), (chips[2], 1), (two, 1), (chips[0], 1)]
    par = [core, 1 - core]

    def a_copies(p):
        slot = lax.rem(p, NBUF)
        step = ROWS // SPLIT
        return [pltpu.make_async_copy(a_ref.at[p, pl.ds(k * step, step)],
                                      abuf.at[slot, pl.ds(k * step, step)],
                                      asem.at[slot]) for k in range(SPLIT)]

    def a_start(p):
        for c in a_copies(p):
            c.start()

    def a_wait(p):
        slot = lax.rem(p, NBUF)
        pltpu.make_async_copy(a_ref.at[p], abuf.at[slot], asem.at[slot]).wait()

    cin = [pltpu.make_async_copy(co_ref, coin, csem.at[0]), pltpu.make_async_copy(cv_ref, cvin, csem.at[1])]
    for c in cin:
        c.start()
    for p in range(NBUF - 1):
        a_start(p)

    barrier = pltpu.get_barrier_semaphore()
    for k in range(1, ND):
        pl.semaphore_signal(barrier, inc=1, device_id=(frag, lax.rem(me + k, ND)), device_id_type=MESH)

    cot[...] = jnp.zeros(cot.shape, BF)
    cvt[...] = jnp.zeros(cvt.shape, BF)
    for c in cin:
        c.wait()
    cot[0:NO, 0:NQ] = coin[...]
    cvt[0:NV, 0:NQ] = cvin[...]
    cv[...] = mm_nt(one_hot(iota((128, 128), 0) == iota((128, 128), 1)), cvt[...]).astype(BF)
    xr = mm(one_hot((iota((64, 16), 0) >> 3) == iota((64, 16), 1)), cot[...]).astype(BF)
    diff = iota((128, 960), 1) - iota((128, 960), 0)
    hit = diff == 0
    for k in range(1, 8):
        hit = hit | (diff == 120 * k)
    off = iota((64, 960), 1) - 120 * (iota((64, 960), 0) & 7)
    k1[...] = jnp.where((off >= 0) & (off < 120), mm(xr, one_hot(hit)), 0.0).astype(BF)
    pi = mm(one_hot((iota((128, 16), 0) & 7) == iota((128, 16), 1)), cot[...]).astype(BF)
    for h, d in enumerate((me, sib)):
        col = iota((128, 240), 1)
        w = mm(pi, one_hot(iota((128, 240), 0) == (col >> 4) + NP * d))
        keep = (iota((128, 240), 0) >> 3) == (col & 15)
        k4c[h] = jnp.where(keep, w, 0.0).astype(BF)
    pl.semaphore_wait(barrier, ND - 1)

    pad = jnp.zeros((960, 8), BF)
    lane = iota((16, 128), 1)

    def step1(p, t, g):
        slot = lax.rem(p, NBUF)
        left = jnp.concatenate([abuf[slot, 1920 * g:1920 * g + 960, :], pad], axis=1)
        if g < 7:
            right = jnp.concatenate([abuf[slot, 1920 * g + 960:1920 * g + 1920, :], pad], axis=1)
            out = mm(k1[...], jnp.concatenate([left, right], axis=1))
            lo = out[:, :128].reshape(8, 8, 128)
            hi = out[:, 128:].reshape(8, 8, 128)
        else:
            lo = mm(k1[...], left).reshape(8, 8, 128)
            hi = jnp.zeros((8, 8, 128), F32)
        t[:, 16 * g:16 * g + 16, :] = jnp.concatenate([lo, hi], axis=1).astype(BF)

    def step2(t, x):
        h = mm(t[x:x + 2].reshape(256, 128), cv[...]).astype(BF)
        return jnp.concatenate([h[:128], h[128:]], axis=1)

    def step3(p, x, h):
        g = mm(cvt[0:112, :], h)
        for y in range(2):
            last = g[GR:GR + 16, 128 * y:128 * y + 128]
            tiles = [jnp.where(lane < NV, g[16 * k:16 * k + 16, 128 * y:128 * y + 128],
                               pltpu.roll(last, (NV - GC * k) % 128, 1)) for k in range(VB)]
            tiles = jnp.concatenate(tiles, axis=0)
            sg[x // 2, y, p, 0:EX] = tiles[:EX].astype(BF)
            sg[x // 2, y, p, RS0:RS0 + RSA] = tiles[EX:].astype(BF)

    def step2o(t):
        hoo = mm_nt(cot[...], t[...].reshape(1024, 128))
        return jnp.concatenate([hoo[0:8, 128 * x:128 * x + 128] for x in range(8)], axis=0).astype(BF)

    def step3o(p, hoo):
        goo = mm(hoo, cv[...]).astype(BF).reshape(4, 2, 8, 128)
        for y in range(2):
            sg[:, y, p, GO:GO + 8] = goo[:, y]

    def work(p, told, tnew):
        def one(g):
            if tnew is not None:
                step1(p, tnew, g)

        h0 = step2(told, 0)
        one(0)
        h1 = step2(told, 2)
        one(1)
        step3(p - 1, 0, h0)
        h2 = step2(told, 4)
        one(2)
        step3(p - 1, 2, h1)
        h3 = step2(told, 6)
        one(3)
        step3(p - 1, 4, h2)
        hoo = step2o(told)
        one(4)
        step3(p - 1, 6, h3)
        one(5)
        step3o(p - 1, hoo)
        one(6)
        one(7)

    def sends(p):
        out = [pltpu.make_async_remote_copy(
            src_ref=sg.at[:, 1 - core, p, RS0:RS1], dst_ref=rs.at[:, p],
            send_sem=ssem, recv_sem=rssem, device_id=(frag, sib), device_id_type=MESH)]
        for k, (chip, q) in enumerate(peers):
            out.append(pltpu.make_async_remote_copy(
                src_ref=sg.at[chip, par[q], p, 0:SENT], dst_ref=rg.at[me, p, 0:SENT],
                send_sem=sgsem.at[k], recv_sem=rgsem.at[me],
                device_id=(frag, 2 * chip + par[q]), device_id_type=MESH))
        return out

    def send(p):
        for c in sends(p):
            c.start()
        rg[me, p, 0:SENT] = sg[chips[0], core, p, 0:SENT]

    if RS0 + RSA < RS1:
        sg[:, :, :, RS0 + RSA:RS1, :] = jnp.zeros((4, 2, NP, RS1 - RS0 - RSA, 128), BF)
    a_wait(0)
    a_start(NBUF - 1)
    for g in range(8):
        step1(0, ta, g)

    def body(k, carry):
        for p, told, tnew in ((2 * k + 1, ta, tb), (2 * k + 2, tb, ta)):
            @pl.when(p + NBUF - 1 < NP)
            def _():
                a_start(p + NBUF - 1)

            if told is ta:
                @pl.when(k > 0)
                def _():
                    send(p - 2)
            else:
                send(p - 2)

            a_wait(p)
            work(p, told, tnew)
        return carry

    lax.fori_loop(0, NP // 2, body, 0)
    send(NP - 2)
    work(NP, ta, None)
    send(NP - 1)

    def rcopy(src, dst, ss, rr, dev):
        return pltpu.make_async_remote_copy(src_ref=src, dst_ref=dst, send_sem=ss, recv_sem=rr,
                                            device_id=(frag, dev), device_id_type=MESH)

    def bwait(view, sem):
        pltpu.make_async_copy(view, view, sem).wait()

    units = [(3, 0), (3, 1), (1, 0), (2, 0), (2, 1), (1, 1), (0, 0), (0, 1)]

    def part(buf, at, kc):
        return mm(kc, jnp.concatenate([buf[at + (slice(None), slice(r, r + 16))].reshape(240, 128)
                                       for r in range(0, 16 * HB, 16)], axis=1))

    for c, half in units:
        r = RS0 + 16 * HB * half
        w = part(sg.at[:, :, :, r:r + 16 * HB], (chips[c], core), k4c[0])
        for b in range(HB):
            sb[c, 128 * (HB * half + b):128 * (HB * half + b) + 128, :] = w[:, 128 * b:128 * b + 128]

    def half_rows(half):
        return slice(XROWS, RSR) if half else slice(0, XROWS)

    def rows(half, c):
        h = half_rows(half)
        n = (h.stop - h.start) // NCH
        return slice(h.start + n * c, h.start + n * c + n)

    def first(c, half):
        m = 1 if c == 3 else 0
        return rcopy(sb.at[c, half_rows(half)], p1.at[m, half_rows(half)], p1s.at[half, m], p1r.at[half, m],
                     (xn, yn)[half])

    sent_after = {1: (3, 0), 2: (3, 1)}
    bwait(rs, rssem)
    for n, (c, half) in enumerate(units):
        r = 16 * HB * half
        w = part(rs.at[:, :, r:r + 16 * HB], (chips[c],), k4c[1])
        for b in range(HB):
            at = slice(128 * (HB * half + b), 128 * (HB * half + b) + 128)
            sb[c, at, :] = sb[c, at, :] + w[:, 128 * b:128 * b + 128]
        if n in sent_after:
            first(*sent_after[n]).start()

    def put(w, a0):
        o2_ref[a0:a0 + w.shape[0]] = w[:, :, :NV]
        for k in range(VB):
            lo, hi = max(a0, 16 * k), min(a0 + w.shape[0], 16 * k + NV - GR)
            if lo < hi:
                n = min(GC, NV - GC * k)
                o2_ref[GR + lo - 16 * k:GR + hi - 16 * k, :, GC * k:GC * k + n] = w[lo - a0:hi - a0, :, NV:NV + n]

    for c in range(15):
        col = iota((128, 128), 1)
        w = mm(pi, one_hot(iota((128, 128), 0) == (col >> 4) + 8 * c))
        k4[:, c * 128:(c + 1) * 128] = jnp.where((iota((128, 128), 0) >> 3) == (col & 15), w, 0.0).astype(BF)
    e6[...] = one_hot((iota((128, 960), 1) >> 3) == iota((128, 960), 0))

    def v1_rows(t):
        row = iota((96, 128), 0) + 96 * t
        z = mm(one_hot((row >> 3) == iota((96, 128), 1)), cvt[...]).astype(BF)
        w = mm(z, e6[...])
        keep = (iota((96, 960), 0) & 7) == (iota((96, 960), 1) & 7)
        v1k[pl.ds(pl.multiple_of(96 * t, 96), 96), :] = jnp.where(keep, w, 0.0).astype(BF)

    def v1_build(t, carry):
        v1_rows(t)
        return carry

    lax.fori_loop(0, 9, v1_build, 0)
    for half, col in ((0, 1), (1, 2)):
        bwait(p1.at[1, half_rows(half)], p1s.at[half, 1])
        first(col, half).start()
    for half in range(2):
        bwait(p1.at[1, half_rows(half)], p1r.at[half, 1])
        z2[half_rows(half), :] = sb[2 - half, half_rows(half), :] + p1[1, half_rows(half), :]
    for c in range(NCH):
        for half in range(2):
            rcopy(z2.at[rows(half, c)], p2.at[rows(half, c)], p2s.at[half, c], p2r.at[half, c],
                  (yn, xn)[half]).start()
    for k in range(1, ND):
        src = lax.rem(me + k, ND)
        bwait(rg.at[src, :, 0:SENT], rgsem.at[src])

    v = rg[:, :, GO:GO + 8, :].reshape(960, 128)

    def v1_out(t, carry):
        w = mm(v1k[pl.ds(pl.multiple_of(96 * t, 96), 96), :], v)
        o1_ref[pl.ds(12 * t, 12)] = w.reshape(12, 8, 128)[:, :, :NV]
        return carry

    lax.fori_loop(0, 9, v1_out, 0)

    nx = -(-EX // 16)
    for ab in range(0, nx, 2):
        n = min(2, nx - ab)
        w = mm(k4[...], jnp.concatenate([rg[:, :, 16 * (ab + u):16 * (ab + u) + 16, :].reshape(1920, 128)
                                         for u in range(n)], axis=1)).reshape(16, 8, 128 * n)
        for u in range(n):
            put(w[:min(16, EX - 16 * (ab + u)), :, 128 * u:128 * u + 128], 16 * (ab + u))

    for half in range(2):
        bwait(p1.at[0, half_rows(half)], p1r.at[half, 0])
        sb[0, half_rows(half), :] = sb[0, half_rows(half), :] + p1[0, half_rows(half), :]
    for c in range(NCH):
        for half in range(2):
            bwait(p2.at[rows(half, c)], p2r.at[half, c])
            w = sb[0, rows(half, c), :] + p2[rows(half, c), :]
            put(w.reshape(-1, 8, 128), EX + rows(half, c).start // 8)

    for k in range(ND - 1):
        bwait(rg.at[0, :, 0:SENT], sgsem.at[k])
    bwait(rs, ssem)
    for c in range(NCH):
        for half in range(2):
            bwait(p2.at[rows(half, c)], p2s.at[half, c])
    for half in range(2):
        bwait(p1.at[0, half_rows(half)], p1s.at[half, 0])


def write_out(x1_ref, x2_ref, y1_ref, y2_ref, sem):
    copies = [pltpu.make_async_copy(x1_ref, y1_ref, sem.at[0]), pltpu.make_async_copy(x2_ref, y2_ref, sem.at[1])]
    for c in copies:
        c.start()
    for c in copies:
        c.wait()


def solution(mesh):
    def local_part(ao, co, cv):
        a = ao.reshape(NP, ROWS, NQ)
        co, cv = (pltpu.with_memory_space_constraint(t.T, pltpu.HBM) for t in (co, cv))
        vm = pl.BlockSpec(memory_space=pltpu.VMEM)
        o1, o2 = pl.pallas_call(
            kernel,
            out_shape=[jax.ShapeDtypeStruct((NV, NO, NV), F32), jax.ShapeDtypeStruct((NV, NO, NV), F32)],
            in_specs=[pl.BlockSpec(memory_space=pltpu.HBM)] * 3,
            out_specs=[vm, vm],
            scratch_shapes=[
                pltpu.VMEM((NBUF, ROWS, NQ), BF),
                pltpu.VMEM((8, 128, 128), BF),
                pltpu.VMEM((8, 128, 128), BF),
                pltpu.VMEM((4, 2, NP, RS1, 128), BF),
                pltpu.VMEM((8, NP, RS0, 128), BF),
                pltpu.VMEM((4, NP, RS1 - RS0, 128), BF),
                pltpu.VMEM((4, 128 * RSB, 128), F32),
                pltpu.VMEM((2, RSR, 128), F32),
                pltpu.VMEM((RSR, 128), F32),
                pltpu.VMEM((RSR, 128), F32),
                pltpu.VMEM((64, 960), BF),
                pltpu.VMEM((128, 1920), BF),
                pltpu.VMEM((2, 128, 240), BF),
                pltpu.VMEM((864, 960), BF),
                pltpu.VMEM((128, 960), BF),
                pltpu.VMEM((NO, NQ), BF),
                pltpu.VMEM((NV, NQ), BF),
                pltpu.VMEM((16, 128), BF),
                pltpu.VMEM((128, 128), BF),
                pltpu.VMEM((128, 128), BF),
                pltpu.SemaphoreType.DMA((NBUF,)),
                pltpu.SemaphoreType.DMA((2,)),
                pltpu.SemaphoreType.DMA((ND,)),
                pltpu.SemaphoreType.DMA((ND,)),
                pltpu.SemaphoreType.DMA,
                pltpu.SemaphoreType.DMA,
                pltpu.SemaphoreType.DMA((2, 2)),
                pltpu.SemaphoreType.DMA((2, 2)),
                pltpu.SemaphoreType.DMA((2, NCH)),
                pltpu.SemaphoreType.DMA((2, NCH)),
            ],
            compiler_params=pltpu.CompilerParams(collective_id=0, has_side_effects=True,
                                                 vmem_limit_bytes=34 * 1024 * 1024),
            name='mo_blocks',
        )(a, co, cv)
        o1, o2 = pl.pallas_call(
            write_out,
            out_shape=[jax.ShapeDtypeStruct((NV, NO, NV), F32), jax.ShapeDtypeStruct((NV, NO, NV), F32)],
            in_specs=[vm, vm],
            out_specs=[pl.BlockSpec(memory_space=pltpu.HBM)] * 2,
            scratch_shapes=[pltpu.SemaphoreType.DMA((2,))],
            compiler_params=pltpu.CompilerParams(vmem_limit_bytes=2 * 1024 * 1024),
            name='write_out',
        )(o1, o2)
        return o1.transpose(0, 2, 1), o2.transpose(1, 0, 2)

    return jax.shard_map(local_part, mesh=mesh,
                         in_specs=(P(('frag', 'dev')), P('frag'), P('frag')),
                         out_specs=(P('frag', None, 'dev'), P('frag', None, 'dev')),
                         check_vma=False)
```
